32 devices in a mesh: row: 8 (over z, x), col: 4 (over y, core).
Axes of the slice: x: 2, y: 2, z: 4, core: 2. Of those that a mesh axis runs over, the one named last changes fastest.
Arguments:
- p_values: bfloat16 [96, 512, 128], P('row', 'col'), may hold values from -0.8984375 to 0.8984375
- p_where: int32 [96, 8], P('row', 'col'), may hold values from 0 to 63, as said below
- p_count: int32 [8, 4], P('row', 'col'), may hold values from 6 to 12, as said below
- h_values: bfloat16 [96, 512, 128], P('row', 'col'), may hold values from -3 to 3
- h_where: int32 [96, 8], P('row', 'col'), may hold values from 0 to 63, as said below
- h_count: int32 [8, 4], P('row', 'col'), may hold values from 6 to 12, as said below
Outputs:
- ph_values: bfloat16 [96, 512, 128], P('row', 'col')
- php_values: bfloat16 [96, 512, 128], P('row', 'col')
- energy: float32 [], replicated
The draws below stay inside these ranges and needn't reach their ends.
Inputs may be any that keep to these rules, and one draw needn't show every extreme that they name: `p_where`: the 12 slots of the device of row index i and column index j name distinct blocks of its own tile: block rows i * 8 to i * 8 + 7 and the j-th of 4 equal ranges of block columns. `h_where`: as for p_where. `p_count`: some device has all 12 slots live. `h_count`: some device has all 12 slots live.
All inputs are finite; a program needn't handle non-finite values.
Results may differ from the reference program's by a relative error of at most 0.0049.
Values may be sent and summed in bfloat16 or wider, within the bound.
A program may use at most 64 MiB of HBM per device.

```python
import jax
import jax.numpy as jnp
from jax import lax

BLK = 128
TILE = 8
CAP = 12
NBLK = 64
N_ROW = 8
N_COL = 4


def tile_coords(key):
    tile_cols = NBLK // N_COL
    keys_all = jax.random.split(key, N_ROW * N_COL)

    def one_tile(tile_key):
        return jax.random.permutation(tile_key, TILE * tile_cols)[:CAP]
    picks = jax.vmap(one_tile)(keys_all).reshape(N_ROW, N_COL, CAP)
    row_base = (jnp.arange(N_ROW, dtype=jnp.int32) * TILE)[:, None, None]
    col_base = (jnp.arange(N_COL, dtype=jnp.int32) * tile_cols)[None, :, None]
    block_rows = picks // tile_cols + row_base
    block_cols = picks % tile_cols + col_base
    stacked = jnp.stack([block_rows, block_cols], axis=-1)
    return jnp.transpose(stacked, (0, 2, 1, 3)).reshape(N_ROW * CAP, N_COL * 2).astype(jnp.int32)


def slot_counts(key):
    low_key, full_key = jax.random.split(key)
    counts = jax.random.randint(low_key, (N_ROW * N_COL,), (CAP + 1) // 2, CAP + 1)
    where_full = jax.random.randint(full_key, (), 0, N_ROW * N_COL)
    return counts.at[where_full].set(CAP).reshape(N_ROW, N_COL).astype(jnp.int32)


def draw_p_where(key, part):
    return tile_coords(jax.random.fold_in(key, 3))


def draw_h_where(key, part):
    return tile_coords(jax.random.fold_in(key, 5))


def draw_p_count(key, part):
    return slot_counts(jax.random.fold_in(key, 7))


def draw_h_count(key, part):
    return slot_counts(jax.random.fold_in(key, 11))


def level_of(own_key, extent, cuts, smallest, top_value):
    loudness = 1.0
    for dim, parts in cuts:
        heights = jax.random.uniform(jax.random.fold_in(jax.random.fold_in(own_key, 6), dim), (parts,), jnp.float32, smallest / len(cuts), top_value / len(cuts))
        loudness = loudness * jnp.repeat(jnp.exp(heights), extent[dim] // parts).reshape((-1,) + (1,) * (len(extent) - 1 - dim))
    return loudness


def gaussian(own_key, shape, deviation, bound, cuts=(), kind=jnp.bfloat16):
    loudness = level_of(own_key, shape, cuts, -0.22, 0.18) if cuts else 1.0
    result = jax.random.normal(own_key, shape, jnp.float32) * deviation * loudness
    return jnp.minimum(jnp.maximum(result, -bound), bound).astype(kind)


def setup_inputs(seed: int = 0) -> dict:
    splits = jax.random.split(jax.random.key(seed), 7)
    return {
        "p_values": gaussian(splits[0], (N_ROW * CAP, N_COL * BLK, BLK), 0.15, 0.8984375, ((0, 8), (1, 4))),
        "p_where": draw_p_where(jax.random.fold_in(splits[6], 71), 0),
        "p_count": draw_p_count(jax.random.fold_in(splits[6], 71), 0),
        "h_values": gaussian(splits[3], (N_ROW * CAP, N_COL * BLK, BLK), 0.5, 3.0, ((0, 8), (1, 4))),
        "h_where": draw_h_where(jax.random.fold_in(splits[6], 71), 0),
        "h_count": draw_h_count(jax.random.fold_in(splits[6], 71), 0),
    }


def index_table(where_arg, count_arg):
    shaped = where_arg.reshape(N_ROW, CAP, N_COL, 2)
    block_rows = shaped[..., 0].reshape(-1)
    block_cols = shaped[..., 1].reshape(-1)
    slot_ids = jnp.arange(CAP, dtype=jnp.int32)[None, :, None]
    live_slots = (slot_ids < count_arg[:, None, :]).reshape(-1)
    flat_ids = jnp.arange(N_ROW * CAP * N_COL, dtype=jnp.int32)
    target_rows = jnp.where(live_slots, block_rows, NBLK).astype(jnp.int32)
    table = jnp.full((NBLK, NBLK), -1, jnp.int32).at[target_rows, block_cols].set(flat_ids, mode="drop")
    return table, block_rows, block_cols, live_slots


def flatten_values(values):
    return values.reshape(N_ROW * CAP, N_COL, BLK, BLK).reshape(-1, BLK, BLK)


def unflatten_values(flat):
    return flat.reshape(N_ROW * CAP, N_COL, BLK, BLK).reshape(N_ROW * CAP, N_COL * BLK, BLK)


def sparse_product(left_flat, left_table, right_flat, right_table, block_rows, block_cols):
    def one_block(coords):
        row_ids = left_table[coords[0], :]
        col_ids = right_table[:, coords[1]]
        left_blocks = jnp.take(left_flat, jnp.maximum(row_ids, 0), axis=0)
        right_blocks = jnp.take(right_flat, jnp.maximum(col_ids, 0), axis=0)
        left_blocks = jnp.where((row_ids >= 0)[:, None, None], left_blocks.astype(jnp.float32), jnp.float32(0.0))
        right_blocks = jnp.where((col_ids >= 0)[:, None, None], right_blocks.astype(jnp.float32), jnp.float32(0.0))
        return jnp.einsum("kxy,kyz->xz", left_blocks, right_blocks)

    return lax.map(one_block, (block_rows, block_cols))


def reference(p_values, p_where, p_count, h_values, h_where, h_count):
    p_table, block_rows, block_cols, live_slots = index_table(p_where, p_count)
    h_table, h_rows, h_cols, h_live = index_table(h_where, h_count)
    p_flat = flatten_values(p_values)
    h_flat = flatten_values(h_values)
    first_sum = sparse_product(p_flat, p_table, h_flat, h_table, block_rows, block_cols)
    first_sum = jnp.where(live_slots[:, None, None], first_sum, jnp.float32(0.0))
    traces = jnp.trace(first_sum, axis1=1, axis2=2)
    energy = jnp.sum(jnp.where(live_slots & (block_rows == block_cols), traces, jnp.float32(0.0)))
    ph_flat = first_sum.astype(jnp.bfloat16)
    second_sum = sparse_product(ph_flat, p_table, p_flat, p_table, block_rows, block_cols)
    second_sum = jnp.where(live_slots[:, None, None], second_sum, jnp.float32(0.0))
    php_flat = second_sum.astype(jnp.bfloat16)
    return unflatten_values(ph_flat), unflatten_values(php_flat), energy
```

```python
import functools

import jax
import jax.numpy as jnp
from jax import lax
from jax.experimental import pallas as pl
from jax.experimental.pallas import tpu as pltpu
from jax.sharding import PartitionSpec as P

TILE = 8
CHUNKS = 6
IN_FLIGHT = 16
MESH = pl.DeviceIdType.MESH
ANY = pl.BlockSpec(memory_space=pl.ANY)
VMEM = pl.BlockSpec(memory_space=pltpu.VMEM)
SMEM = pl.BlockSpec(memory_space=pltpu.SMEM)


def at_row(r):
    return (r, lax.axis_index("col"))


def at_col(c):
    return (lax.axis_index("row"), c)


def remote(src, dst, send_sem, recv_sem, device):
    return pltpu.make_async_remote_copy(
        src_ref=src,
        dst_ref=dst,
        send_sem=send_sem,
        recv_sem=recv_sem,
        device_id=device,
        device_id_type=MESH,
    )


def greet(rows, cols):
    me_row, me_col = lax.axis_index("row"), lax.axis_index("col")
    barrier = pltpu.get_barrier_semaphore()
    for d in range(1, rows):
        pl.semaphore_signal(
            barrier, inc=1, device_id=at_row((me_row + d) % rows), device_id_type=MESH
        )
    for d in range(1, cols):
        pl.semaphore_signal(
            barrier, inc=1, device_id=at_col((me_col + d) % cols), device_id_type=MESH
        )
    pl.semaphore_wait(barrier, rows + cols - 2)


class ColumnGather:
    def __init__(self, rows, own, land, out, up_send, down_send, x_send, recv, local):
        self.own, self.land, self.out = own, land, out
        self.up_send, self.down_send, self.x_send = up_send, down_send, x_send
        self.recv, self.local = recv, local
        self.inner = 2 if rows % 2 == 0 else 1
        self.outer = rows // self.inner
        self.chunks = recv.shape[1]
        self.size = own.shape[0] // self.chunks
        self.me = lax.axis_index("row")
        self.x, self.z = self.me % self.inner, self.me // self.inner
        self.cross_first = 1 if self.inner == 2 and self.chunks > 1 else 0

    def later(self, ch):
        return (ch + self.cross_first) % self.chunks

    def row(self, z, line):
        return z * self.inner + (self.x if line == 0 else self.inner - 1 - self.x)

    def part(self, ch):
        return pl.ds(ch * self.size, self.size)

    def copy(self, r, ch, own, way):
        sems, target = {
            "up": (self.up_send, self.me + self.inner),
            "down": (self.down_send, self.me - self.inner),
            "x": (self.x_send, self.row(self.z, 1)),
        }[way]
        part = self.part(ch)
        src = self.own.at[part] if own else self.land.at[r, part]
        return remote(src, self.land.at[r, part], sems.at[r, ch], self.recv.at[r, ch], at_row(target))

    def keep(self, r, ch):
        part = self.part(ch)
        return pltpu.make_async_copy(self.land.at[r, part], self.out.at[r, part], self.local.at[r, ch])

    def along(self, r, ch, own, act):
        @pl.when(self.z < self.outer - 1)
        def _():
            act(self.copy(r, ch, own, "up"))

        @pl.when(self.z > 0)
        def _():
            act(self.copy(r, ch, own, "down"))

    def arrive(self, r, ch):
        self.copy(r, ch, False, "x").wait_recv()
        self.keep(r, ch).start()

    def start(self):
        for ch in range(self.chunks):
            if self.inner == 2:
                self.copy(self.me, ch, True, "x").start()
            self.along(self.me, self.later(ch), True, lambda copy: copy.start())
        if self.cross_first:
            r = self.row(self.z, 1)
            self.arrive(r, 0)
            self.along(r, 0, False, lambda copy: copy.start())

    def pieces(self):
        lines = [(self.later(ch), 0) for ch in range(self.chunks)]
        return lines + [(0, 1)] * self.cross_first

    def relayed(self, d, side, ch, line, act):
        z = self.z - d if side == 0 else self.z + d
        there = self.z >= d if side == 0 else self.z + d < self.outer
        r = self.row(z, line)

        @pl.when(there)
        def _():
            if act == "start":
                self.arrive(r, ch)
            on = self.z < self.outer - 1 if side == 0 else self.z > 0

            @pl.when(on)
            def _():
                copy = self.copy(r, ch, False, "up" if side == 0 else "down")
                copy.start() if act == "start" else copy.wait_send()

            if self.inner == 2 and ch >= self.cross_first:
                copy = self.copy(r, ch, False, "x")
                copy.start() if act == "start" else copy.wait_send()

    def relay(self, d):
        for ch, line in self.pieces():
            for side in range(2):
                self.relayed(d, side, ch, line, "start")

    def finish(self):
        if self.inner == 2:
            for ch in range(self.cross_first, self.chunks):
                self.arrive(self.row(self.z, 1), ch)
            for d in range(1, self.outer):
                for side in range(2):
                    z = self.z - d if side == 0 else self.z + d
                    there = self.z >= d if side == 0 else self.z + d < self.outer

                    @pl.when(there)
                    def _():
                        for ch in range(self.cross_first, self.chunks):
                            self.arrive(self.row(z, 1), ch)
        for ch in range(self.chunks):
            if self.inner == 2:
                self.copy(self.me, ch, True, "x").wait_send()
            self.along(self.me, ch, True, lambda copy: copy.wait_send())
        if self.cross_first:
            self.along(self.row(self.z, 1), 0, False, lambda copy: copy.wait_send())
        for d in range(1, self.outer):
            for ch, line in self.pieces():
                for side in range(2):
                    self.relayed(d, side, ch, line, "wait")
        for r in range(self.inner * self.outer):
            @pl.when(r != self.me)
            def _():
                for ch in range(self.chunks):
                    self.keep(r, ch).wait()


def col_copies(cols, own, out, send, recv):
    me = lax.axis_index("col")
    made = []
    for d in range(1, cols):
        made.append(
            remote(own, out.at[me], send.at[d], recv.at[d], at_col((me + d) % cols))
        )
    return made


def row_copies(rows, own, out, send, recv):
    me = lax.axis_index("row")
    made = []
    for d in range(1, rows):
        made.append(
            remote(own, out.at[me], send.at[d], recv.at[d], at_row((me + d) % rows))
        )
    return made


def first_gather(
    rows, cols, p_ref, h_ref, meta_ref, prow, hcol, prow_meta, col_meta,
    land, up_send, down_send, x_send, recv, out_sems,
    p_send, p_recv, mc_send, mc_recv, mr_send, mr_recv, local,
):
    me_row, me_col = lax.axis_index("row"), lax.axis_index("col")
    keep = [
        pltpu.make_async_copy(h_ref, hcol.at[me_row], local.at[0]),
        pltpu.make_async_copy(p_ref, prow.at[me_col], local.at[1]),
        pltpu.make_async_copy(meta_ref, prow_meta.at[me_col], local.at[2]),
        pltpu.make_async_copy(meta_ref, col_meta.at[me_row], local.at[3]),
    ]
    greet(rows, cols)
    gather = ColumnGather(
        rows, h_ref, land, hcol, up_send, down_send, x_send, recv, out_sems
    )
    across = (
        col_copies(cols, p_ref, prow, p_send, p_recv)
        + col_copies(cols, meta_ref, prow_meta, mc_send, mc_recv)
        + row_copies(rows, meta_ref, col_meta, mr_send, mr_recv)
    )
    for copy in across + keep:
        copy.start()
    gather.start()
    for d in range(1, gather.outer):
        gather.relay(d)
    gather.finish()
    for copy in across + keep:
        copy.wait()


def second_gather(
    rows, cols, p_ref, f_ref, e_ref, frow, pcol, e_out,
    e_cols, e_rows, e_sum,
    land, up_send, down_send, x_send, recv, out_sems,
    p_send, p_recv, ec_send, ec_recv, er_send, er_recv, local,
):
    me_row, me_col = lax.axis_index("row"), lax.axis_index("col")
    keep = [
        pltpu.make_async_copy(p_ref, pcol.at[me_row], local.at[0]),
        pltpu.make_async_copy(f_ref, frow.at[me_col], local.at[1]),
    ]
    greet(rows, cols)
    energies = col_copies(cols, e_ref, e_cols, ec_send, ec_recv)
    for copy in energies:
        copy.start()
    gather = ColumnGather(
        rows, p_ref, land, pcol, up_send, down_send, x_send, recv, out_sems
    )
    across = col_copies(cols, f_ref, frow, p_send, p_recv)
    for copy in across + keep:
        copy.start()
    gather.start()
    e_cols[me_col] = e_ref[...]
    for copy in energies:
        copy.wait()
    total = e_cols[0]
    for c in range(1, cols):
        total = total + e_cols[c]
    e_sum[...] = total
    e_rows[me_row] = total
    if gather.outer > 1:
        gather.relay(1)
    sums = row_copies(rows, e_sum, e_rows, er_send, er_recv)
    for copy in sums:
        copy.start()
    for d in range(2, gather.outer):
        gather.relay(d)
    for copy in sums:
        copy.wait()
    total = e_rows[0]
    for r in range(1, rows):
        total = total + e_rows[r]
    e_out[...] = total
    gather.finish()
    for copy in across + keep:
        copy.wait()


def block_products(
    rows, cols, right_lane, with_trace, lmeta, rmeta, left, right, *rest
):
    if with_trace:
        out, e_out = rest[:2]
    else:
        e_in, out, e_out = rest[:3]
    acc, lbuf, rbuf, head, nxt, inner, mask, table, ml, mr, ms, sems = rest[-12:]
    slots = out.shape[0]
    i, j = lax.axis_index("row"), lax.axis_index("col")
    nblk = rows * TILE
    tile_cols = nblk // cols
    words = -(-nblk // 32)
    count_lane = 4 * slots
    acc[...] = jnp.zeros_like(acc)

    for t in range(TILE + 1):
        head[t] = -1

    for t in range(tile_cols * words + 1):
        mask[t] = 0

    @pl.loop(0, cols)
    def _(c):
        live = lmeta[c, 0, count_lane]
        for s in range(slots):
            row = jnp.where(s < live, lmeta[c, 0, s] - i * TILE, TILE)
            idx = c * slots + s
            inner[idx] = lmeta[c, 0, slots + s]
            nxt[idx] = head[row]
            head[row] = idx

    @pl.loop(0, rows)
    def _(r):
        live = rmeta[r, 0, count_lane + (1 if right_lane else 0)]
        for s in range(slots):
            k = rmeta[r, 0, right_lane + s]
            col = rmeta[r, 0, right_lane + slots + s] - j * tile_cols
            word = jnp.where(s < live, col * words + (k >> 5), tile_cols * words)
            mask[word] = mask[word] | (jnp.int32(1) << (k & 31))
            table[jnp.where(s < live, k * tile_cols + col, nblk * tile_cols)] = r * slots + s

    def find_slot(s, n):
        row = lmeta[j, 0, s] - i * TILE
        col = lmeta[j, 0, slots + s] - j * tile_cols

        def more(state):
            return state[0] >= 0

        def step(state):
            at, n = state
            k = inner[at]
            ml[n] = at
            mr[n] = table[k * tile_cols + col]
            ms[n] = s
            return nxt[at], n + ((mask[col * words + (k >> 5)] >> (k & 31)) & 1)

        return lax.while_loop(more, step, (head[row], n))[1]

    own_count = lmeta[j, 0, count_lane]
    found = lax.fori_loop(0, own_count, find_slot, jnp.int32(0))

    def fetch(base, m):
        a, b = ml[base + m], mr[base + m]
        return (
            pltpu.make_async_copy(left.at[a], lbuf.at[m], sems.at[0, m]),
            pltpu.make_async_copy(right.at[b], rbuf.at[m], sems.at[1, m]),
        )

    @pl.loop(0, (found + IN_FLIGHT - 1) // IN_FLIGHT)
    def _(chunk):
        base = chunk * IN_FLIGHT
        size = jnp.minimum(found - base, IN_FLIGHT)

        @pl.loop(0, size)
        def _(m):
            for copy in fetch(base, m):
                copy.start()

        @pl.loop(0, size)
        def _(m):
            for copy in fetch(base, m):
                copy.wait()
            s = ms[base + m]
            acc[s] += jnp.dot(lbuf[m], rbuf[m], preferred_element_type=jnp.float32)

    out[...] = acc[...].astype(out.dtype)
    if with_trace:
        size = acc.shape[1]
        e_out[...] = jnp.zeros_like(e_out)
        diagonal = lax.broadcasted_iota(jnp.int32, (size, size), 0) == lax.broadcasted_iota(
            jnp.int32, (size, size), 1
        )

        @pl.loop(0, own_count)
        def _(s):
            @pl.when(lmeta[j, 0, s] == lmeta[j, 0, slots + s])
            def _():
                e_out[...] += jnp.sum(jnp.where(diagonal, acc[s], 0.0))
    else:
        e_out[0, 0] = e_in[0, 0]


def dense_path(rows, cols, p_values, p_where, p_count, h_values, h_where, h_count):
    slots, size, _ = p_values.shape
    dtype = p_values.dtype
    nblk = rows * TILE
    tile_cols = nblk // cols
    words = -(-nblk // 32)
    meta = jnp.concatenate(
        [p_where[:, 0], p_where[:, 1], h_where[:, 0], h_where[:, 1], p_count[0], h_count[0]]
    )
    meta = jnp.broadcast_to(jnp.pad(meta, (0, 128 - meta.shape[0]))[None, :], (8, 128))
    dma = pltpu.SemaphoreType.DMA
    chunks = CHUNKS if slots % CHUNKS == 0 else 1
    chunk_sems = [pltpu.VMEM((rows, slots, size, size), dtype)] + [dma((rows, chunks))] * 5
    col_sems = [dma((cols,)), dma((cols,))]
    row_sems = [dma((rows,)), dma((rows,))]
    tile = (slots, size, size)
    prow, hcol, prow_meta, col_meta = pl.pallas_call(
        functools.partial(first_gather, rows, cols),
        out_shape=[
            jax.ShapeDtypeStruct((cols,) + tile, dtype),
            jax.ShapeDtypeStruct((rows,) + tile, dtype),
            jax.ShapeDtypeStruct((cols, 8, 128), jnp.int32),
            jax.ShapeDtypeStruct((rows, 8, 128), jnp.int32),
        ],
        in_specs=[VMEM] * 3,
        out_specs=[ANY] * 4,
        scratch_shapes=chunk_sems + col_sems + col_sems + row_sems + [dma((4,))],
        compiler_params=pltpu.CompilerParams(collective_id=0, has_side_effects=True),
        name="first_gather",
    )(p_values, h_values, meta)

    def products(right_lane, with_trace, lmeta, rmeta, left, right, *more):
        smem = lambda n: pltpu.SMEM((n,), jnp.int32)
        most = slots * nblk + 1
        return pl.pallas_call(
            functools.partial(block_products, rows, cols, right_lane, with_trace),
            out_shape=[
                jax.ShapeDtypeStruct(tile, dtype),
                jax.ShapeDtypeStruct((8, 128) if with_trace else (1, 1), jnp.float32),
            ],
            in_specs=[SMEM, SMEM, ANY, ANY] + [SMEM] * len(more),
            out_specs=[VMEM, VMEM if with_trace else SMEM],
            scratch_shapes=[
                pltpu.VMEM(tile, jnp.float32),
                pltpu.VMEM((IN_FLIGHT, size, size), dtype),
                pltpu.VMEM((IN_FLIGHT, size, size), dtype),
                smem(TILE + 1),
                smem(cols * slots),
                smem(cols * slots),
                smem(tile_cols * words + 1),
                smem(nblk * tile_cols + 1),
                smem(most),
                smem(most),
                smem(most),
                dma((2, IN_FLIGHT)),
            ],
            name="products",
        )(
            lmeta,
            rmeta,
            left.reshape((cols * slots, size, size)),
            right.reshape((rows * slots, size, size)),
            *more,
        )

    ph_values, part = products(2 * slots, True, prow_meta, col_meta, prow, hcol)
    frow, pcol, energy = pl.pallas_call(
        functools.partial(second_gather, rows, cols),
        out_shape=[
            jax.ShapeDtypeStruct((cols,) + tile, dtype),
            jax.ShapeDtypeStruct((rows,) + tile, dtype),
            jax.ShapeDtypeStruct((8, 128), jnp.float32),
        ],
        in_specs=[VMEM] * 3,
        out_specs=[ANY, ANY, VMEM],
        scratch_shapes=[
            pltpu.VMEM((cols, 8, 128), jnp.float32),
            pltpu.VMEM((rows, 8, 128), jnp.float32),
            pltpu.VMEM((8, 128), jnp.float32),
        ]
        + chunk_sems + col_sems + col_sems + row_sems + [dma((2,))],
        compiler_params=pltpu.CompilerParams(collective_id=1, has_side_effects=True),
        name="second_gather",
    )(p_values, ph_values, part)
    php_values, energy = products(0, False, prow_meta, col_meta, frow, pcol, energy)
    return (ph_values, php_values, energy[0, 0])


CAP_H_Z, CAP_P_Z = 18, 12
CAP_H, CAP_P = 13, 9
CAP_F = 5
CAP_1, CAP_2 = 15, 13
LIST = 16
F32, BF16, I32 = jnp.float32, jnp.bfloat16, jnp.int32


def log2(n):
    return n.bit_length() - 1


def power(n):
    return n > 0 and n & (n - 1) == 0


class Shape:
    def __init__(self, rows, cols, slots, size):
        self.rows, self.cols, self.slots, self.size = rows, cols, slots, size
        self.devices = rows * cols
        self.nblk = rows * TILE
        self.inner = 2 if rows % 2 == 0 else 1
        self.outer = rows // self.inner
        self.group = min(cols, 4)
        self.team = self.inner * self.group
        self.strip = size // self.team
        self.width = self.nblk // cols
        self.chips = cols // 2
        self.partner = slots
        self.others = 2 * slots
        self.row_n = self.outer - 1
        self.row_m = self.row_n + self.inner
        self.row_f = self.row_m + 2
        self.table = -(-(self.row_f + self.chips - 1) // 8) * 8

    def fits(self):
        return (
            power(self.rows)
            and power(self.cols)
            and self.cols >= 2
            and self.rows >= 2
            and self.nblk <= 128
            and self.width * TILE <= 128
            and self.slots <= 15
            and self.strip % 16 == 0
            and self.group * LIST <= 64
        )


def mm(a, b):
    return lax.dot_general(a.astype(BF16), b.astype(BF16), (((1,), (0,)), ((), ())), preferred_element_type=F32)


def mt(a, b):
    return lax.dot_general(a.astype(BF16), b.astype(BF16), (((1,), (1,)), ((), ())), preferred_element_type=F32)


def tm(a, b):
    return lax.dot_general(a.astype(BF16), b.astype(BF16), (((0,), (0,)), ((), ())), preferred_element_type=F32)


def ones(cond):
    return jnp.where(cond, 1.0, 0.0).astype(F32)


def iota(shape, dim):
    return lax.broadcasted_iota(I32, shape, dim)


def make_lists(sh, x, z, j, pw, p_count, message, tabv):
    n, width = sh.nblk, sh.width
    i = z * sh.inner + x
    lw, ll = log2(width), 3 + log2(sh.inner)
    r, l = iota((n, n), 0), iota((n, n), 1)
    g = j // sh.group
    eight = jnp.ones((8, n), F32)

    a0, d0 = iota((sh.cols * n, sh.devices), 0), iota((sh.cols * n, sh.devices), 1)
    pick = ones(d0 == ((a0 & (n - 1)) >> 3) * sh.cols + (a0 >> log2(n)))
    spread = mm(pick, message)
    a1, l1 = iota((sh.cols * n, 128), 0), iota((sh.cols * n, 128), 1)
    spread = jnp.where((l1 >> lw) == (a1 & 7), spread, 0.0)
    l2, m2 = iota((128, n), 0), iota((128, n), 1)
    spread = mm(spread, ones((l2 & (width - 1)) == (m2 & (width - 1))))
    both = jnp.zeros((n, n), F32)
    for c in range(sh.cols):
        both = both + jnp.where((l >> lw) == c, spread[c * n : (c + 1) * n], 0.0)
    hs = jnp.floor(both * (1.0 / 16.0))
    ps = both - 16.0 * hs
    pm, hm = ones(ps > 0.5), ones(hs > 0.5)
    fm = pm * ones(mm(pm, hm) > 0.5)
    slot = {"H": hs - 1.0, "P": ps - 1.0}
    live = {"H": hm, "P": pm}
    left = {"H": pm, "P": fm}
    lane_tile = l >> lw
    group_tri = ones((lane_tile // sh.group == (r >> lw) // sh.group) & (r < l))
    group_full = ones(lane_tile // sh.group == (r >> lw) // sh.group)
    seg_tri = ones((lane_tile == (r >> lw)) & (r < l))
    seg_full = ones(lane_tile == (r >> lw))
    low = ones(l < r)
    up = ones(r < l)
    low_layer = ones((l < r) & ((l >> ll) == (r >> ll)))
    in_group = ones(lane_tile // sh.group == g)
    over = jnp.zeros((1, n), F32)

    def count_over(over, v, pos, cap):
        return over + jnp.sum(v * ones(pos > cap - 0.5), axis=0, keepdims=True)

    def extract(starts, counts, v, pos, payloads, size):
        at = iota((size, n), 0).astype(F32)
        rows = ones((starts <= at) & (at < starts + counts))
        hit = mm(rows, v * (pos + 1.0)) == at + 1.0
        return rows, [jnp.where(hit, mm(rows, p), 0.0) for p in payloads]

    def put(row, lane, value, count):
        tabv[row : row + 1, lane : lane + count] = value[0:1, 0:count].astype(I32)

    team = ((r >> 3) & (sh.inner - 1)) * sh.group + lane_tile % sh.group
    pos_mine = {}
    for kind, cap_z, cap, shift in (("H", CAP_H_Z, CAP_H, 0), ("P", CAP_P_Z, CAP_P, 64)):
        near = (team * sh.slots).astype(F32) + slot[kind]
        need = []
        for xd in range(sh.inner):
            here = ones((r >> 3) == z * sh.inner + xd)
            need.append(ones(tm(left[kind] * here, pm) > 0.5) * live[kind])
        for dz in range(sh.outer):
            if dz == 0:
                v = need[0] if sh.inner == 1 else jnp.maximum(need[0], need[1])
            else:
                there = ones((r >> ll) == (z + dz) % sh.outer)
                v = ones(tm(left[kind] * there, pm) > 0.5) * live[kind] * ones((r >> ll) == z)
            v = v * in_group
            pos = mm(v, group_tri) + mm(low_layer, mm(v, group_full))
            if dz == 0:
                pos_z = pos
                continue
            counts = mt(eight, v)
            starts = mm(counts, up)
            size = -(-cap_z // 8) * 8
            _, (found,) = extract(starts[0:1], counts[0:1], v, pos, [near], size)
            put(dz - 1, shift, mt(eight, found), size)
            over = count_over(over, v, pos, cap_z)
        far = (sh.team * sh.slots + (r >> ll) * cap_z).astype(F32) + jnp.minimum(pos_z, cap_z - 1.0)
        payload = jnp.where((r >> ll) == z, near, far)
        mine = jnp.zeros((n, n), F32)
        e0, e1 = iota((8, n), 0), iota((8, n), 1)
        columns = ones(((e1 >> lw) == g * sh.group + e0) & (e0 < sh.group))
        for xd in range(sh.inner):
            v = need[xd]
            pos = mm(v, seg_tri) + mm(low, mm(v, seg_full))
            over = count_over(over, v, pos, cap)
            mine = mine + jnp.where(x == xd, 1.0, 0.0) * pos
            counts = mt(columns, v)
            starts = mm(counts, up)
            rows = []
            at = iota((LIST, n), 0).astype(F32)
            for a in range(sh.group):
                rows.append(ones((starts[a : a + 1] <= at) & (at < starts[a : a + 1] + counts[a : a + 1])))
            rows = jnp.concatenate(rows, axis=0)
            total = sh.group * LIST
            t0, t1 = iota((total, n), 0), iota((total, n), 1)
            here = (mm(rows, v * (pos + 1.0)) == ((t0 & (LIST - 1)) + 1).astype(F32)) & (
                (t1 >> lw) == g * sh.group + (t0 >> log2(LIST))
            )
            found = mt(eight, jnp.where(here, mm(rows, payload), 0.0))
            put(sh.row_n + xd, shift, found, total)
        pos_mine[kind] = jnp.minimum(mine, cap - 1.0)

    chip = j // 2
    lane_chip = lane_tile // 2
    in_rows = ones((r >> 3) == i)
    for dc in range(sh.chips):
        there = ones(lane_chip == (chip + dc) % sh.chips)
        v = ones(mt(pm * there, pm) > 0.5) * fm * in_rows
        pos = mm(v, seg_tri) + mm(low, mm(v, seg_full))
        if dc == 0:
            pos_f = jnp.minimum(pos, CAP_F - 1.0)
            continue
        v = v * ones(lane_tile == j)
        counts = mt(eight, v)
        starts = mm(counts, up)
        _, (found,) = extract(starts[0:1], counts[0:1], v, pos, [slot["P"]], 8)
        put(sh.row_f + dc - 1, 0, mt(eight, found), 8)
        over = count_over(over, v, pos, CAP_F)

    s0, s1 = iota((LIST, n), 0), iota((LIST, n), 1)
    row_of = jnp.full((LIST, n), -1, I32)
    col_of = jnp.full((LIST, n), -1, I32)
    for s in range(sh.slots):
        row_of = jnp.where((s0 == s) & (s < p_count[0, 0]), pw[s, 0], row_of)
        col_of = jnp.where((s0 == s) & (s < p_count[0, 0]), pw[s, 1], col_of)
    oh_row, oh_col = ones(row_of == s1), ones(col_of == s1)
    k_tile = lane_tile.astype(F32)
    left_1 = k_tile * sh.slots + slot["P"]
    left_2 = jnp.where(
        lane_tile == j,
        slot["P"],
        jnp.where(lane_chip == chip, sh.partner + slot["P"], sh.others + k_tile * CAP_F + pos_f),
    )
    q0, q1 = iota((LIST, LIST), 0), iota((LIST, LIST), 1)
    for step, (kind, from_left, cap) in enumerate((("H", left_1, CAP_1), ("P", left_2, CAP_2))):
        w = mm(oh_row, left[kind]) * mt(oh_col, live[kind])
        li = mm(oh_row, from_left * pm)
        ri = mt(oh_col, pos_mine[kind])
        counts_s = mm(w, jnp.ones((n, n), F32))
        pos = mm(w, up) + mm(ones(q1 < q0), counts_s)
        over = count_over(over, w, pos, cap)
        counts = mt(eight, w)
        starts = mm(counts, ones(q0 < q1))
        at = q0.astype(F32)
        rows = ones((starts[0:1] <= at) & (at < starts[0:1] + counts[0:1]))
        hit = mm(rows, w * (pos + 1.0)) == s0.astype(F32) + 1.0
        row = sh.row_m + step
        put(row, 0, mt(eight, jnp.where(hit, mm(rows, li), 0.0)), LIST)
        put(row, 16, mt(eight, jnp.where(hit, mm(rows, ri), 0.0)), LIST)
        keep = rows * ones(at > starts[0:1])
        put(row, 32, mt(jnp.ones((8, LIST), F32), keep), LIST)
        last = jnp.where(counts > 0.5, jnp.minimum(starts + counts - 1.0, cap), 1.0 * cap)
        put(row, 48, last, LIST)
    return over


def sparse_products(
    sh, p_ref, h_ref, pw, pc, hw, hc, ph_out, php_out, e_out,
    message, messages, near_h, near_p, store_h, store_p, prow, pack_hz, pack_pz, pack_h, pack_p,
    land_h, land_p, terms_1, terms_2, fstore, pack_f, tabv, tab, emsg, emsgs, esum,
    m_send, m_recv, s_send, s_recv, p_send, p_fwd, p_recv, z_send, z_recv,
    t_send, t_recv, f_send, f_fwd, f_recv, e_send, e_recv, t_copy,
):
    i, j = lax.axis_index("row"), lax.axis_index("col")
    x, z = i % sh.inner, i // sh.inner
    me = i * sh.cols + j
    g, a = j // sh.group, j % sh.group
    chip, core = j // 2, j % 2
    mate = (i, chip * 2 + 1 - core)
    team = x * sh.group + a
    slots, strip, size = sh.slots, sh.strip, sh.size
    all_but_me = sh.devices - 1

    def device(d):
        t = (me + d) % sh.devices
        return (t // sh.cols, t % sh.cols)

    def member(d):
        q = (team + d) % sh.team
        return q, (z * sh.inner + q // sh.group, g * sh.group + q % sh.group)

    def in_strip(q):
        return pl.ds(pl.multiple_of(q * strip, strip), strip)

    lane = iota((1, 128), 1)
    packed = jnp.zeros((1, 128), F32)
    for where, count, scale in ((pw, pc, 1.0), (hw, hc, 16.0)):
        for s in range(slots):
            at = (where[s, 0] - i * TILE) * sh.width + where[s, 1] - j * sh.width
            packed = packed + jnp.where((lane == at) & (s < count[0, 0]), scale * (s + 1), 0.0)
    message[0] = packed
    messages[me] = packed

    barrier = pltpu.get_barrier_semaphore()

    @pl.loop(1, sh.devices)
    def _(d):
        pl.semaphore_signal(barrier, inc=1, device_id=device(d), device_id_type=MESH)

    for s in range(slots):
        near_h[team * slots + s] = h_ref[s, in_strip(team), :]
        near_p[team * slots + s] = p_ref[s, in_strip(team), :]
        prow[j * slots + s] = p_ref[s]
    pl.semaphore_wait(barrier, all_but_me)

    def tell(d):
        return remote(message.at[pl.ds(0, 1)], messages.at[pl.ds(me, 1)], m_send, m_recv, device(d))

    @pl.loop(1, sh.devices)
    def _(d):
        tell(d).start()

    def strips(d, which):
        q, dev = member(d)
        ref, near = ((h_ref, near_h), (p_ref, near_p))[which]
        return remote(
            ref.at[:, in_strip(q), :], near.at[pl.ds(team * slots, slots)],
            s_send.at[which, d], s_recv.at[which, team], dev,
        )

    def strips_in(d, which):
        q, dev = member(d)
        ref, near = ((h_ref, near_h), (p_ref, near_p))[which]
        return remote(
            ref.at[:, in_strip(q), :], near.at[pl.ds(q * slots, slots)],
            s_send.at[which, d], s_recv.at[which, q], dev,
        )

    for which in range(2):
        for d in range(1, sh.team):
            strips(d, which).start()

    def other(dc):
        c = (chip + dc) % sh.chips
        return c, c * 2 + core

    def p_block(col):
        return prow.at[pl.ds(col * slots, slots)]

    def p_out(dc):
        return remote(p_ref, p_block(j), p_send.at[dc], p_recv.at[j], (i, other(dc)[1]) if dc else mate)

    def p_in(col):
        return remote(p_ref, p_block(col), p_send.at[0], p_recv.at[col], mate)

    def p_forward(dc):
        col = other(dc)[1]
        return remote(p_block(col), p_block(col), p_fwd.at[dc], p_recv.at[col], mate)

    for dc in range(sh.chips):
        p_out(dc).start()

    def bulk(ref, sem):
        part = ref.at[pl.ds(0, all_but_me)]
        return pltpu.make_async_copy(part, part, sem)

    bulk(messages, m_recv).wait()
    over = make_lists(sh, x, z, j, pw, pc, messages[:, 0, :], tabv)
    table = pltpu.make_async_copy(tabv, tab, t_copy)
    table.start()
    table.wait()

    def entry(ref, row, lane):
        return ref[jnp.minimum(jnp.maximum(tab[row, lane], 0), ref.shape[0] - 1)]

    kinds = (
        (store_h, pack_hz, pack_h, land_h, CAP_H_Z, CAP_H, near_h),
        (store_p, pack_pz, pack_p, land_p, CAP_P_Z, CAP_P, near_p),
    )

    def zone(which, layer):
        store, cap = kinds[which][0], kinds[which][4]
        return store.at[pl.ds(sh.team * slots + layer * cap, cap)]

    def across(which, dz):
        pack = kinds[which][1]
        zd = (z + dz) % sh.outer
        return remote(
            pack.at[dz - 1], zone(which, z), z_send.at[which, dz], z_recv.at[which, z],
            (zd * sh.inner + x, j),
        )

    def across_in(which, dz):
        pack = kinds[which][1]
        zs = (z + dz) % sh.outer
        return remote(
            pack.at[dz - 1], zone(which, zs), z_send.at[which, dz], z_recv.at[which, zs],
            (zs * sh.inner + x, j),
        )

    for which in range(2):
        store, pack, _, _, cap, _, near = kinds[which]
        for d in range(1, sh.team):
            strips_in(d, which).wait_recv()
        for dz in range(1, sh.outer):
            for k in range(cap):
                pack[dz - 1, k] = entry(near, dz - 1, 64 * which + k)
        for dz in range(1, sh.outer):
            across(which, dz).start()
        store[0 : sh.team * slots] = near[...]

    for dc in range(1, sh.chips):
        p_in(other(dc)[1]).wait_recv()
        p_forward(dc).start()

    def part(which, d):
        pack, land = kinds[which][2], kinds[which][3]
        _, dev = member(d)
        return remote(
            pack.at[d - 1], land.at[:, in_strip(team), :], t_send.at[which, d], t_recv.at[which, team], dev
        )

    def part_in(which, d):
        pack, land = kinds[which][2], kinds[which][3]
        q, dev = member(d)
        return remote(
            pack.at[d - 1], land.at[:, in_strip(q), :], t_send.at[which, d], t_recv.at[which, q], dev
        )

    for which in range(2):
        store, _, pack, land, _, cap, _ = kinds[which]
        for dz in range(1, sh.outer):
            across_in(which, dz).wait_recv()

        @pl.loop(1, sh.team)
        def _(d):
            q, _ = member(d)
            for k in range(cap):
                lane = 64 * which + (q % sh.group) * LIST + k
                pack[d - 1, k] = entry(store, sh.row_n + q // sh.group, lane)

        for d in range(1, sh.team):
            part(which, d).start()
        for k in range(cap):
            land[k, in_strip(team), :] = entry(store, sh.row_n + x, 64 * which + a * LIST + k)

    def multiply(step, left, right, terms, cap):
        row = sh.row_m + step
        acc = None
        for k in range(cap):
            d = jnp.dot(entry(left, row, k), entry(right, row, 16 + k), preferred_element_type=F32)
            acc = d if acc is None else d + acc * tab[row, 32 + k].astype(F32)
            terms[k] = acc
        terms[cap] = jnp.zeros((size, size), F32)

    p_in(mate[1]).wait_recv()
    for dc in range(1, sh.chips):
        p_in(other(dc)[0] * 2 + 1 - core).wait_recv()
    for d in range(1, sh.team):
        part_in(0, d).wait_recv()
    multiply(0, prow, land_h, terms_1, CAP_1)
    trace = jnp.zeros((size, size), F32)
    for s in range(slots):
        value = entry(terms_1, sh.row_m, 48 + s)
        trace = trace + value * jnp.where(pw[s, 0] == pw[s, 1], 1.0, 0.0)
        rounded = value.astype(BF16)
        fstore[s] = rounded
        ph_out[s] = rounded

    def f_block(col):
        return fstore.at[pl.ds(sh.others + col * CAP_F, CAP_F)]

    def f_out(dc):
        return remote(pack_f.at[dc - 1], f_block(j), f_send.at[dc], f_recv.at[j], (i, other(dc)[1]))

    def f_in(dc):
        return remote(pack_f.at[dc - 1], f_block(other(dc)[1]), f_send.at[dc], f_recv.at[other(dc)[1]], (i, other(dc)[1]))

    def f_forward(dc):
        col = other(dc)[1]
        return remote(f_block(col), f_block(col), f_fwd.at[dc], f_recv.at[col], mate)

    def f_forward_in(dc):
        col = other(dc)[0] * 2 + 1 - core
        return remote(f_block(col), f_block(col), f_fwd.at[dc], f_recv.at[col], mate)

    own_f = remote(
        ph_out, fstore.at[pl.ds(sh.partner, slots)], f_send.at[0], f_recv.at[sh.cols], mate
    )
    for dc in range(1, sh.chips):
        for k in range(CAP_F):
            pack_f[dc - 1, k] = entry(ph_out, sh.row_f + dc - 1, k)
    for dc in range(1, sh.chips):
        f_out(dc).start()
    own_f.start()

    diagonal = iota((size, size), 0) == iota((size, size), 1)
    emsg[0, 0] = jnp.sum(jnp.where(diagonal, trace, 0.0), axis=0, keepdims=True)
    emsg[0, 1] = jnp.sum(over, axis=1, keepdims=True) + jnp.zeros((1, 128), F32)
    emsgs[me] = emsg[0]

    def tell_energy(d):
        return remote(emsg.at[pl.ds(0, 1)], emsgs.at[pl.ds(me, 1)], e_send, e_recv, device(d))

    @pl.loop(1, sh.devices)
    def _(d):
        tell_energy(d).start()

    for dc in range(1, sh.chips):
        f_in(dc).wait_recv()
        f_forward(dc).start()
    for d in range(1, sh.team):
        part_in(1, d).wait_recv()
    own_f.wait_recv()
    for dc in range(1, sh.chips):
        f_forward_in(dc).wait_recv()
    multiply(1, fstore, land_p, terms_2, CAP_2)
    for s in range(slots):
        php_out[s] = entry(terms_2, sh.row_m + 1, 48 + s).astype(BF16)

    bulk(emsgs, e_recv).wait()
    for line in range(2):
        total = jnp.sum(emsgs[:, line], axis=0)
        e_out[line : line + 1, :] = jnp.sum(total, axis=1, keepdims=True) + jnp.zeros((1, 128), F32)

    bulk(messages, m_send).wait()
    bulk(emsgs, e_send).wait()
    for which in range(2):
        for d in range(1, sh.team):
            strips(d, which).wait_send()
            part(which, d).wait_send()
        for dz in range(1, sh.outer):
            across(which, dz).wait_send()
    for dc in range(sh.chips):
        p_out(dc).wait_send()
    own_f.wait_send()
    for dc in range(1, sh.chips):
        p_forward(dc).wait_send()
        f_out(dc).wait_send()
        f_forward(dc).wait_send()


def sparse_path(sh, p_values, p_where, p_count, h_values, h_where, h_count):
    slots, size, strip = sh.slots, sh.size, sh.strip
    block, piece = (size, size), (strip, size)
    bf = lambda *shape: pltpu.VMEM(shape, BF16)
    f32 = lambda *shape: pltpu.VMEM(shape, F32)
    dma = pltpu.SemaphoreType.DMA
    near = sh.team * slots
    away = max(sh.outer - 1, 1)
    chips = max(sh.chips - 1, 1)
    tile = jax.ShapeDtypeStruct((slots,) + block, BF16)
    return pl.pallas_call(
        functools.partial(sparse_products, sh),
        out_shape=[tile, tile, jax.ShapeDtypeStruct((2, 128), F32)],
        in_specs=[VMEM, VMEM, SMEM, SMEM, SMEM, SMEM],
        out_specs=[VMEM, VMEM, VMEM],
        scratch_shapes=[
            f32(1, 1, 128),
            f32(sh.devices, 1, 128),
            bf(near, *piece),
            bf(near, *piece),
            bf(near + sh.outer * CAP_H_Z, *piece),
            bf(near + sh.outer * CAP_P_Z, *piece),
            bf(sh.cols * slots, *block),
            bf(away, CAP_H_Z, *piece),
            bf(away, CAP_P_Z, *piece),
            bf(sh.team, CAP_H, *piece),
            bf(sh.team, CAP_P, *piece),
            bf(CAP_H, *block),
            bf(CAP_P, *block),
            f32(CAP_1 + 1, *block),
            f32(CAP_2 + 1, *block),
            bf(sh.others + sh.cols * CAP_F, *block),
            bf(chips, CAP_F, *block),
            pltpu.VMEM((sh.table, 128), I32),
            pltpu.SMEM((sh.table, 128), I32),
            f32(1, 2, 1, 128),
            f32(sh.devices, 2, 1, 128),
            f32(8, 128),
            dma, dma,
            dma((2, sh.team)), dma((2, sh.team)),
            dma((sh.chips,)), dma((sh.chips,)), dma((sh.cols,)),
            dma((2, sh.outer)), dma((2, sh.outer)),
            dma((2, sh.team)), dma((2, sh.team)),
            dma((sh.chips,)), dma((sh.chips,)), dma((sh.cols + 1,)),
            dma, dma, dma,
        ],
        compiler_params=pltpu.CompilerParams(collective_id=2, has_side_effects=True),
        name="sparse_products",
    )(p_values, h_values, p_where, p_count, h_where, h_count)


def per_device(rows, cols, *args):
    slots, size, _ = args[0].shape
    sh = Shape(rows, cols, slots, size)
    if not sh.fits():
        return dense_path(rows, cols, *args)
    ph, php, summary = sparse_path(sh, *args)
    return lax.cond(
        summary[1, 0] > 0.0,
        lambda: dense_path(rows, cols, *args),
        lambda: (ph, php, summary[0, 0]),
    )


def solution(mesh):
    placed = (
        P("row", "col", None),
        P("row", "col"),
        P("row", "col"),
        P("row", "col", None),
        P("row", "col"),
        P("row", "col"),
    )
    return jax.shard_map(
        functools.partial(per_device, mesh.shape["row"], mesh.shape["col"]),
        mesh=mesh,
        in_specs=placed,
        out_specs=(P("row", "col", None), P("row", "col", None), P()),
        check_vma=False,
    )
```

```python
import functools

import jax
import jax.numpy as jnp
from jax import lax
from jax.experimental import pallas as pl
from jax.experimental.pallas import tpu as pltpu
from jax.sharding import PartitionSpec as P

TILE = 8
CHUNKS = 6
IN_FLIGHT = 16
MESH = pl.DeviceIdType.MESH
ANY = pl.BlockSpec(memory_space=pl.ANY)
VMEM = pl.BlockSpec(memory_space=pltpu.VMEM)
SMEM = pl.BlockSpec(memory_space=pltpu.SMEM)


def at_row(r):
    return (r, lax.axis_index("col"))


def at_col(c):
    return (lax.axis_index("row"), c)


def remote(src, dst, send_sem, recv_sem, device):
    return pltpu.make_async_remote_copy(
        src_ref=src,
        dst_ref=dst,
        send_sem=send_sem,
        recv_sem=recv_sem,
        device_id=device,
        device_id_type=MESH,
    )


def greet(rows, cols):
    me_row, me_col = lax.axis_index("row"), lax.axis_index("col")
    barrier = pltpu.get_barrier_semaphore()
    for d in range(1, rows):
        pl.semaphore_signal(
            barrier, inc=1, device_id=at_row((me_row + d) % rows), device_id_type=MESH
        )
    for d in range(1, cols):
        pl.semaphore_signal(
            barrier, inc=1, device_id=at_col((me_col + d) % cols), device_id_type=MESH
        )
    pl.semaphore_wait(barrier, rows + cols - 2)


class ColumnGather:
    def __init__(self, rows, own, land, out, up_send, down_send, x_send, recv, local):
        self.own, self.land, self.out = own, land, out
        self.up_send, self.down_send, self.x_send = up_send, down_send, x_send
        self.recv, self.local = recv, local
        self.inner = 2 if rows % 2 == 0 else 1
        self.outer = rows // self.inner
        self.chunks = recv.shape[1]
        self.size = own.shape[0] // self.chunks
        self.me = lax.axis_index("row")
        self.x, self.z = self.me % self.inner, self.me // self.inner
        self.cross_first = 1 if self.inner == 2 and self.chunks > 1 else 0

    def later(self, ch):
        return (ch + self.cross_first) % self.chunks

    def row(self, z, line):
        return z * self.inner + (self.x if line == 0 else self.inner - 1 - self.x)

    def part(self, ch):
        return pl.ds(ch * self.size, self.size)

    def copy(self, r, ch, own, way):
        sems, target = {
            "up": (self.up_send, self.me + self.inner),
            "down": (self.down_send, self.me - self.inner),
            "x": (self.x_send, self.row(self.z, 1)),
        }[way]
        part = self.part(ch)
        src = self.own.at[part] if own else self.land.at[r, part]
        return remote(src, self.land.at[r, part], sems.at[r, ch], self.recv.at[r, ch], at_row(target))

    def keep(self, r, ch):
        part = self.part(ch)
        return pltpu.make_async_copy(self.land.at[r, part], self.out.at[r, part], self.local.at[r, ch])

    def along(self, r, ch, own, act):
        @pl.when(self.z < self.outer - 1)
        def _():
            act(self.copy(r, ch, own, "up"))

        @pl.when(self.z > 0)
        def _():
            act(self.copy(r, ch, own, "down"))

    def arrive(self, r, ch):
        self.copy(r, ch, False, "x").wait_recv()
        self.keep(r, ch).start()

    def start(self):
        for ch in range(self.chunks):
            if self.inner == 2:
                self.copy(self.me, ch, True, "x").start()
            self.along(self.me, self.later(ch), True, lambda copy: copy.start())
        if self.cross_first:
            r = self.row(self.z, 1)
            self.arrive(r, 0)
            self.along(r, 0, False, lambda copy: copy.start())

    def pieces(self):
        lines = [(self.later(ch), 0) for ch in range(self.chunks)]
        return lines + [(0, 1)] * self.cross_first

    def relayed(self, d, side, ch, line, act):
        z = self.z - d if side == 0 else self.z + d
        there = self.z >= d if side == 0 else self.z + d < self.outer
        r = self.row(z, line)

        @pl.when(there)
        def _():
            if act == "start":
                self.arrive(r, ch)
            on = self.z < self.outer - 1 if side == 0 else self.z > 0

            @pl.when(on)
            def _():
                copy = self.copy(r, ch, False, "up" if side == 0 else "down")
                copy.start() if act == "start" else copy.wait_send()

            if self.inner == 2 and ch >= self.cross_first:
                copy = self.copy(r, ch, False, "x")
                copy.start() if act == "start" else copy.wait_send()

    def relay(self, d):
        for ch, line in self.pieces():
            for side in range(2):
                self.relayed(d, side, ch, line, "start")

    def finish(self):
        if self.inner == 2:
            for ch in range(self.cross_first, self.chunks):
                self.arrive(self.row(self.z, 1), ch)
            for d in range(1, self.outer):
                for side in range(2):
                    z = self.z - d if side == 0 else self.z + d
                    there = self.z >= d if side == 0 else self.z + d < self.outer

                    @pl.when(there)
                    def _():
                        for ch in range(self.cross_first, self.chunks):
                            self.arrive(self.row(z, 1), ch)
        for ch in range(self.chunks):
            if self.inner == 2:
                self.copy(self.me, ch, True, "x").wait_send()
            self.along(self.me, ch, True, lambda copy: copy.wait_send())
        if self.cross_first:
            self.along(self.row(self.z, 1), 0, False, lambda copy: copy.wait_send())
        for d in range(1, self.outer):
            for ch, line in self.pieces():
                for side in range(2):
                    self.relayed(d, side, ch, line, "wait")
        for r in range(self.inner * self.outer):
            @pl.when(r != self.me)
            def _():
                for ch in range(self.chunks):
                    self.keep(r, ch).wait()


def col_copies(cols, own, out, send, recv):
    me = lax.axis_index("col")
    made = []
    for d in range(1, cols):
        made.append(
            remote(own, out.at[me], send.at[d], recv.at[d], at_col((me + d) % cols))
        )
    return made


def row_copies(rows, own, out, send, recv):
    me = lax.axis_index("row")
    made = []
    for d in range(1, rows):
        made.append(
            remote(own, out.at[me], send.at[d], recv.at[d], at_row((me + d) % rows))
        )
    return made


def first_gather(
    rows, cols, p_ref, h_ref, meta_ref, prow, hcol, prow_meta, col_meta,
    land, up_send, down_send, x_send, recv, out_sems,
    p_send, p_recv, mc_send, mc_recv, mr_send, mr_recv, local,
):
    me_row, me_col = lax.axis_index("row"), lax.axis_index("col")
    keep = [
        pltpu.make_async_copy(h_ref, hcol.at[me_row], local.at[0]),
        pltpu.make_async_copy(p_ref, prow.at[me_col], local.at[1]),
        pltpu.make_async_copy(meta_ref, prow_meta.at[me_col], local.at[2]),
        pltpu.make_async_copy(meta_ref, col_meta.at[me_row], local.at[3]),
    ]
    greet(rows, cols)
    gather = ColumnGather(
        rows, h_ref, land, hcol, up_send, down_send, x_send, recv, out_sems
    )
    across = (
        col_copies(cols, p_ref, prow, p_send, p_recv)
        + col_copies(cols, meta_ref, prow_meta, mc_send, mc_recv)
        + row_copies(rows, meta_ref, col_meta, mr_send, mr_recv)
    )
    for copy in across + keep:
        copy.start()
    gather.start()
    for d in range(1, gather.outer):
        gather.relay(d)
    gather.finish()
    for copy in across + keep:
        copy.wait()


def second_gather(
    rows, cols, p_ref, f_ref, e_ref, frow, pcol, e_out,
    e_cols, e_rows, e_sum,
    land, up_send, down_send, x_send, recv, out_sems,
    p_send, p_recv, ec_send, ec_recv, er_send, er_recv, local,
):
    me_row, me_col = lax.axis_index("row"), lax.axis_index("col")
    keep = [
        pltpu.make_async_copy(p_ref, pcol.at[me_row], local.at[0]),
        pltpu.make_async_copy(f_ref, frow.at[me_col], local.at[1]),
    ]
    greet(rows, cols)
    energies = col_copies(cols, e_ref, e_cols, ec_send, ec_recv)
    for copy in energies:
        copy.start()
    gather = ColumnGather(
        rows, p_ref, land, pcol, up_send, down_send, x_send, recv, out_sems
    )
    across = col_copies(cols, f_ref, frow, p_send, p_recv)
    for copy in across + keep:
        copy.start()
    gather.start()
    e_cols[me_col] = e_ref[...]
    for copy in energies:
        copy.wait()
    total = e_cols[0]
    for c in range(1, cols):
        total = total + e_cols[c]
    e_sum[...] = total
    e_rows[me_row] = total
    if gather.outer > 1:
        gather.relay(1)
    sums = row_copies(rows, e_sum, e_rows, er_send, er_recv)
    for copy in sums:
        copy.start()
    for d in range(2, gather.outer):
        gather.relay(d)
    for copy in sums:
        copy.wait()
    total = e_rows[0]
    for r in range(1, rows):
        total = total + e_rows[r]
    e_out[...] = total
    gather.finish()
    for copy in across + keep:
        copy.wait()


def block_products(
    rows, cols, right_lane, with_trace, lmeta, rmeta, left, right, *rest
):
    if with_trace:
        out, e_out = rest[:2]
    else:
        e_in, out, e_out = rest[:3]
    acc, lbuf, rbuf, head, nxt, inner, mask, table, ml, mr, ms, sems = rest[-12:]
    slots = out.shape[0]
    i, j = lax.axis_index("row"), lax.axis_index("col")
    nblk = rows * TILE
    tile_cols = nblk // cols
    words = -(-nblk // 32)
    count_lane = 4 * slots
    acc[...] = jnp.zeros_like(acc)

    for t in range(TILE + 1):
        head[t] = -1

    for t in range(tile_cols * words + 1):
        mask[t] = 0

    @pl.loop(0, cols)
    def _(c):
        live = lmeta[c, 0, count_lane]
        for s in range(slots):
            row = jnp.where(s < live, lmeta[c, 0, s] - i * TILE, TILE)
            idx = c * slots + s
            inner[idx] = lmeta[c, 0, slots + s]
            nxt[idx] = head[row]
            head[row] = idx

    @pl.loop(0, rows)
    def _(r):
        live = rmeta[r, 0, count_lane + (1 if right_lane else 0)]
        for s in range(slots):
            k = rmeta[r, 0, right_lane + s]
            col = rmeta[r, 0, right_lane + slots + s] - j * tile_cols
            word = jnp.where(s < live, col * words + (k >> 5), tile_cols * words)
            mask[word] = mask[word] | (jnp.int32(1) << (k & 31))
            table[jnp.where(s < live, k * tile_cols + col, nblk * tile_cols)] = r * slots + s

    def find_slot(s, n):
        row = lmeta[j, 0, s] - i * TILE
        col = lmeta[j, 0, slots + s] - j * tile_cols

        def more(state):
            return state[0] >= 0

        def step(state):
            at, n = state
            k = inner[at]
            ml[n] = at
            mr[n] = table[k * tile_cols + col]
            ms[n] = s
            return nxt[at], n + ((mask[col * words + (k >> 5)] >> (k & 31)) & 1)

        return lax.while_loop(more, step, (head[row], n))[1]

    own_count = lmeta[j, 0, count_lane]
    found = lax.fori_loop(0, own_count, find_slot, jnp.int32(0))

    def fetch(base, m):
        a, b = ml[base + m], mr[base + m]
        return (
            pltpu.make_async_copy(left.at[a], lbuf.at[m], sems.at[0, m]),
            pltpu.make_async_copy(right.at[b], rbuf.at[m], sems.at[1, m]),
        )

    @pl.loop(0, (found + IN_FLIGHT - 1) // IN_FLIGHT)
    def _(chunk):
        base = chunk * IN_FLIGHT
        size = jnp.minimum(found - base, IN_FLIGHT)

        @pl.loop(0, size)
        def _(m):
            for copy in fetch(base, m):
                copy.start()

        @pl.loop(0, size)
        def _(m):
            for copy in fetch(base, m):
                copy.wait()
            s = ms[base + m]
            acc[s] += jnp.dot(lbuf[m], rbuf[m], preferred_element_type=jnp.float32)

    out[...] = acc[...].astype(out.dtype)
    if with_trace:
        size = acc.shape[1]
        e_out[...] = jnp.zeros_like(e_out)
        diagonal = lax.broadcasted_iota(jnp.int32, (size, size), 0) == lax.broadcasted_iota(
            jnp.int32, (size, size), 1
        )

        @pl.loop(0, own_count)
        def _(s):
            @pl.when(lmeta[j, 0, s] == lmeta[j, 0, slots + s])
            def _():
                e_out[...] += jnp.sum(jnp.where(diagonal, acc[s], 0.0))
    else:
        e_out[0, 0] = e_in[0, 0]


def dense_path(rows, cols, p_values, p_where, p_count, h_values, h_where, h_count):
    slots, size, _ = p_values.shape
    dtype = p_values.dtype
    nblk = rows * TILE
    tile_cols = nblk // cols
    words = -(-nblk // 32)
    meta = jnp.concatenate(
        [p_where[:, 0], p_where[:, 1], h_where[:, 0], h_where[:, 1], p_count[0], h_count[0]]
    )
    meta = jnp.broadcast_to(jnp.pad(meta, (0, 128 - meta.shape[0]))[None, :], (8, 128))
    dma = pltpu.SemaphoreType.DMA
    chunks = CHUNKS if slots % CHUNKS == 0 else 1
    chunk_sems = [pltpu.VMEM((rows, slots, size, size), dtype)] + [dma((rows, chunks))] * 5
    col_sems = [dma((cols,)), dma((cols,))]
    row_sems = [dma((rows,)), dma((rows,))]
    tile = (slots, size, size)
    prow, hcol, prow_meta, col_meta = pl.pallas_call(
        functools.partial(first_gather, rows, cols),
        out_shape=[
            jax.ShapeDtypeStruct((cols,) + tile, dtype),
            jax.ShapeDtypeStruct((rows,) + tile, dtype),
            jax.ShapeDtypeStruct((cols, 8, 128), jnp.int32),
            jax.ShapeDtypeStruct((rows, 8, 128), jnp.int32),
        ],
        in_specs=[VMEM] * 3,
        out_specs=[ANY] * 4,
        scratch_shapes=chunk_sems + col_sems + col_sems + row_sems + [dma((4,))],
        compiler_params=pltpu.CompilerParams(collective_id=0, has_side_effects=True),
        name="first_gather",
    )(p_values, h_values, meta)

    def products(right_lane, with_trace, lmeta, rmeta, left, right, *more):
        smem = lambda n: pltpu.SMEM((n,), jnp.int32)
        most = slots * nblk + 1
        return pl.pallas_call(
            functools.partial(block_products, rows, cols, right_lane, with_trace),
            out_shape=[
                jax.ShapeDtypeStruct(tile, dtype),
                jax.ShapeDtypeStruct((8, 128) if with_trace else (1, 1), jnp.float32),
            ],
            in_specs=[SMEM, SMEM, ANY, ANY] + [SMEM] * len(more),
            out_specs=[VMEM, VMEM if with_trace else SMEM],
            scratch_shapes=[
                pltpu.VMEM(tile, jnp.float32),
                pltpu.VMEM((IN_FLIGHT, size, size), dtype),
                pltpu.VMEM((IN_FLIGHT, size, size), dtype),
                smem(TILE + 1),
                smem(cols * slots),
                smem(cols * slots),
                smem(tile_cols * words + 1),
                smem(nblk * tile_cols + 1),
                smem(most),
                smem(most),
                smem(most),
                dma((2, IN_FLIGHT)),
            ],
            name="products",
        )(
            lmeta,
            rmeta,
            left.reshape((cols * slots, size, size)),
            right.reshape((rows * slots, size, size)),
            *more,
        )

    ph_values, part = products(2 * slots, True, prow_meta, col_meta, prow, hcol)
    frow, pcol, energy = pl.pallas_call(
        functools.partial(second_gather, rows, cols),
        out_shape=[
            jax.ShapeDtypeStruct((cols,) + tile, dtype),
            jax.ShapeDtypeStruct((rows,) + tile, dtype),
            jax.ShapeDtypeStruct((8, 128), jnp.float32),
        ],
        in_specs=[VMEM] * 3,
        out_specs=[ANY, ANY, VMEM],
        scratch_shapes=[
            pltpu.VMEM((cols, 8, 128), jnp.float32),
            pltpu.VMEM((rows, 8, 128), jnp.float32),
            pltpu.VMEM((8, 128), jnp.float32),
        ]
        + chunk_sems + col_sems + col_sems + row_sems + [dma((2,))],
        compiler_params=pltpu.CompilerParams(collective_id=1, has_side_effects=True),
        name="second_gather",
    )(p_values, ph_values, part)
    php_values, energy = products(0, False, prow_meta, col_meta, frow, pcol, energy)
    return (ph_values, php_values, energy[0, 0])


CAP_H_Z, CAP_P_Z = 17, 12
CAP_H, CAP_P = 14, 9
CAP_R, CAP_V = 7, 7
CAP_1, CAP_2 = 18, 12
LIST, LIST_Z, LIST_1, EIGHT = 16, 24, 24, 8
F32, BF16, I32 = jnp.float32, jnp.bfloat16, jnp.int32


def log2(n):
    return n.bit_length() - 1


def power(n):
    return n > 0 and n & (n - 1) == 0


class Shape:
    def __init__(self, rows, cols, slots, size):
        self.rows, self.cols, self.slots, self.size = rows, cols, slots, size
        self.devices = rows * cols
        self.nblk = rows * TILE
        self.inner = 2 if rows % 2 == 0 else 1
        self.outer = rows // self.inner
        self.layer = self.inner * TILE
        self.team = self.inner * cols
        self.strip = size // self.team
        self.width = self.nblk // cols
        self.chips = cols // 2
        self.others = 2 * slots

    def fits(self):
        return (
            power(self.rows)
            and power(self.cols)
            and self.cols >= 2
            and self.outer >= 2
            and self.nblk <= 64
            and self.width * TILE <= 128
            and self.slots <= 15
            and self.strip % 16 == 0
            and self.team * LIST <= 128
            and (self.outer - 1) * LIST_Z <= 128
            and (self.chips - 1) * EIGHT <= 128
        )


def mm(a, b):
    return lax.dot_general(a.astype(BF16), b.astype(BF16), (((1,), (0,)), ((), ())), preferred_element_type=F32)


def mt(a, b):
    return lax.dot_general(a.astype(BF16), b.astype(BF16), (((1,), (1,)), ((), ())), preferred_element_type=F32)


def tm(a, b):
    return lax.dot_general(a.astype(BF16), b.astype(BF16), (((0,), (0,)), ((), ())), preferred_element_type=F32)


def ones(cond):
    return jnp.where(cond, 1.0, 0.0).astype(F32)


def iota(shape, dim):
    return lax.broadcasted_iota(I32, shape, dim)


def block_index(shape, dim, size):
    return iota(shape, dim) // size


def total_over(counts, starts, cap):
    over = ones(starts + counts > cap + 0.5)
    return jnp.sum(jnp.sum(over, axis=0, keepdims=True), axis=1, keepdims=True)


def stack(parts):
    return jnp.concatenate(parts, axis=0)


class Lists:
    def __init__(self, sh, x, z, j, message):
        self.sh, self.x, self.z, self.j = sh, x, z, j
        n, width, layer = sh.nblk, sh.width, sh.layer
        lw = log2(width)
        r, l = iota((n, n), 0), iota((n, n), 1)
        a0, d0 = iota((sh.cols * n, sh.devices), 0), iota((sh.cols * n, sh.devices), 1)
        spread = mm(ones(d0 == ((a0 & (n - 1)) >> 3) * sh.cols + (a0 >> log2(n))), message)
        a1, l1 = iota((sh.cols * n, 128), 0), iota((sh.cols * n, 128), 1)
        spread = jnp.where((l1 >> lw) == (a1 & 7), spread, 0.0)
        l2, m2 = iota((128, n), 0), iota((128, n), 1)
        spread = mm(spread, ones((l2 & (width - 1)) == (m2 & (width - 1))))
        both = jnp.zeros((n, n), F32)
        for c in range(sh.cols):
            both = both + jnp.where((l >> lw) == c, spread[c * n : (c + 1) * n], 0.0)
        hs = jnp.floor(both * (1.0 / 16.0))
        ps = both - 16.0 * hs
        self.pm, self.hm = ones(ps > 0.5), ones(hs > 0.5)
        self.fm = self.pm * ones(mm(self.pm, self.hm) > 0.5)
        self.up, self.low = ones(r < l), ones(l < r)
        self.low_layer = ones((l < r) & (l // layer == r // layer))
        self.full = jnp.ones((n, n), F32)
        self.r, self.l, self.lane_tile = r, l, l >> lw
        team = ((r >> 3) & (sh.inner - 1)) * sh.cols + self.lane_tile
        at = (team * sh.slots).astype(F32)
        self.near = {"H": at + hs - 1.0, "P": at + ps - 1.0}
        s0, s1 = iota((layer, n), 0), iota((layer, n), 1)
        self.sel = ones(s1 == z * layer + s0)
        self.row_i, self.row_tile = s0, (s1 >> lw)
        self.p_layer, self.f_layer = mm(self.sel, self.pm), mm(self.sel, self.fm)
        self.slot_layer = mm(self.sel, ps) - 1.0

    def enumerate(self, v, count, lane_pos=None):
        k, n = v.shape
        counts = mt(jnp.ones((count, n), F32), v)
        a, b = iota((k, k), 0), iota((k, k), 1)
        starts = mm(counts, ones(a < b))
        at = iota((count, k), 0).astype(F32)
        rows = ones((starts <= at) & (at < starts + counts))
        local = mm(rows * (at - starts + 1.0), jnp.ones((k, n), F32))
        if lane_pos is None:
            lane_pos = mm(v, self.up)
        found = mm(rows, v * (lane_pos + 1.0))
        lanes = ones((found == local) & (local > 0.5))
        return rows, lanes, counts, starts, lane_pos

    def position(self, v, low):
        return mm(v, self.up) + mm(low, mm(v, self.full))

    def across(self, tab):
        sh, z, layer, n = self.sh, self.z, self.sh.layer, self.sh.nblk
        p_s, f_s = mt(self.sel, self.pm), mt(self.sel, self.fm)
        i_layer = self.l[0:layer] // layer
        lhs, live, pay = [], [], []
        for kind, left, right in (("H", p_s, self.hm), ("P", f_s, self.pm)):
            live_kind, pay_kind = mm(self.sel, right), mm(self.sel, self.near[kind])
            for dz in range(1, sh.outer):
                lhs.append(left * ones(i_layer == (z + dz) % sh.outer))
                live.append(live_kind)
                pay.append(pay_kind)
        v = ones(mm(stack(lhs), self.pm) > 0.5) * stack(live)
        k = v.shape[0]
        lists = 2 * (sh.outer - 1)
        a, b = iota((k, k), 0), iota((k, k), 1)
        counts = mt(jnp.ones((EIGHT, n), F32), v)
        starts = mm(counts, ones((a < b) & (a // layer == b // layer)))
        t0 = iota((lists * LIST_Z, k), 0)
        at = (t0 % LIST_Z).astype(F32)
        rows = ones(
            (starts[0:1] <= at)
            & (at < starts[0:1] + counts[0:1])
            & (t0 // LIST_Z == block_index((lists * LIST_Z, k), 1, layer))
        )
        local = mm(rows * (at - starts[0:1] + 1.0), jnp.ones((k, n), F32))
        found = mm(rows, v * (mm(v, self.up) + 1.0))
        picked = jnp.where((found == local) & (local > 0.5), mm(rows, stack(pay)), 0.0)
        half = (sh.outer - 1) * LIST_Z
        for which in range(2):
            line = mt(jnp.ones((EIGHT, n), F32), picked[which * half : (which + 1) * half])
            tab[which : which + 1, 0:half] = line[0:1].astype(I32)
        lane_h = block_index((EIGHT, k), 1, layer) < sh.outer - 1
        cap = jnp.where(lane_h, 1.0 * CAP_H_Z, 1.0 * CAP_P_Z)
        return total_over(counts - cap, starts, 0.0)

    def row_lists(self, tab):
        sh, x, j, layer, n = self.sh, self.x, self.j, self.sh.layer, self.sh.nblk
        tiles = [ones(self.row_tile == c) for c in range(sh.cols)]
        wide = stack([self.p_layer * t for t in tiles])
        passed = ones(mt(wide, self.pm) > 0.5) * stack([self.f_layer] * sh.cols)
        own = wide
        self.outputs = jnp.maximum(own, passed)
        self.remote_f = passed * (1.0 - ones(stack([t for t in tiles]) > 0.5))
        reads = ones(mt(self.outputs, self.hm) > 0.5) * stack([self.p_layer] * sh.cols)
        mine = ones((self.row_i >> 3) == x)
        chip = j // 2
        low = ones(iota((layer, layer), 1) < iota((layer, layer), 0))
        seg_tri = ones((self.lane_tile == (self.r >> log2(sh.width))) & (self.r < self.l))
        seg_full = ones(self.lane_tile == (self.r >> log2(sh.width)))
        over = jnp.zeros((1, 1), F32)
        for dc in range(sh.chips):
            c = (chip + dc) % sh.chips
            v = jnp.zeros((layer, n), F32)
            for k in range(sh.cols):
                v = jnp.maximum(v, reads[k * layer : (k + 1) * layer] * jnp.where(k // 2 == c, 1.0, 0.0))
            v = v * mine
            if dc == 0:
                pos = mm(v, seg_tri) + mm(low, mm(v, seg_full))
                pos = jnp.minimum(pos, CAP_R - 1.0)
                continue
            v = v * ones(self.row_tile == j)
            rows, lanes, counts, starts, _ = self.enumerate(v, EIGHT)
            line = mt(jnp.ones((EIGHT, n), F32), lanes * mm(rows, self.slot_layer))
            tab[0:1, (dc - 1) * EIGHT : dc * EIGHT] = line[0:1].astype(I32)
            over = over + total_over(counts, starts, CAP_R)
        self.left_1 = jnp.where(
            self.row_tile == j,
            self.slot_layer,
            jnp.where(
                self.row_tile // 2 == chip,
                sh.slots + self.slot_layer,
                sh.others + self.row_tile.astype(F32) * CAP_R + pos,
            ),
        )
        return over

    def team_lists(self, tab):
        sh, x, z, j, layer, n = self.sh, self.x, self.z, self.j, self.sh.layer, self.sh.nblk
        a, b = iota((layer, layer), 0), iota((layer, layer), 1)
        eye = ones(a == b)
        turned = {"H": tm(self.p_layer, eye), "P": tm(self.f_layer, eye)}
        lane_x = iota((n, layer), 1) >> 3
        live = {"H": self.hm, "P": self.pm}
        k_layer = self.r // layer
        over = jnp.zeros((1, 1), F32)
        self.pos = {}
        for which, (kind, cap_z, cap) in enumerate((("H", CAP_H_Z, CAP_H), ("P", CAP_P_Z, CAP_P))):
            pos_z = self.position(ones(mm(turned[kind], self.p_layer) > 0.5) * live[kind], self.low_layer)
            far = (sh.team * sh.slots + k_layer * cap_z).astype(F32) + jnp.minimum(pos_z, cap_z - 1.0)
            payload = jnp.where(k_layer == z, self.near[kind], far)
            by_x = stack([turned[kind] * ones(lane_x == xd) for xd in range(sh.inner)])
            needs = []
            if kind == "H":
                made = [
                    ones(mm(by_x, self.outputs[c * layer : (c + 1) * layer]) > 0.5) for c in range(sh.cols)
                ]
            else:
                one = ones(mm(by_x, self.p_layer) > 0.5)
                made = [one * ones((iota((sh.inner * n, n), 1) >> log2(sh.width)) == c) for c in range(sh.cols)]
            for xd in range(sh.inner):
                for c in range(sh.cols):
                    needs.append(made[c][xd * n : (xd + 1) * n] * live[kind])
            all_needs = stack(needs)
            lane_pos = mm(all_needs, self.up)
            counts = stack([mt(jnp.ones((LIST, n), F32), v) for v in needs])
            starts = mm(counts, self.up)
            over = over + total_over(counts, starts, cap)
            at = (iota((sh.team * LIST, n), 0) % LIST).astype(F32)
            rows = ones((starts <= at) & (at < starts + counts))
            local = mm(rows * (at - starts + 1.0), self.full)
            marked = all_needs * (lane_pos + 1.0)
            found = stack(
                [
                    mm(rows[t * LIST : (t + 1) * LIST], marked[t * n : (t + 1) * n])
                    for t in range(sh.team)
                ]
            )
            picked = jnp.where((found == local) & (local > 0.5), mm(rows, payload), 0.0)
            line = mt(jnp.ones((EIGHT, n), F32), picked)
            tab[which : which + 1, 0 : sh.team * LIST] = line[0:1].astype(I32)
            me = x * sh.cols + j
            mine = jnp.zeros((n, n), F32)
            for t in range(sh.team):
                mine = mine + needs[t] * jnp.where(me == t, 1.0, 0.0)
            self.pos[kind] = jnp.minimum(self.position(mine, self.low), cap - 1.0)
        return over

    def products(self, pw, p_count, tab):
        sh, x, z, j, layer, n = self.sh, self.x, self.z, self.j, self.sh.layer, self.sh.nblk
        v = jnp.zeros((layer, n), F32)
        for c in range(sh.cols):
            v = v + self.remote_f[c * layer : (c + 1) * layer] * jnp.where(c == j, 1.0, 0.0)
        v = v * ones((self.row_i >> 3) == x)
        extra_rows, extra_cols, counts, starts, lane_pos = self.enumerate(v, EIGHT)
        over = total_over(counts, starts, CAP_V)
        low = ones(iota((layer, layer), 1) < iota((layer, layer), 0))
        pos_v = jnp.minimum(lane_pos + mm(low, mm(v, self.full)), CAP_V - 1.0)
        s0, s1 = iota((LIST, n), 0), iota((LIST, n), 1)
        u0, u1 = iota((LIST, layer), 0), iota((LIST, layer), 1)
        row_of = jnp.full((LIST, layer), -1, I32)
        col_of = jnp.full((LIST, n), -1, I32)
        for s in range(sh.slots):
            live = s < p_count[0, 0]
            row_of = jnp.where((u0 == s) & live, pw[0, s] - z * layer, row_of)
            col_of = jnp.where((s0 == s) & live, pw[1, s], col_of)
        own_rows, own_cols = ones(row_of == u1), ones(col_of == s1)
        left_2 = jnp.where(self.row_tile == j, self.slot_layer, sh.slots + pos_v)
        for step in range(2):
            if step == 0:
                oh_row, oh_col = stack([own_rows, extra_rows]), stack([own_cols, extra_cols])
                left, right, from_left, kind, cap, count = self.p_layer, self.hm, self.left_1, "H", CAP_1, LIST_1
            else:
                oh_row, oh_col = own_rows, own_cols
                left, right, from_left, kind, cap, count = self.f_layer, self.pm, left_2, "P", CAP_2, LIST
            w = mm(oh_row, left) * mt(oh_col, right)
            rows, lanes, counts, starts, _ = self.enumerate(w, count)
            over = over + total_over(counts, starts, cap)
            k = w.shape[0]
            at = iota((count, k), 0).astype(F32)
            eight = jnp.ones((EIGHT, n), F32)
            lines = (
                mt(eight, lanes * mm(rows, mm(oh_row, from_left * left))),
                mt(eight, lanes * mm(rows, mt(oh_col, self.pos[kind]))),
                mt(jnp.ones((EIGHT, k), F32), rows * ones(at > starts)),
                jnp.where(counts > 0.5, jnp.minimum(starts + counts - 1.0, cap), 1.0 * cap),
            )
            for q, line in enumerate(lines):
                size = line.shape[1]
                tab[2 + step : 3 + step, 32 * q : 32 * q + size] = line[0:1].astype(I32)
        return over


def sparse_products(
    sh, p_ref, h_ref, pw, pc, hw, hc, ph_out, php_out, e_out, over_out,
    message, messages, near_h, near_p, store_h, store_p, prow, pack_r, pack_hz, pack_pz, pack_h, pack_p,
    land_h, land_p, terms_1, terms_2, fstore, tabv_z, tabv_r, tabv, tab_z, tab_r, tab, emsg, emsgs,
    m_send, m_recv, s_send, s_recv, p_send, p_fwd, p_recv, z_send, z_recv,
    t_send, t_recv, e_send, e_recv, t_copy,
):
    i, j = lax.axis_index("row"), lax.axis_index("col")
    x, z = i % sh.inner, i // sh.inner
    me = i * sh.cols + j
    chip, core = j // 2, j % 2
    mate = (i, chip * 2 + 1 - core)
    team = x * sh.cols + j
    slots, strip, size = sh.slots, sh.strip, sh.size
    all_but_me = sh.devices - 1

    def device(d):
        t = (me + d) % sh.devices
        return (t // sh.cols, t % sh.cols)

    def member(d):
        q = (team + d) % sh.team
        return q, (z * sh.inner + q // sh.cols, q % sh.cols)

    def in_strip(q):
        return pl.ds(pl.multiple_of(q * strip, strip), strip)

    lane = iota((1, 128), 1)
    packed = jnp.zeros((1, 128), F32)
    for where, count, scale in ((pw, pc, 1.0), (hw, hc, 16.0)):
        for s in range(slots):
            at = (where[0, s] - i * TILE) * sh.width + where[1, s] - j * sh.width
            packed = packed + jnp.where((lane == at) & (s < count[0, 0]), scale * (s + 1), 0.0)
    message[0] = packed
    messages[me] = packed

    barrier = pltpu.get_barrier_semaphore()

    @pl.loop(1, sh.devices)
    def _(d):
        pl.semaphore_signal(barrier, inc=1, device_id=device(d), device_id_type=MESH)

    for s in range(slots):
        near_h[team * slots + s] = h_ref[s, in_strip(team), :]
        near_p[team * slots + s] = p_ref[s, in_strip(team), :]
        prow[s] = p_ref[s]
    pl.semaphore_wait(barrier, all_but_me)

    def tell(d):
        return remote(message.at[pl.ds(0, 1)], messages.at[pl.ds(me, 1)], m_send, m_recv, device(d))

    @pl.loop(1, sh.devices)
    def _(d):
        tell(d).start()

    def strips(d, which):
        q, dev = member(d)
        ref, near = ((h_ref, near_h), (p_ref, near_p))[which]
        return remote(
            ref.at[:, in_strip(q), :], near.at[pl.ds(team * slots, slots)],
            s_send.at[which, d], s_recv.at[which, team], dev,
        )

    def strips_in(d, which):
        q, dev = member(d)
        ref, near = ((h_ref, near_h), (p_ref, near_p))[which]
        return remote(
            ref.at[:, in_strip(q), :], near.at[pl.ds(q * slots, slots)],
            s_send.at[which, d], s_recv.at[which, q], dev,
        )

    for which in range(2):
        for d in range(1, sh.team):
            strips(d, which).start()

    def other(dc):
        c = (chip + dc) % sh.chips
        return c, c * 2 + core

    p_mate = remote(p_ref, prow.at[pl.ds(slots, slots)], p_send.at[0], p_recv.at[sh.cols], mate)
    p_mate.start()

    def p_block(col):
        return prow.at[pl.ds(sh.others + col * CAP_R, CAP_R)]

    def p_out(dc):
        return remote(pack_r.at[dc - 1], p_block(j), p_send.at[dc], p_recv.at[j], (i, other(dc)[1]))

    def p_in(dc):
        col = other(dc)[1]
        return remote(pack_r.at[dc - 1], p_block(col), p_send.at[dc], p_recv.at[col], (i, col))

    def p_forward(dc):
        col = other(dc)[1]
        return remote(p_block(col), p_block(col), p_fwd.at[dc], p_recv.at[col], mate)

    def p_forward_in(dc):
        col = other(dc)[0] * 2 + 1 - core
        return remote(p_block(col), p_block(col), p_fwd.at[dc], p_recv.at[col], mate)

    def bulk(ref, sem):
        part = ref.at[pl.ds(0, all_but_me)]
        return pltpu.make_async_copy(part, part, sem)

    bulk(messages, m_recv).wait()
    lists = Lists(sh, x, z, j, messages[:, 0, :])

    def publish(source, target, which):
        copy = pltpu.make_async_copy(source, target, t_copy.at[which])
        copy.start()
        copy.wait()

    def entry(ref, table, row, lane):
        return ref[jnp.minimum(jnp.maximum(table[row, lane], 0), ref.shape[0] - 1)]

    over = lists.across(tabv_z)
    publish(tabv_z, tab_z, 0)

    kinds = (
        (store_h, pack_hz, pack_h, land_h, CAP_H_Z, CAP_H, near_h),
        (store_p, pack_pz, pack_p, land_p, CAP_P_Z, CAP_P, near_p),
    )

    def zone(which, layer):
        store, cap = kinds[which][0], kinds[which][4]
        return store.at[pl.ds(sh.team * slots + layer * cap, cap)]

    def across(which, dz):
        pack = kinds[which][1]
        zd = (z + dz) % sh.outer
        return remote(
            pack.at[dz - 1], zone(which, z), z_send.at[which, dz], z_recv.at[which, z],
            (zd * sh.inner + x, j),
        )

    def across_in(which, dz):
        pack = kinds[which][1]
        zs = (z + dz) % sh.outer
        return remote(
            pack.at[dz - 1], zone(which, zs), z_send.at[which, dz], z_recv.at[which, zs],
            (zs * sh.inner + x, j),
        )

    for which in range(2):
        store, pack, _, _, cap, _, near = kinds[which]
        for d in range(1, sh.team):
            strips_in(d, which).wait_recv()
        for dz in range(1, sh.outer):
            for k in range(cap):
                pack[dz - 1, k] = entry(near, tab_z, which, (dz - 1) * LIST_Z + k)
        for dz in range(1, sh.outer):
            across(which, dz).start()
        store[0 : sh.team * slots] = near[...]

    over = over + lists.row_lists(tabv_r)
    publish(tabv_r, tab_r, 1)
    for dc in range(1, sh.chips):
        for k in range(CAP_R):
            pack_r[dc - 1, k] = entry(p_ref, tab_r, 0, (dc - 1) * EIGHT + k)
    for dc in range(1, sh.chips):
        p_out(dc).start()

    over = over + lists.team_lists(tabv)
    over = over + lists.products(pw, pc, tabv)
    publish(tabv, tab, 2)

    def part(which, d):
        pack, land = kinds[which][2], kinds[which][3]
        _, dev = member(d)
        return remote(
            pack.at[d - 1], land.at[:, in_strip(team), :], t_send.at[which, d], t_recv.at[which, team], dev
        )

    def part_in(which, d):
        pack, land = kinds[which][2], kinds[which][3]
        q, dev = member(d)
        return remote(
            pack.at[d - 1], land.at[:, in_strip(q), :], t_send.at[which, d], t_recv.at[which, q], dev
        )

    for which in range(2):
        store, _, pack, land, _, cap, _ = kinds[which]
        for dz in range(1, sh.outer):
            across_in(which, dz).wait_recv()

        @pl.loop(1, sh.team)
        def _(d):
            q, _ = member(d)
            for k in range(cap):
                pack[d - 1, k] = entry(store, tab, which, q * LIST + k)

        for d in range(1, sh.team):
            part(which, d).start()
        for k in range(cap):
            land[k, in_strip(team), :] = entry(store, tab, which, team * LIST + k)

    def multiply(step, left, right, terms, cap):
        row = 2 + step
        acc = None
        for k in range(cap):
            d = jnp.dot(entry(left, tab, row, k), entry(right, tab, row, 32 + k), preferred_element_type=F32)
            acc = d if acc is None else d + acc * tab[row, 64 + k].astype(F32)
            terms[k] = acc
        terms[cap] = jnp.zeros((size, size), F32)

    for dc in range(1, sh.chips):
        p_in(dc).wait_recv()
        p_forward(dc).start()
    p_mate.wait_recv()
    for dc in range(1, sh.chips):
        p_forward_in(dc).wait_recv()
    for d in range(1, sh.team):
        part_in(0, d).wait_recv()
    multiply(0, prow, land_h, terms_1, CAP_1)
    trace = jnp.zeros((size, size), F32)
    for s in range(slots):
        value = entry(terms_1, tab, 2, 96 + s)
        trace = trace + value * jnp.where(pw[0, s] == pw[1, s], 1.0, 0.0)
        rounded = value.astype(BF16)
        fstore[s] = rounded
        ph_out[s] = rounded

    for k in range(CAP_V):
        fstore[slots + k] = entry(terms_1, tab, 2, 96 + LIST + k).astype(BF16)

    diagonal = iota((size, size), 0) == iota((size, size), 1)
    emsg[0, 0] = jnp.sum(jnp.where(diagonal, trace, 0.0), axis=0, keepdims=True)
    emsg[0, 1] = over + jnp.zeros((1, 128), F32)
    emsgs[me] = emsg[0]

    def tell_energy(d):
        return remote(emsg.at[pl.ds(0, 1)], emsgs.at[pl.ds(me, 1)], e_send, e_recv, device(d))

    @pl.loop(1, sh.devices)
    def _(d):
        tell_energy(d).start()

    for d in range(1, sh.team):
        part_in(1, d).wait_recv()
    multiply(1, fstore, land_p, terms_2, CAP_2)
    for s in range(slots):
        php_out[s] = entry(terms_2, tab, 3, 96 + s).astype(BF16)

    bulk(emsgs, e_recv).wait()
    e_out[0, 0] = jnp.sum(jnp.sum(emsgs[:, 0], axis=0))
    over_out[0, 0] = jnp.sum(jnp.sum(emsgs[:, 1], axis=0))

    bulk(messages, m_send).wait()
    bulk(emsgs, e_send).wait()
    for which in range(2):
        for d in range(1, sh.team):
            strips(d, which).wait_send()
            part(which, d).wait_send()
        for dz in range(1, sh.outer):
            across(which, dz).wait_send()
    p_mate.wait_send()
    for dc in range(1, sh.chips):
        p_out(dc).wait_send()
        p_forward(dc).wait_send()


def sparse_path(sh, p_values, p_where, p_count, h_values, h_where, h_count):
    slots, size, strip = sh.slots, sh.size, sh.strip
    block, piece = (size, size), (strip, size)
    bf = lambda *shape: pltpu.VMEM(shape, BF16)
    f32 = lambda *shape: pltpu.VMEM(shape, F32)
    dma = pltpu.SemaphoreType.DMA
    near = sh.team * slots
    away = max(sh.outer - 1, 1)
    chips = max(sh.chips - 1, 1)
    tile = jax.ShapeDtypeStruct((slots,) + block, BF16)
    scalar = jax.ShapeDtypeStruct((1, 1), F32)
    return pl.pallas_call(
        functools.partial(sparse_products, sh),
        out_shape=[tile, tile, scalar, scalar],
        in_specs=[VMEM, VMEM, SMEM, SMEM, SMEM, SMEM],
        out_specs=[VMEM, VMEM, SMEM, SMEM],
        scratch_shapes=[
            f32(1, 1, 128),
            f32(sh.devices, 1, 128),
            bf(near, *piece),
            bf(near, *piece),
            bf(near + sh.outer * CAP_H_Z, *piece),
            bf(near + sh.outer * CAP_P_Z, *piece),
            bf(sh.others + sh.cols * CAP_R, *block),
            bf(chips, CAP_R, *block),
            bf(away, CAP_H_Z, *piece),
            bf(away, CAP_P_Z, *piece),
            bf(sh.team, CAP_H, *piece),
            bf(sh.team, CAP_P, *piece),
            bf(CAP_H, *block),
            bf(CAP_P, *block),
            f32(CAP_1 + 1, *block),
            f32(CAP_2 + 1, *block),
            bf(slots + CAP_V, *block),
            pltpu.VMEM((8, 128), I32),
            pltpu.VMEM((8, 128), I32),
            pltpu.VMEM((8, 128), I32),
            pltpu.SMEM((8, 128), I32),
            pltpu.SMEM((8, 128), I32),
            pltpu.SMEM((8, 128), I32),
            f32(1, 2, 1, 128),
            f32(sh.devices, 2, 1, 128),
            dma, dma,
            dma((2, sh.team)), dma((2, sh.team)),
            dma((sh.chips,)), dma((sh.chips,)), dma((sh.cols + 1,)),
            dma((2, sh.outer)), dma((2, sh.outer)),
            dma((2, sh.team)), dma((2, sh.team)),
            dma, dma, dma((3,)),
        ],
        compiler_params=pltpu.CompilerParams(collective_id=2, has_side_effects=True, vmem_limit_bytes=24 << 20),
        name="sparse_products",
    )(p_values, h_values, p_where.T, p_count, h_where.T, h_count)


def per_device(rows, cols, *args):
    slots, size, _ = args[0].shape
    sh = Shape(rows, cols, slots, size)
    if not sh.fits():
        return dense_path(rows, cols, *args)
    ph, php, energy, over = sparse_path(sh, *args)
    return lax.cond(
        over[0, 0] > 0.0,
        lambda: dense_path(rows, cols, *args),
        lambda: (ph, php, energy[0, 0]),
    )


def solution(mesh):
    placed = (
        P("row", "col", None),
        P("row", "col"),
        P("row", "col"),
        P("row", "col", None),
        P("row", "col"),
        P("row", "col"),
    )
    return jax.shard_map(
        functools.partial(per_device, mesh.shape["row"], mesh.shape["col"]),
        mesh=mesh,
        in_specs=placed,
        out_specs=(P("row", "col", None), P("row", "col", None), P()),
        check_vma=False,
    )
```

```python
import functools

import jax
import jax.numpy as jnp
from jax import lax
from jax.experimental import pallas as pl
from jax.experimental.pallas import tpu as pltpu
from jax.sharding import PartitionSpec as P

TILE = 8
CHUNKS = 6
IN_FLIGHT = 16
MESH = pl.DeviceIdType.MESH
ANY = pl.BlockSpec(memory_space=pl.ANY)
VMEM = pl.BlockSpec(memory_space=pltpu.VMEM)
SMEM = pl.BlockSpec(memory_space=pltpu.SMEM)


def at_row(r):
    return (r, lax.axis_index("col"))


def at_col(c):
    return (lax.axis_index("row"), c)


def remote(src, dst, send_sem, recv_sem, device):
    return pltpu.make_async_remote_copy(
        src_ref=src,
        dst_ref=dst,
        send_sem=send_sem,
        recv_sem=recv_sem,
        device_id=device,
        device_id_type=MESH,
    )


def greet(rows, cols):
    me_row, me_col = lax.axis_index("row"), lax.axis_index("col")
    barrier = pltpu.get_barrier_semaphore()
    for d in range(1, rows):
        pl.semaphore_signal(
            barrier, inc=1, device_id=at_row((me_row + d) % rows), device_id_type=MESH
        )
    for d in range(1, cols):
        pl.semaphore_signal(
            barrier, inc=1, device_id=at_col((me_col + d) % cols), device_id_type=MESH
        )
    pl.semaphore_wait(barrier, rows + cols - 2)


class ColumnGather:
    def __init__(self, rows, own, land, out, up_send, down_send, x_send, recv, local):
        self.own, self.land, self.out = own, land, out
        self.up_send, self.down_send, self.x_send = up_send, down_send, x_send
        self.recv, self.local = recv, local
        self.inner = 2 if rows % 2 == 0 else 1
        self.outer = rows // self.inner
        self.chunks = recv.shape[1]
        self.size = own.shape[0] // self.chunks
        self.me = lax.axis_index("row")
        self.x, self.z = self.me % self.inner, self.me // self.inner
        self.cross_first = 1 if self.inner == 2 and self.chunks > 1 else 0

    def later(self, ch):
        return (ch + self.cross_first) % self.chunks

    def row(self, z, line):
        return z * self.inner + (self.x if line == 0 else self.inner - 1 - self.x)

    def part(self, ch):
        return pl.ds(ch * self.size, self.size)

    def copy(self, r, ch, own, way):
        sems, target = {
            "up": (self.up_send, self.me + self.inner),
            "down": (self.down_send, self.me - self.inner),
            "x": (self.x_send, self.row(self.z, 1)),
        }[way]
        part = self.part(ch)
        src = self.own.at[part] if own else self.land.at[r, part]
        return remote(src, self.land.at[r, part], sems.at[r, ch], self.recv.at[r, ch], at_row(target))

    def keep(self, r, ch):
        part = self.part(ch)
        return pltpu.make_async_copy(self.land.at[r, part], self.out.at[r, part], self.local.at[r, ch])

    def along(self, r, ch, own, act):
        @pl.when(self.z < self.outer - 1)
        def _():
            act(self.copy(r, ch, own, "up"))

        @pl.when(self.z > 0)
        def _():
            act(self.copy(r, ch, own, "down"))

    def arrive(self, r, ch):
        self.copy(r, ch, False, "x").wait_recv()
        self.keep(r, ch).start()

    def start(self):
        for ch in range(self.chunks):
            if self.inner == 2:
                self.copy(self.me, ch, True, "x").start()
            self.along(self.me, self.later(ch), True, lambda copy: copy.start())
        if self.cross_first:
            r = self.row(self.z, 1)
            self.arrive(r, 0)
            self.along(r, 0, False, lambda copy: copy.start())

    def pieces(self):
        lines = [(self.later(ch), 0) for ch in range(self.chunks)]
        return lines + [(0, 1)] * self.cross_first

    def relayed(self, d, side, ch, line, act):
        z = self.z - d if side == 0 else self.z + d
        there = self.z >= d if side == 0 else self.z + d < self.outer
        r = self.row(z, line)

        @pl.when(there)
        def _():
            if act == "start":
                self.arrive(r, ch)
            on = self.z < self.outer - 1 if side == 0 else self.z > 0

            @pl.when(on)
            def _():
                copy = self.copy(r, ch, False, "up" if side == 0 else "down")
                copy.start() if act == "start" else copy.wait_send()

            if self.inner == 2 and ch >= self.cross_first:
                copy = self.copy(r, ch, False, "x")
                copy.start() if act == "start" else copy.wait_send()

    def relay(self, d):
        for ch, line in self.pieces():
            for side in range(2):
                self.relayed(d, side, ch, line, "start")

    def finish(self):
        if self.inner == 2:
            for ch in range(self.cross_first, self.chunks):
                self.arrive(self.row(self.z, 1), ch)
            for d in range(1, self.outer):
                for side in range(2):
                    z = self.z - d if side == 0 else self.z + d
                    there = self.z >= d if side == 0 else self.z + d < self.outer

                    @pl.when(there)
                    def _():
                        for ch in range(self.cross_first, self.chunks):
                            self.arrive(self.row(z, 1), ch)
        for ch in range(self.chunks):
            if self.inner == 2:
                self.copy(self.me, ch, True, "x").wait_send()
            self.along(self.me, ch, True, lambda copy: copy.wait_send())
        if self.cross_first:
            self.along(self.row(self.z, 1), 0, False, lambda copy: copy.wait_send())
        for d in range(1, self.outer):
            for ch, line in self.pieces():
                for side in range(2):
                    self.relayed(d, side, ch, line, "wait")
        for r in range(self.inner * self.outer):
            @pl.when(r != self.me)
            def _():
                for ch in range(self.chunks):
                    self.keep(r, ch).wait()


def col_copies(cols, own, out, send, recv):
    me = lax.axis_index("col")
    made = []
    for d in range(1, cols):
        made.append(
            remote(own, out.at[me], send.at[d], recv.at[d], at_col((me + d) % cols))
        )
    return made


def row_copies(rows, own, out, send, recv):
    me = lax.axis_index("row")
    made = []
    for d in range(1, rows):
        made.append(
            remote(own, out.at[me], send.at[d], recv.at[d], at_row((me + d) % rows))
        )
    return made


def first_gather(
    rows, cols, p_ref, h_ref, meta_ref, prow, hcol, prow_meta, col_meta,
    land, up_send, down_send, x_send, recv, out_sems,
    p_send, p_recv, mc_send, mc_recv, mr_send, mr_recv, local,
):
    me_row, me_col = lax.axis_index("row"), lax.axis_index("col")
    keep = [
        pltpu.make_async_copy(h_ref, hcol.at[me_row], local.at[0]),
        pltpu.make_async_copy(p_ref, prow.at[me_col], local.at[1]),
        pltpu.make_async_copy(meta_ref, prow_meta.at[me_col], local.at[2]),
        pltpu.make_async_copy(meta_ref, col_meta.at[me_row], local.at[3]),
    ]
    greet(rows, cols)
    gather = ColumnGather(
        rows, h_ref, land, hcol, up_send, down_send, x_send, recv, out_sems
    )
    across = (
        col_copies(cols, p_ref, prow, p_send, p_recv)
        + col_copies(cols, meta_ref, prow_meta, mc_send, mc_recv)
        + row_copies(rows, meta_ref, col_meta, mr_send, mr_recv)
    )
    for copy in across + keep:
        copy.start()
    gather.start()
    for d in range(1, gather.outer):
        gather.relay(d)
    gather.finish()
    for copy in across + keep:
        copy.wait()


def second_gather(
    rows, cols, p_ref, f_ref, e_ref, frow, pcol, e_out,
    e_cols, e_rows, e_sum,
    land, up_send, down_send, x_send, recv, out_sems,
    p_send, p_recv, ec_send, ec_recv, er_send, er_recv, local,
):
    me_row, me_col = lax.axis_index("row"), lax.axis_index("col")
    keep = [
        pltpu.make_async_copy(p_ref, pcol.at[me_row], local.at[0]),
        pltpu.make_async_copy(f_ref, frow.at[me_col], local.at[1]),
    ]
    greet(rows, cols)
    energies = col_copies(cols, e_ref, e_cols, ec_send, ec_recv)
    for copy in energies:
        copy.start()
    gather = ColumnGather(
        rows, p_ref, land, pcol, up_send, down_send, x_send, recv, out_sems
    )
    across = col_copies(cols, f_ref, frow, p_send, p_recv)
    for copy in across + keep:
        copy.start()
    gather.start()
    e_cols[me_col] = e_ref[...]
    for copy in energies:
        copy.wait()
    total = e_cols[0]
    for c in range(1, cols):
        total = total + e_cols[c]
    e_sum[...] = total
    e_rows[me_row] = total
    if gather.outer > 1:
        gather.relay(1)
    sums = row_copies(rows, e_sum, e_rows, er_send, er_recv)
    for copy in sums:
        copy.start()
    for d in range(2, gather.outer):
        gather.relay(d)
    for copy in sums:
        copy.wait()
    total = e_rows[0]
    for r in range(1, rows):
        total = total + e_rows[r]
    e_out[...] = total
    gather.finish()
    for copy in across + keep:
        copy.wait()


def block_products(
    rows, cols, right_lane, with_trace, lmeta, rmeta, left, right, *rest
):
    if with_trace:
        out, e_out = rest[:2]
    else:
        e_in, out, e_out = rest[:3]
    acc, lbuf, rbuf, head, nxt, inner, mask, table, ml, mr, ms, sems = rest[-12:]
    slots = out.shape[0]
    i, j = lax.axis_index("row"), lax.axis_index("col")
    nblk = rows * TILE
    tile_cols = nblk // cols
    words = -(-nblk // 32)
    count_lane = 4 * slots
    acc[...] = jnp.zeros_like(acc)

    for t in range(TILE + 1):
        head[t] = -1

    for t in range(tile_cols * words + 1):
        mask[t] = 0

    @pl.loop(0, cols)
    def _(c):
        live = lmeta[c, 0, count_lane]
        for s in range(slots):
            row = jnp.where(s < live, lmeta[c, 0, s] - i * TILE, TILE)
            idx = c * slots + s
            inner[idx] = lmeta[c, 0, slots + s]
            nxt[idx] = head[row]
            head[row] = idx

    @pl.loop(0, rows)
    def _(r):
        live = rmeta[r, 0, count_lane + (1 if right_lane else 0)]
        for s in range(slots):
            k = rmeta[r, 0, right_lane + s]
            col = rmeta[r, 0, right_lane + slots + s] - j * tile_cols
            word = jnp.where(s < live, col * words + (k >> 5), tile_cols * words)
            mask[word] = mask[word] | (jnp.int32(1) << (k & 31))
            table[jnp.where(s < live, k * tile_cols + col, nblk * tile_cols)] = r * slots + s

    def find_slot(s, n):
        row = lmeta[j, 0, s] - i * TILE
        col = lmeta[j, 0, slots + s] - j * tile_cols

        def more(state):
            return state[0] >= 0

        def step(state):
            at, n = state
            k = inner[at]
            ml[n] = at
            mr[n] = table[k * tile_cols + col]
            ms[n] = s
            return nxt[at], n + ((mask[col * words + (k >> 5)] >> (k & 31)) & 1)

        return lax.while_loop(more, step, (head[row], n))[1]

    own_count = lmeta[j, 0, count_lane]
    found = lax.fori_loop(0, own_count, find_slot, jnp.int32(0))

    def fetch(base, m):
        a, b = ml[base + m], mr[base + m]
        return (
            pltpu.make_async_copy(left.at[a], lbuf.at[m], sems.at[0, m]),
            pltpu.make_async_copy(right.at[b], rbuf.at[m], sems.at[1, m]),
        )

    @pl.loop(0, (found + IN_FLIGHT - 1) // IN_FLIGHT)
    def _(chunk):
        base = chunk * IN_FLIGHT
        size = jnp.minimum(found - base, IN_FLIGHT)

        @pl.loop(0, size)
        def _(m):
            for copy in fetch(base, m):
                copy.start()

        @pl.loop(0, size)
        def _(m):
            for copy in fetch(base, m):
                copy.wait()
            s = ms[base + m]
            acc[s] += jnp.dot(lbuf[m], rbuf[m], preferred_element_type=jnp.float32)

    out[...] = acc[...].astype(out.dtype)
    if with_trace:
        size = acc.shape[1]
        e_out[...] = jnp.zeros_like(e_out)
        diagonal = lax.broadcasted_iota(jnp.int32, (size, size), 0) == lax.broadcasted_iota(
            jnp.int32, (size, size), 1
        )

        @pl.loop(0, own_count)
        def _(s):
            @pl.when(lmeta[j, 0, s] == lmeta[j, 0, slots + s])
            def _():
                e_out[...] += jnp.sum(jnp.where(diagonal, acc[s], 0.0))
    else:
        e_out[0, 0] = e_in[0, 0]


def dense_path(rows, cols, p_values, p_where, p_count, h_values, h_where, h_count):
    slots, size, _ = p_values.shape
    dtype = p_values.dtype
    nblk = rows * TILE
    tile_cols = nblk // cols
    words = -(-nblk // 32)
    meta = jnp.concatenate(
        [p_where[:, 0], p_where[:, 1], h_where[:, 0], h_where[:, 1], p_count[0], h_count[0]]
    )
    meta = jnp.broadcast_to(jnp.pad(meta, (0, 128 - meta.shape[0]))[None, :], (8, 128))
    dma = pltpu.SemaphoreType.DMA
    chunks = CHUNKS if slots % CHUNKS == 0 else 1
    chunk_sems = [pltpu.VMEM((rows, slots, size, size), dtype)] + [dma((rows, chunks))] * 5
    col_sems = [dma((cols,)), dma((cols,))]
    row_sems = [dma((rows,)), dma((rows,))]
    tile = (slots, size, size)
    prow, hcol, prow_meta, col_meta = pl.pallas_call(
        functools.partial(first_gather, rows, cols),
        out_shape=[
            jax.ShapeDtypeStruct((cols,) + tile, dtype),
            jax.ShapeDtypeStruct((rows,) + tile, dtype),
            jax.ShapeDtypeStruct((cols, 8, 128), jnp.int32),
            jax.ShapeDtypeStruct((rows, 8, 128), jnp.int32),
        ],
        in_specs=[VMEM] * 3,
        out_specs=[ANY] * 4,
        scratch_shapes=chunk_sems + col_sems + col_sems + row_sems + [dma((4,))],
        compiler_params=pltpu.CompilerParams(collective_id=0, has_side_effects=True),
        name="first_gather",
    )(p_values, h_values, meta)

    def products(right_lane, with_trace, lmeta, rmeta, left, right, *more):
        smem = lambda n: pltpu.SMEM((n,), jnp.int32)
        most = slots * nblk + 1
        return pl.pallas_call(
            functools.partial(block_products, rows, cols, right_lane, with_trace),
            out_shape=[
                jax.ShapeDtypeStruct(tile, dtype),
                jax.ShapeDtypeStruct((8, 128) if with_trace else (1, 1), jnp.float32),
            ],
            in_specs=[SMEM, SMEM, ANY, ANY] + [SMEM] * len(more),
            out_specs=[VMEM, VMEM if with_trace else SMEM],
            scratch_shapes=[
                pltpu.VMEM(tile, jnp.float32),
                pltpu.VMEM((IN_FLIGHT, size, size), dtype),
                pltpu.VMEM((IN_FLIGHT, size, size), dtype),
                smem(TILE + 1),
                smem(cols * slots),
                smem(cols * slots),
                smem(tile_cols * words + 1),
                smem(nblk * tile_cols + 1),
                smem(most),
                smem(most),
                smem(most),
                dma((2, IN_FLIGHT)),
            ],
            name="products",
        )(
            lmeta,
            rmeta,
            left.reshape((cols * slots, size, size)),
            right.reshape((rows * slots, size, size)),
            *more,
        )

    ph_values, part = products(2 * slots, True, prow_meta, col_meta, prow, hcol)
    frow, pcol, energy = pl.pallas_call(
        functools.partial(second_gather, rows, cols),
        out_shape=[
            jax.ShapeDtypeStruct((cols,) + tile, dtype),
            jax.ShapeDtypeStruct((rows,) + tile, dtype),
            jax.ShapeDtypeStruct((8, 128), jnp.float32),
        ],
        in_specs=[VMEM] * 3,
        out_specs=[ANY, ANY, VMEM],
        scratch_shapes=[
            pltpu.VMEM((cols, 8, 128), jnp.float32),
            pltpu.VMEM((rows, 8, 128), jnp.float32),
            pltpu.VMEM((8, 128), jnp.float32),
        ]
        + chunk_sems + col_sems + col_sems + row_sems + [dma((2,))],
        compiler_params=pltpu.CompilerParams(collective_id=1, has_side_effects=True),
        name="second_gather",
    )(p_values, ph_values, part)
    php_values, energy = products(0, False, prow_meta, col_meta, frow, pcol, energy)
    return (ph_values, php_values, energy[0, 0])


CAP_H_Z, CAP_P_Z = 17, 12
CAP_H, CAP_P = 14, 9
CAP_R, CAP_V = 7, 7
CAP_1, CAP_2 = 18, 12
LIST, LIST_Z, LIST_1, EIGHT = 16, 24, 24, 8
F32, BF16, I32 = jnp.float32, jnp.bfloat16, jnp.int32


def log2(n):
    return n.bit_length() - 1


def power(n):
    return n > 0 and n & (n - 1) == 0


class Shape:
    def __init__(self, rows, cols, slots, size):
        self.rows, self.cols, self.slots, self.size = rows, cols, slots, size
        self.devices = rows * cols
        self.nblk = rows * TILE
        self.inner = 2 if rows % 2 == 0 else 1
        self.outer = rows // self.inner
        self.layer = self.inner * TILE
        self.team = self.inner * cols
        self.strip = size // self.team
        self.width = self.nblk // cols
        self.chips = cols // 2
        self.others = 2 * slots

    def fits(self):
        return (
            power(self.rows)
            and power(self.cols)
            and self.cols >= 2
            and self.outer >= 2
            and self.nblk <= 64
            and self.width * TILE <= 128
            and self.slots <= 15
            and self.strip % 16 == 0
            and self.team * LIST <= 128
            and (self.outer - 1) * LIST_Z <= 128
            and (self.chips - 1) * EIGHT <= 128
        )


def mm(a, b):
    return lax.dot_general(a.astype(BF16), b.astype(BF16), (((1,), (0,)), ((), ())), preferred_element_type=F32)


def mt(a, b):
    return lax.dot_general(a.astype(BF16), b.astype(BF16), (((1,), (1,)), ((), ())), preferred_element_type=F32)


def tm(a, b):
    return lax.dot_general(a.astype(BF16), b.astype(BF16), (((0,), (0,)), ((), ())), preferred_element_type=F32)


def ones(cond):
    return jnp.where(cond, 1.0, 0.0).astype(F32)


def iota(shape, dim):
    return lax.broadcasted_iota(I32, shape, dim)


def block_index(shape, dim, size):
    return iota(shape, dim) // size


def total_over(counts, starts, cap):
    over = ones(starts + counts > cap + 0.5)
    return jnp.sum(jnp.sum(over, axis=0, keepdims=True), axis=1, keepdims=True)


def stack(parts):
    return jnp.concatenate(parts, axis=0)


class Lists:
    def __init__(self, sh, x, z, j, message):
        self.sh, self.x, self.z, self.j = sh, x, z, j
        n, width, layer = sh.nblk, sh.width, sh.layer
        lw = log2(width)
        r, l = iota((n, n), 0), iota((n, n), 1)
        a0, d0 = iota((sh.cols * n, sh.devices), 0), iota((sh.cols * n, sh.devices), 1)
        spread = mm(ones(d0 == ((a0 & (n - 1)) >> 3) * sh.cols + (a0 >> log2(n))), message)
        a1, l1 = iota((sh.cols * n, 128), 0), iota((sh.cols * n, 128), 1)
        spread = jnp.where((l1 >> lw) == (a1 & 7), spread, 0.0)
        l2, m2 = iota((128, n), 0), iota((128, n), 1)
        spread = mm(spread, ones((l2 & (width - 1)) == (m2 & (width - 1))))
        both = jnp.zeros((n, n), F32)
        for c in range(sh.cols):
            both = both + jnp.where((l >> lw) == c, spread[c * n : (c + 1) * n], 0.0)
        hs = jnp.floor(both * (1.0 / 16.0))
        ps = both - 16.0 * hs
        self.pos = {}
        self.pm, self.hm = ones(ps > 0.5), ones(hs > 0.5)
        self.fm = self.pm * ones(mm(self.pm, self.hm) > 0.5)
        self.up, self.low = ones(r < l), ones(l < r)
        self.low_layer = ones((l < r) & (l // layer == r // layer))
        self.full = jnp.ones((n, n), F32)
        self.r, self.l, self.lane_tile = r, l, l >> lw
        team = ((r >> 3) & (sh.inner - 1)) * sh.cols + self.lane_tile
        at = (team * sh.slots).astype(F32)
        self.near = {"H": at + hs - 1.0, "P": at + ps - 1.0}
        s0, s1 = iota((layer, n), 0), iota((layer, n), 1)
        self.sel = ones(s1 == z * layer + s0)
        self.row_i, self.row_tile = s0, (s1 >> lw)
        self.p_layer, self.f_layer = mm(self.sel, self.pm), mm(self.sel, self.fm)
        self.slot_layer = mm(self.sel, ps) - 1.0

    def enumerate(self, v, count, lane_pos=None):
        k, n = v.shape
        counts = mt(jnp.ones((count, n), F32), v)
        a, b = iota((k, k), 0), iota((k, k), 1)
        starts = mm(counts, ones(a < b))
        at = iota((count, k), 0).astype(F32)
        rows = ones((starts <= at) & (at < starts + counts))
        local = mm(rows * (at - starts + 1.0), jnp.ones((k, n), F32))
        if lane_pos is None:
            lane_pos = mm(v, self.up)
        found = mm(rows, v * (lane_pos + 1.0))
        lanes = ones((found == local) & (local > 0.5))
        return rows, lanes, counts, starts, lane_pos

    def position(self, v, low):
        return mm(v, self.up) + mm(low, mm(v, self.full))

    def across(self, tab):
        sh, z, layer, n = self.sh, self.z, self.sh.layer, self.sh.nblk
        p_s, f_s = mt(self.sel, self.pm), mt(self.sel, self.fm)
        i_layer = self.l[0:layer] // layer
        lhs, live, pay = [], [], []
        for kind, left, right in (("H", p_s, self.hm), ("P", f_s, self.pm)):
            live_kind, pay_kind = mm(self.sel, right), mm(self.sel, self.near[kind])
            for dz in range(1, sh.outer):
                lhs.append(left * ones(i_layer == (z + dz) % sh.outer))
                live.append(live_kind)
                pay.append(pay_kind)
        v = ones(mm(stack(lhs), self.pm) > 0.5) * stack(live)
        k = v.shape[0]
        lists = 2 * (sh.outer - 1)
        a, b = iota((k, k), 0), iota((k, k), 1)
        counts = mt(jnp.ones((EIGHT, n), F32), v)
        starts = mm(counts, ones((a < b) & (a // layer == b // layer)))
        t0 = iota((lists * LIST_Z, k), 0)
        at = (t0 % LIST_Z).astype(F32)
        rows = ones(
            (starts[0:1] <= at)
            & (at < starts[0:1] + counts[0:1])
            & (t0 // LIST_Z == block_index((lists * LIST_Z, k), 1, layer))
        )
        local = mm(rows * (at - starts[0:1] + 1.0), jnp.ones((k, n), F32))
        found = mm(rows, v * (mm(v, self.up) + 1.0))
        picked = jnp.where((found == local) & (local > 0.5), mm(rows, stack(pay)), 0.0)
        half = (sh.outer - 1) * LIST_Z
        for which in range(2):
            line = mt(jnp.ones((EIGHT, n), F32), picked[which * half : (which + 1) * half])
            tab[which : which + 1, 0:half] = line[0:1].astype(I32)
        lane_h = block_index((EIGHT, k), 1, layer) < sh.outer - 1
        cap = jnp.where(lane_h, 1.0 * CAP_H_Z, 1.0 * CAP_P_Z)
        return total_over(counts - cap, starts, 0.0)

    def row_lists(self, tab):
        sh, x, j, layer, n = self.sh, self.x, self.j, self.sh.layer, self.sh.nblk
        tiles = [ones(self.row_tile == c) for c in range(sh.cols)]
        wide = stack([self.p_layer * t for t in tiles])
        passed = ones(mt(wide, self.pm) > 0.5) * stack([self.f_layer] * sh.cols)
        own = wide
        self.outputs = jnp.maximum(own, passed)
        self.remote_f = passed * (1.0 - ones(stack([t for t in tiles]) > 0.5))
        reads = ones(mt(self.outputs, self.hm) > 0.5) * stack([self.p_layer] * sh.cols)
        mine = ones((self.row_i >> 3) == x)
        chip = j // 2
        low = ones(iota((layer, layer), 1) < iota((layer, layer), 0))
        seg_tri = ones((self.lane_tile == (self.r >> log2(sh.width))) & (self.r < self.l))
        seg_full = ones(self.lane_tile == (self.r >> log2(sh.width)))
        over = jnp.zeros((1, 1), F32)
        for dc in range(sh.chips):
            c = (chip + dc) % sh.chips
            v = jnp.zeros((layer, n), F32)
            for k in range(sh.cols):
                v = jnp.maximum(v, reads[k * layer : (k + 1) * layer] * jnp.where(k // 2 == c, 1.0, 0.0))
            v = v * mine
            if dc == 0:
                pos = mm(v, seg_tri) + mm(low, mm(v, seg_full))
                pos = jnp.minimum(pos, CAP_R - 1.0)
                continue
            v = v * ones(self.row_tile == j)
            rows, lanes, counts, starts, _ = self.enumerate(v, EIGHT)
            line = mt(jnp.ones((EIGHT, n), F32), lanes * mm(rows, self.slot_layer))
            tab[0:1, (dc - 1) * EIGHT : dc * EIGHT] = line[0:1].astype(I32)
            over = over + total_over(counts, starts, CAP_R)
        self.left_1 = jnp.where(
            self.row_tile == j,
            self.slot_layer,
            jnp.where(
                self.row_tile // 2 == chip,
                sh.slots + self.slot_layer,
                sh.others + self.row_tile.astype(F32) * CAP_R + pos,
            ),
        )
        return over

    def team_lists(self, which, tab):
        sh, x, z, j, layer, n = self.sh, self.x, self.z, self.j, self.sh.layer, self.sh.nblk
        a, b = iota((layer, layer), 0), iota((layer, layer), 1)
        turn = lambda m: tm(m, ones(a == b))
        kind, cap_z, cap = (("H", CAP_H_Z, CAP_H), ("P", CAP_P_Z, CAP_P))[which]
        turned = turn(self.p_layer if kind == "H" else self.f_layer)
        live = self.hm if kind == "H" else self.pm
        lane_x = iota((n, layer), 1) >> 3
        k_layer = self.r // layer
        pos_z = self.position(ones(mm(turned, self.p_layer) > 0.5) * live, self.low_layer)
        far = (sh.team * sh.slots + k_layer * cap_z).astype(F32) + jnp.minimum(pos_z, cap_z - 1.0)
        payload = jnp.where(k_layer == z, self.near[kind], far)
        by_x = stack([turned * ones(lane_x == xd) for xd in range(sh.inner)])
        needs = []
        if kind == "H":
            made = [
                ones(mm(by_x, self.outputs[c * layer : (c + 1) * layer]) > 0.5) for c in range(sh.cols)
            ]
        else:
            one = ones(mm(by_x, self.p_layer) > 0.5)
            made = [one * ones((iota((sh.inner * n, n), 1) >> log2(sh.width)) == c) for c in range(sh.cols)]
        for xd in range(sh.inner):
            for c in range(sh.cols):
                needs.append(made[c][xd * n : (xd + 1) * n] * live)
        all_needs = stack(needs)
        lane_pos = mm(all_needs, self.up)
        counts = stack([mt(jnp.ones((LIST, n), F32), v) for v in needs])
        starts = mm(counts, self.up)
        over = total_over(counts, starts, cap)
        at = (iota((sh.team * LIST, n), 0) % LIST).astype(F32)
        rows = ones((starts <= at) & (at < starts + counts))
        local = mm(rows * (at - starts + 1.0), self.full)
        marked = all_needs * (lane_pos + 1.0)
        found = stack(
            [
                mm(rows[t * LIST : (t + 1) * LIST], marked[t * n : (t + 1) * n])
                for t in range(sh.team)
            ]
        )
        picked = jnp.where((found == local) & (local > 0.5), mm(rows, payload), 0.0)
        line = mt(jnp.ones((EIGHT, n), F32), picked)
        tab[0:1, 0 : sh.team * LIST] = line[0:1].astype(I32)
        me = x * sh.cols + j
        mine = jnp.zeros((n, n), F32)
        for t in range(sh.team):
            mine = mine + needs[t] * jnp.where(me == t, 1.0, 0.0)
        self.pos[kind] = jnp.minimum(self.position(mine, self.low), cap - 1.0)
        return over

    def products(self, pw, p_count, tab):
        sh, x, z, j, layer, n = self.sh, self.x, self.z, self.j, self.sh.layer, self.sh.nblk
        v = jnp.zeros((layer, n), F32)
        for c in range(sh.cols):
            v = v + self.remote_f[c * layer : (c + 1) * layer] * jnp.where(c == j, 1.0, 0.0)
        v = v * ones((self.row_i >> 3) == x)
        extra_rows, extra_cols, counts, starts, lane_pos = self.enumerate(v, EIGHT)
        over = total_over(counts, starts, CAP_V)
        low = ones(iota((layer, layer), 1) < iota((layer, layer), 0))
        pos_v = jnp.minimum(lane_pos + mm(low, mm(v, self.full)), CAP_V - 1.0)
        s0, s1 = iota((LIST, n), 0), iota((LIST, n), 1)
        u0, u1 = iota((LIST, layer), 0), iota((LIST, layer), 1)
        row_of = jnp.full((LIST, layer), -1, I32)
        col_of = jnp.full((LIST, n), -1, I32)
        for s in range(sh.slots):
            live = s < p_count[0, 0]
            row_of = jnp.where((u0 == s) & live, pw[0, s] - z * layer, row_of)
            col_of = jnp.where((s0 == s) & live, pw[1, s], col_of)
        own_rows, own_cols = ones(row_of == u1), ones(col_of == s1)
        left_2 = jnp.where(self.row_tile == j, self.slot_layer, sh.slots + pos_v)
        for step in range(2):
            if step == 0:
                oh_row, oh_col = stack([own_rows, extra_rows]), stack([own_cols, extra_cols])
                left, right, from_left, kind, cap, count = self.p_layer, self.hm, self.left_1, "H", CAP_1, LIST_1
            else:
                oh_row, oh_col = own_rows, own_cols
                left, right, from_left, kind, cap, count = self.f_layer, self.pm, left_2, "P", CAP_2, LIST
            w = mm(oh_row, left) * mt(oh_col, right)
            rows, lanes, counts, starts, _ = self.enumerate(w, count)
            over = over + total_over(counts, starts, cap)
            k = w.shape[0]
            at = iota((count, k), 0).astype(F32)
            eight = jnp.ones((EIGHT, n), F32)
            lines = (
                mt(eight, lanes * mm(rows, mm(oh_row, from_left * left))),
                mt(eight, lanes * mm(rows, mt(oh_col, self.pos[kind]))),
                mt(jnp.ones((EIGHT, k), F32), rows * ones(at > starts)),
                jnp.where(counts > 0.5, jnp.minimum(starts + counts - 1.0, cap), 1.0 * cap),
            )
            for q, line in enumerate(lines):
                size = line.shape[1]
                tab[2 + step : 3 + step, 32 * q : 32 * q + size] = line[0:1].astype(I32)
        return over


def sparse_products(
    sh, p_hbm, h_hbm, pw_hbm, pc_hbm, hw_hbm, hc_hbm, out, e_out, over_out,
    p_ref, h_ref, pw, pc, hw, hc,
    message, messages, near_h, near_p, store_h, store_p, prow, pack_r, pack_hz, pack_pz, pack_h, pack_p,
    land_h, land_p, terms_1, terms_2, fstore, tabv_z, tabv_r, tabv_h, tabv, tab_z, tab_r, tab_h, tab, emsg, emsgs,
    m_send, m_recv, s_send, s_recv, p_send, p_fwd, p_recv, z_send, z_recv,
    t_send, t_recv, e_send, e_recv, t_copy, fetch,
):
    i, j = lax.axis_index("row"), lax.axis_index("col")
    x, z = i % sh.inner, i // sh.inner
    me = i * sh.cols + j
    chip, core = j // 2, j % 2
    mate = (i, chip * 2 + 1 - core)
    team = x * sh.cols + j
    slots, strip, size = sh.slots, sh.strip, sh.size
    all_but_me = sh.devices - 1

    def device(d):
        t = (me + d) % sh.devices
        return (t // sh.cols, t % sh.cols)

    def member(d):
        q = (team + d) % sh.team
        return q, (z * sh.inner + q // sh.cols, q % sh.cols)

    def in_strip(q):
        return pl.ds(pl.multiple_of(q * strip, strip), strip)

    fetches = [
        pltpu.make_async_copy(source, target, fetch.at[k])
        for k, (source, target) in enumerate(
            (
                (pw_hbm, pw), (pc_hbm, pc), (hw_hbm, hw), (hc_hbm, hc),
                (h_hbm, h_ref), (p_hbm, p_ref),
            )
        )
    ]
    for copy in fetches:
        copy.start()
    barrier = pltpu.get_barrier_semaphore()

    @pl.loop(1, sh.devices)
    def _(d):
        pl.semaphore_signal(barrier, inc=1, device_id=device(d), device_id_type=MESH)

    for copy in fetches[:4]:
        copy.wait()
    lane = iota((1, 128), 1)
    packed = jnp.zeros((1, 128), F32)
    for where, count, scale in ((pw, pc, 1.0), (hw, hc, 16.0)):
        for s in range(slots):
            at = (where[0, s] - i * TILE) * sh.width + where[1, s] - j * sh.width
            packed = packed + jnp.where((lane == at) & (s < count[0, 0]), scale * (s + 1), 0.0)
    message[0] = packed
    messages[me] = packed
    for copy in fetches[4:]:
        copy.wait()
    for s in range(slots):
        near_h[team * slots + s] = h_ref[s, in_strip(team), :]
        near_p[team * slots + s] = p_ref[s, in_strip(team), :]
        prow[s] = p_ref[s]
    pl.semaphore_wait(barrier, all_but_me)

    def tell(d):
        return remote(message.at[pl.ds(0, 1)], messages.at[pl.ds(me, 1)], m_send, m_recv, device(d))

    @pl.loop(1, sh.devices)
    def _(d):
        tell(d).start()

    def strips(d, which):
        q, dev = member(d)
        ref, near = ((h_ref, near_h), (p_ref, near_p))[which]
        return remote(
            ref.at[:, in_strip(q), :], near.at[pl.ds(team * slots, slots)],
            s_send.at[which, d], s_recv.at[which, team], dev,
        )

    def strips_in(d, which):
        q, dev = member(d)
        ref, near = ((h_ref, near_h), (p_ref, near_p))[which]
        return remote(
            ref.at[:, in_strip(q), :], near.at[pl.ds(q * slots, slots)],
            s_send.at[which, d], s_recv.at[which, q], dev,
        )

    for which in range(2):
        for d in range(1, sh.team):
            strips(d, which).start()

    def other(dc):
        c = (chip + dc) % sh.chips
        return c, c * 2 + core

    p_mate = remote(p_ref, prow.at[pl.ds(slots, slots)], p_send.at[0], p_recv.at[sh.cols], mate)
    p_mate.start()

    def p_block(col):
        return prow.at[pl.ds(sh.others + col * CAP_R, CAP_R)]

    def p_out(dc):
        return remote(pack_r.at[dc - 1], p_block(j), p_send.at[dc], p_recv.at[j], (i, other(dc)[1]))

    def p_in(dc):
        col = other(dc)[1]
        return remote(pack_r.at[dc - 1], p_block(col), p_send.at[dc], p_recv.at[col], (i, col))

    def p_forward(dc):
        col = other(dc)[1]
        return remote(p_block(col), p_block(col), p_fwd.at[dc], p_recv.at[col], mate)

    def p_forward_in(dc):
        col = other(dc)[0] * 2 + 1 - core
        return remote(p_block(col), p_block(col), p_fwd.at[dc], p_recv.at[col], mate)

    def bulk(ref, sem):
        part = ref.at[pl.ds(0, all_but_me)]
        return pltpu.make_async_copy(part, part, sem)

    bulk(messages, m_recv).wait()
    lists = Lists(sh, x, z, j, messages[:, 0, :])

    def publish(source, target, which):
        copy = pltpu.make_async_copy(source, target, t_copy.at[which])
        copy.start()
        copy.wait()

    def entry(ref, table, row, lane):
        return ref[jnp.minimum(jnp.maximum(table[row, lane], 0), ref.shape[0] - 1)]

    kinds = (
        (store_h, pack_hz, pack_h, land_h, CAP_H_Z, CAP_H, near_h, tab_h),
        (store_p, pack_pz, pack_p, land_p, CAP_P_Z, CAP_P, near_p, tab),
    )

    def zone(which, layer):
        store, cap = kinds[which][0], kinds[which][4]
        return store.at[pl.ds(sh.team * slots + layer * cap, cap)]

    def across(which, dz):
        pack = kinds[which][1]
        zd = (z + dz) % sh.outer
        return remote(
            pack.at[dz - 1], zone(which, z), z_send.at[which, dz], z_recv.at[which, z],
            (zd * sh.inner + x, j),
        )

    def across_in(which, dz):
        pack = kinds[which][1]
        zs = (z + dz) % sh.outer
        return remote(
            pack.at[dz - 1], zone(which, zs), z_send.at[which, dz], z_recv.at[which, zs],
            (zs * sh.inner + x, j),
        )

    def part(which, d):
        pack, land = kinds[which][2], kinds[which][3]
        _, dev = member(d)
        return remote(
            pack.at[d - 1], land.at[:, in_strip(team), :], t_send.at[which, d], t_recv.at[which, team], dev
        )

    def part_in(which, d):
        pack, land = kinds[which][2], kinds[which][3]
        q, dev = member(d)
        return remote(
            pack.at[d - 1], land.at[:, in_strip(q), :], t_send.at[which, d], t_recv.at[which, q], dev
        )

    def send_across(which):
        store, pack, _, _, cap, _, near, _ = kinds[which]
        for d in range(1, sh.team):
            strips_in(d, which).wait_recv()
        for dz in range(1, sh.outer):
            for k in range(cap):
                pack[dz - 1, k] = entry(near, tab_z, which, (dz - 1) * LIST_Z + k)
        for dz in range(1, sh.outer):
            across(which, dz).start()
        store[0 : sh.team * slots] = near[...]

    def send_parts(which):
        store, _, pack, land, _, cap, _, table = kinds[which]
        for dz in range(1, sh.outer):
            across_in(which, dz).wait_recv()

        @pl.loop(1, sh.team)
        def _(d):
            q, _ = member(d)
            for k in range(cap):
                pack[d - 1, k] = entry(store, table, 0, q * LIST + k)

        for d in range(1, sh.team):
            part(which, d).start()
        for k in range(cap):
            land[k, in_strip(team), :] = entry(store, table, 0, team * LIST + k)

    over = lists.across(tabv_z)
    publish(tabv_z, tab_z, 0)
    send_across(0)
    over = over + lists.row_lists(tabv_r)
    publish(tabv_r, tab_r, 1)
    for dc in range(1, sh.chips):
        for k in range(CAP_R):
            pack_r[dc - 1, k] = entry(p_ref, tab_r, 0, (dc - 1) * EIGHT + k)
    for dc in range(1, sh.chips):
        p_out(dc).start()
    over = over + lists.team_lists(0, tabv_h)
    publish(tabv_h, tab_h, 2)
    send_across(1)
    send_parts(0)
    over = over + lists.team_lists(1, tabv)
    over = over + lists.products(pw, pc, tabv)
    publish(tabv, tab, 3)
    for dc in range(1, sh.chips):
        p_in(dc).wait_recv()
        p_forward(dc).start()
    send_parts(1)

    def multiply(step, left, right, terms, cap):
        row = 2 + step
        acc = None
        for k in range(cap):
            d = jnp.dot(entry(left, tab, row, k), entry(right, tab, row, 32 + k), preferred_element_type=F32)
            acc = d if acc is None else d + acc * tab[row, 64 + k].astype(F32)
            terms[k] = acc
        terms[cap] = jnp.zeros((size, size), F32)

    p_mate.wait_recv()
    for dc in range(1, sh.chips):
        p_forward_in(dc).wait_recv()
    for d in range(1, sh.team):
        part_in(0, d).wait_recv()
    multiply(0, prow, land_h, terms_1, CAP_1)
    trace = jnp.zeros((size, size), F32)
    for s in range(slots):
        value = entry(terms_1, tab, 2, 96 + s)
        trace = trace + value * jnp.where(pw[0, s] == pw[1, s], 1.0, 0.0)
        rounded = value.astype(BF16)
        fstore[s] = rounded
        out[s] = rounded

    for k in range(CAP_V):
        fstore[slots + k] = entry(terms_1, tab, 2, 96 + LIST + k).astype(BF16)

    diagonal = iota((size, size), 0) == iota((size, size), 1)
    emsg[0, 0] = jnp.sum(jnp.where(diagonal, trace, 0.0), axis=0, keepdims=True)
    emsg[0, 1] = over + jnp.zeros((1, 128), F32)
    emsgs[me] = emsg[0]

    def tell_energy(d):
        return remote(emsg.at[pl.ds(0, 1)], emsgs.at[pl.ds(me, 1)], e_send, e_recv, device(d))

    @pl.loop(1, sh.devices)
    def _(d):
        tell_energy(d).start()

    for d in range(1, sh.team):
        part_in(1, d).wait_recv()
    multiply(1, fstore, land_p, terms_2, CAP_2)
    for s in range(slots):
        out[slots + s] = entry(terms_2, tab, 3, 96 + s).astype(BF16)

    bulk(emsgs, e_recv).wait()
    e_out[0, 0] = jnp.sum(jnp.sum(emsgs[:, 0], axis=0))
    over_out[0, 0] = jnp.sum(jnp.sum(emsgs[:, 1], axis=0))

    bulk(messages, m_send).wait()
    bulk(emsgs, e_send).wait()
    for which in range(2):
        for d in range(1, sh.team):
            strips(d, which).wait_send()
            part(which, d).wait_send()
        for dz in range(1, sh.outer):
            across(which, dz).wait_send()
    p_mate.wait_send()
    for dc in range(1, sh.chips):
        p_out(dc).wait_send()
        p_forward(dc).wait_send()


def sparse_path(sh, p_values, p_where, p_count, h_values, h_where, h_count):
    slots, size, strip = sh.slots, sh.size, sh.strip
    block, piece = (size, size), (strip, size)
    bf = lambda *shape: pltpu.VMEM(shape, BF16)
    f32 = lambda *shape: pltpu.VMEM(shape, F32)
    dma = pltpu.SemaphoreType.DMA
    near = sh.team * slots
    away = max(sh.outer - 1, 1)
    chips = max(sh.chips - 1, 1)
    scalar = jax.ShapeDtypeStruct((1, 1), F32)
    return pl.pallas_call(
        functools.partial(sparse_products, sh),
        out_shape=[jax.ShapeDtypeStruct((2 * slots,) + block, BF16), scalar, scalar],
        in_specs=[ANY] * 6,
        out_specs=[VMEM, SMEM, SMEM],
        scratch_shapes=[
            bf(slots, *block),
            bf(slots, *block),
            pltpu.SMEM((2, slots), I32),
            pltpu.SMEM((1, 1), I32),
            pltpu.SMEM((2, slots), I32),
            pltpu.SMEM((1, 1), I32),
            f32(1, 1, 128),
            f32(sh.devices, 1, 128),
            bf(near, *piece),
            bf(near, *piece),
            bf(near + sh.outer * CAP_H_Z, *piece),
            bf(near + sh.outer * CAP_P_Z, *piece),
            bf(sh.others + sh.cols * CAP_R, *block),
            bf(chips, CAP_R, *block),
            bf(away, CAP_H_Z, *piece),
            bf(away, CAP_P_Z, *piece),
            bf(sh.team, CAP_H, *piece),
            bf(sh.team, CAP_P, *piece),
            bf(CAP_H, *block),
            bf(CAP_P, *block),
            f32(CAP_1 + 1, *block),
            f32(CAP_2 + 1, *block),
            bf(slots + CAP_V, *block),
            pltpu.VMEM((8, 128), I32),
            pltpu.VMEM((8, 128), I32),
            pltpu.VMEM((8, 128), I32),
            pltpu.VMEM((8, 128), I32),
            pltpu.SMEM((8, 128), I32),
            pltpu.SMEM((8, 128), I32),
            pltpu.SMEM((8, 128), I32),
            pltpu.SMEM((8, 128), I32),
            f32(1, 2, 1, 128),
            f32(sh.devices, 2, 1, 128),
            dma, dma,
            dma((2, sh.team)), dma((2, sh.team)),
            dma((sh.chips,)), dma((sh.chips,)), dma((sh.cols + 1,)),
            dma((2, sh.outer)), dma((2, sh.outer)),
            dma((2, sh.team)), dma((2, sh.team)),
            dma, dma, dma((4,)), dma((6,)),
        ],
        compiler_params=pltpu.CompilerParams(collective_id=2, has_side_effects=True, vmem_limit_bytes=24 << 20),
        name="sparse_products",
    )(p_values, h_values, p_where.T, p_count, h_where.T, h_count)


def deliver(both):
    def kernel(both_ref, first, second, sems):
        slots = first.shape[0]
        copies = [
            pltpu.make_async_copy(both_ref.at[pl.ds(k * slots, slots)], ref, sems.at[k])
            for k, ref in enumerate((first, second))
        ]
        for copy in copies:
            copy.start()
        for copy in copies:
            copy.wait()

    half = jax.ShapeDtypeStruct((both.shape[0] // 2,) + both.shape[1:], both.dtype)
    return pl.pallas_call(
        kernel,
        out_shape=[half, half],
        in_specs=[VMEM],
        out_specs=[ANY, ANY],
        scratch_shapes=[pltpu.SemaphoreType.DMA((2,))],
        name="deliver",
    )(both)


def per_device(rows, cols, *args):
    slots, size, _ = args[0].shape
    sh = Shape(rows, cols, slots, size)
    if not sh.fits():
        return dense_path(rows, cols, *args)
    both, energy, over = sparse_path(sh, *args)
    return lax.cond(
        over[0, 0] > 0.0,
        lambda: dense_path(rows, cols, *args),
        lambda: (*deliver(both), energy[0, 0]),
    )


def solution(mesh):
    placed = (
        P("row", "col", None),
        P("row", "col"),
        P("row", "col"),
        P("row", "col", None),
        P("row", "col"),
        P("row", "col"),
    )
    return jax.shard_map(
        functools.partial(per_device, mesh.shape["row"], mesh.shape["col"]),
        mesh=mesh,
        in_specs=placed,
        out_specs=(P("row", "col", None), P("row", "col", None), P()),
        check_vma=False,
    )
```

```python
import functools

import jax
import jax.numpy as jnp
from jax import lax
from jax.experimental import pallas as pl
from jax.experimental.pallas import tpu as pltpu
from jax.sharding import PartitionSpec as P

TILE = 8
CHUNKS = 6
IN_FLIGHT = 16
MESH = pl.DeviceIdType.MESH
ANY = pl.BlockSpec(memory_space=pl.ANY)
VMEM = pl.BlockSpec(memory_space=pltpu.VMEM)
SMEM = pl.BlockSpec(memory_space=pltpu.SMEM)


def at_row(r):
    return (r, lax.axis_index("col"))


def at_col(c):
    return (lax.axis_index("row"), c)


def remote(src, dst, send_sem, recv_sem, device):
    return pltpu.make_async_remote_copy(
        src_ref=src,
        dst_ref=dst,
        send_sem=send_sem,
        recv_sem=recv_sem,
        device_id=device,
        device_id_type=MESH,
    )


def greet(rows, cols):
    me_row, me_col = lax.axis_index("row"), lax.axis_index("col")
    barrier = pltpu.get_barrier_semaphore()
    for d in range(1, rows):
        pl.semaphore_signal(
            barrier, inc=1, device_id=at_row((me_row + d) % rows), device_id_type=MESH
        )
    for d in range(1, cols):
        pl.semaphore_signal(
            barrier, inc=1, device_id=at_col((me_col + d) % cols), device_id_type=MESH
        )
    pl.semaphore_wait(barrier, rows + cols - 2)


class ColumnGather:
    def __init__(self, rows, own, land, out, up_send, down_send, x_send, recv, local):
        self.own, self.land, self.out = own, land, out
        self.up_send, self.down_send, self.x_send = up_send, down_send, x_send
        self.recv, self.local = recv, local
        self.inner = 2 if rows % 2 == 0 else 1
        self.outer = rows // self.inner
        self.chunks = recv.shape[1]
        self.size = own.shape[0] // self.chunks
        self.me = lax.axis_index("row")
        self.x, self.z = self.me % self.inner, self.me // self.inner
        self.cross_first = 1 if self.inner == 2 and self.chunks > 1 else 0

    def later(self, ch):
        return (ch + self.cross_first) % self.chunks

    def row(self, z, line):
        return z * self.inner + (self.x if line == 0 else self.inner - 1 - self.x)

    def part(self, ch):
        return pl.ds(ch * self.size, self.size)

    def copy(self, r, ch, own, way):
        sems, target = {
            "up": (self.up_send, self.me + self.inner),
            "down": (self.down_send, self.me - self.inner),
            "x": (self.x_send, self.row(self.z, 1)),
        }[way]
        part = self.part(ch)
        src = self.own.at[part] if own else self.land.at[r, part]
        return remote(src, self.land.at[r, part], sems.at[r, ch], self.recv.at[r, ch], at_row(target))

    def keep(self, r, ch):
        part = self.part(ch)
        return pltpu.make_async_copy(self.land.at[r, part], self.out.at[r, part], self.local.at[r, ch])

    def along(self, r, ch, own, act):
        @pl.when(self.z < self.outer - 1)
        def _():
            act(self.copy(r, ch, own, "up"))

        @pl.when(self.z > 0)
        def _():
            act(self.copy(r, ch, own, "down"))

    def arrive(self, r, ch):
        self.copy(r, ch, False, "x").wait_recv()
        self.keep(r, ch).start()

    def start(self):
        for ch in range(self.chunks):
            if self.inner == 2:
                self.copy(self.me, ch, True, "x").start()
            self.along(self.me, self.later(ch), True, lambda copy: copy.start())
        if self.cross_first:
            r = self.row(self.z, 1)
            self.arrive(r, 0)
            self.along(r, 0, False, lambda copy: copy.start())

    def pieces(self):
        lines = [(self.later(ch), 0) for ch in range(self.chunks)]
        return lines + [(0, 1)] * self.cross_first

    def relayed(self, d, side, ch, line, act):
        z = self.z - d if side == 0 else self.z + d
        there = self.z >= d if side == 0 else self.z + d < self.outer
        r = self.row(z, line)

        @pl.when(there)
        def _():
            if act == "start":
                self.arrive(r, ch)
            on = self.z < self.outer - 1 if side == 0 else self.z > 0

            @pl.when(on)
            def _():
                copy = self.copy(r, ch, False, "up" if side == 0 else "down")
                copy.start() if act == "start" else copy.wait_send()

            if self.inner == 2 and ch >= self.cross_first:
                copy = self.copy(r, ch, False, "x")
                copy.start() if act == "start" else copy.wait_send()

    def relay(self, d):
        for ch, line in self.pieces():
            for side in range(2):
                self.relayed(d, side, ch, line, "start")

    def finish(self):
        if self.inner == 2:
            for ch in range(self.cross_first, self.chunks):
                self.arrive(self.row(self.z, 1), ch)
            for d in range(1, self.outer):
                for side in range(2):
                    z = self.z - d if side == 0 else self.z + d
                    there = self.z >= d if side == 0 else self.z + d < self.outer

                    @pl.when(there)
                    def _():
                        for ch in range(self.cross_first, self.chunks):
                            self.arrive(self.row(z, 1), ch)
        for ch in range(self.chunks):
            if self.inner == 2:
                self.copy(self.me, ch, True, "x").wait_send()
            self.along(self.me, ch, True, lambda copy: copy.wait_send())
        if self.cross_first:
            self.along(self.row(self.z, 1), 0, False, lambda copy: copy.wait_send())
        for d in range(1, self.outer):
            for ch, line in self.pieces():
                for side in range(2):
                    self.relayed(d, side, ch, line, "wait")
        for r in range(self.inner * self.outer):
            @pl.when(r != self.me)
            def _():
                for ch in range(self.chunks):
                    self.keep(r, ch).wait()


def col_copies(cols, own, out, send, recv):
    me = lax.axis_index("col")
    made = []
    for d in range(1, cols):
        made.append(
            remote(own, out.at[me], send.at[d], recv.at[d], at_col((me + d) % cols))
        )
    return made


def row_copies(rows, own, out, send, recv):
    me = lax.axis_index("row")
    made = []
    for d in range(1, rows):
        made.append(
            remote(own, out.at[me], send.at[d], recv.at[d], at_row((me + d) % rows))
        )
    return made


def first_gather(
    rows, cols, p_ref, h_ref, meta_ref, prow, hcol, prow_meta, col_meta,
    land, up_send, down_send, x_send, recv, out_sems,
    p_send, p_recv, mc_send, mc_recv, mr_send, mr_recv, local,
):
    me_row, me_col = lax.axis_index("row"), lax.axis_index("col")
    keep = [
        pltpu.make_async_copy(h_ref, hcol.at[me_row], local.at[0]),
        pltpu.make_async_copy(p_ref, prow.at[me_col], local.at[1]),
        pltpu.make_async_copy(meta_ref, prow_meta.at[me_col], local.at[2]),
        pltpu.make_async_copy(meta_ref, col_meta.at[me_row], local.at[3]),
    ]
    greet(rows, cols)
    gather = ColumnGather(
        rows, h_ref, land, hcol, up_send, down_send, x_send, recv, out_sems
    )
    across = (
        col_copies(cols, p_ref, prow, p_send, p_recv)
        + col_copies(cols, meta_ref, prow_meta, mc_send, mc_recv)
        + row_copies(rows, meta_ref, col_meta, mr_send, mr_recv)
    )
    for copy in across + keep:
        copy.start()
    gather.start()
    for d in range(1, gather.outer):
        gather.relay(d)
    gather.finish()
    for copy in across + keep:
        copy.wait()


def second_gather(
    rows, cols, p_ref, f_ref, e_ref, frow, pcol, e_out,
    e_cols, e_rows, e_sum,
    land, up_send, down_send, x_send, recv, out_sems,
    p_send, p_recv, ec_send, ec_recv, er_send, er_recv, local,
):
    me_row, me_col = lax.axis_index("row"), lax.axis_index("col")
    keep = [
        pltpu.make_async_copy(p_ref, pcol.at[me_row], local.at[0]),
        pltpu.make_async_copy(f_ref, frow.at[me_col], local.at[1]),
    ]
    greet(rows, cols)
    energies = col_copies(cols, e_ref, e_cols, ec_send, ec_recv)
    for copy in energies:
        copy.start()
    gather = ColumnGather(
        rows, p_ref, land, pcol, up_send, down_send, x_send, recv, out_sems
    )
    across = col_copies(cols, f_ref, frow, p_send, p_recv)
    for copy in across + keep:
        copy.start()
    gather.start()
    e_cols[me_col] = e_ref[...]
    for copy in energies:
        copy.wait()
    total = e_cols[0]
    for c in range(1, cols):
        total = total + e_cols[c]
    e_sum[...] = total
    e_rows[me_row] = total
    if gather.outer > 1:
        gather.relay(1)
    sums = row_copies(rows, e_sum, e_rows, er_send, er_recv)
    for copy in sums:
        copy.start()
    for d in range(2, gather.outer):
        gather.relay(d)
    for copy in sums:
        copy.wait()
    total = e_rows[0]
    for r in range(1, rows):
        total = total + e_rows[r]
    e_out[...] = total
    gather.finish()
    for copy in across + keep:
        copy.wait()


def block_products(
    rows, cols, right_lane, with_trace, lmeta, rmeta, left, right, *rest
):
    if with_trace:
        out, e_out = rest[:2]
    else:
        e_in, out, e_out = rest[:3]
    acc, lbuf, rbuf, head, nxt, inner, mask, table, ml, mr, ms, sems = rest[-12:]
    slots = out.shape[0]
    i, j = lax.axis_index("row"), lax.axis_index("col")
    nblk = rows * TILE
    tile_cols = nblk // cols
    words = -(-nblk // 32)
    count_lane = 4 * slots
    acc[...] = jnp.zeros_like(acc)

    for t in range(TILE + 1):
        head[t] = -1

    for t in range(tile_cols * words + 1):
        mask[t] = 0

    @pl.loop(0, cols)
    def _(c):
        live = lmeta[c, 0, count_lane]
        for s in range(slots):
            row = jnp.where(s < live, lmeta[c, 0, s] - i * TILE, TILE)
            idx = c * slots + s
            inner[idx] = lmeta[c, 0, slots + s]
            nxt[idx] = head[row]
            head[row] = idx

    @pl.loop(0, rows)
    def _(r):
        live = rmeta[r, 0, count_lane + (1 if right_lane else 0)]
        for s in range(slots):
            k = rmeta[r, 0, right_lane + s]
            col = rmeta[r, 0, right_lane + slots + s] - j * tile_cols
            word = jnp.where(s < live, col * words + (k >> 5), tile_cols * words)
            mask[word] = mask[word] | (jnp.int32(1) << (k & 31))
            table[jnp.where(s < live, k * tile_cols + col, nblk * tile_cols)] = r * slots + s

    def find_slot(s, n):
        row = lmeta[j, 0, s] - i * TILE
        col = lmeta[j, 0, slots + s] - j * tile_cols

        def more(state):
            return state[0] >= 0

        def step(state):
            at, n = state
            k = inner[at]
            ml[n] = at
            mr[n] = table[k * tile_cols + col]
            ms[n] = s
            return nxt[at], n + ((mask[col * words + (k >> 5)] >> (k & 31)) & 1)

        return lax.while_loop(more, step, (head[row], n))[1]

    own_count = lmeta[j, 0, count_lane]
    found = lax.fori_loop(0, own_count, find_slot, jnp.int32(0))

    def fetch(base, m):
        a, b = ml[base + m], mr[base + m]
        return (
            pltpu.make_async_copy(left.at[a], lbuf.at[m], sems.at[0, m]),
            pltpu.make_async_copy(right.at[b], rbuf.at[m], sems.at[1, m]),
        )

    @pl.loop(0, (found + IN_FLIGHT - 1) // IN_FLIGHT)
    def _(chunk):
        base = chunk * IN_FLIGHT
        size = jnp.minimum(found - base, IN_FLIGHT)

        @pl.loop(0, size)
        def _(m):
            for copy in fetch(base, m):
                copy.start()

        @pl.loop(0, size)
        def _(m):
            for copy in fetch(base, m):
                copy.wait()
            s = ms[base + m]
            acc[s] += jnp.dot(lbuf[m], rbuf[m], preferred_element_type=jnp.float32)

    out[...] = acc[...].astype(out.dtype)
    if with_trace:
        size = acc.shape[1]
        e_out[...] = jnp.zeros_like(e_out)
        diagonal = lax.broadcasted_iota(jnp.int32, (size, size), 0) == lax.broadcasted_iota(
            jnp.int32, (size, size), 1
        )

        @pl.loop(0, own_count)
        def _(s):
            @pl.when(lmeta[j, 0, s] == lmeta[j, 0, slots + s])
            def _():
                e_out[...] += jnp.sum(jnp.where(diagonal, acc[s], 0.0))
    else:
        e_out[0, 0] = e_in[0, 0]


def dense_path(rows, cols, p_values, p_where, p_count, h_values, h_where, h_count):
    slots, size, _ = p_values.shape
    dtype = p_values.dtype
    nblk = rows * TILE
    tile_cols = nblk // cols
    words = -(-nblk // 32)
    meta = jnp.concatenate(
        [p_where[:, 0], p_where[:, 1], h_where[:, 0], h_where[:, 1], p_count[0], h_count[0]]
    )
    meta = jnp.broadcast_to(jnp.pad(meta, (0, 128 - meta.shape[0]))[None, :], (8, 128))
    dma = pltpu.SemaphoreType.DMA
    chunks = CHUNKS if slots % CHUNKS == 0 else 1
    chunk_sems = [pltpu.VMEM((rows, slots, size, size), dtype)] + [dma((rows, chunks))] * 5
    col_sems = [dma((cols,)), dma((cols,))]
    row_sems = [dma((rows,)), dma((rows,))]
    tile = (slots, size, size)
    prow, hcol, prow_meta, col_meta = pl.pallas_call(
        functools.partial(first_gather, rows, cols),
        out_shape=[
            jax.ShapeDtypeStruct((cols,) + tile, dtype),
            jax.ShapeDtypeStruct((rows,) + tile, dtype),
            jax.ShapeDtypeStruct((cols, 8, 128), jnp.int32),
            jax.ShapeDtypeStruct((rows, 8, 128), jnp.int32),
        ],
        in_specs=[VMEM] * 3,
        out_specs=[ANY] * 4,
        scratch_shapes=chunk_sems + col_sems + col_sems + row_sems + [dma((4,))],
        compiler_params=pltpu.CompilerParams(collective_id=0, has_side_effects=True),
        name="first_gather",
    )(p_values, h_values, meta)

    def products(right_lane, with_trace, lmeta, rmeta, left, right, *more):
        smem = lambda n: pltpu.SMEM((n,), jnp.int32)
        most = slots * nblk + 1
        return pl.pallas_call(
            functools.partial(block_products, rows, cols, right_lane, with_trace),
            out_shape=[
                jax.ShapeDtypeStruct(tile, dtype),
                jax.ShapeDtypeStruct((8, 128) if with_trace else (1, 1), jnp.float32),
            ],
            in_specs=[SMEM, SMEM, ANY, ANY] + [SMEM] * len(more),
            out_specs=[VMEM, VMEM if with_trace else SMEM],
            scratch_shapes=[
                pltpu.VMEM(tile, jnp.float32),
                pltpu.VMEM((IN_FLIGHT, size, size), dtype),
                pltpu.VMEM((IN_FLIGHT, size, size), dtype),
                smem(TILE + 1),
                smem(cols * slots),
                smem(cols * slots),
                smem(tile_cols * words + 1),
                smem(nblk * tile_cols + 1),
                smem(most),
                smem(most),
                smem(most),
                dma((2, IN_FLIGHT)),
            ],
            name="products",
        )(
            lmeta,
            rmeta,
            left.reshape((cols * slots, size, size)),
            right.reshape((rows * slots, size, size)),
            *more,
        )

    ph_values, part = products(2 * slots, True, prow_meta, col_meta, prow, hcol)
    frow, pcol, energy = pl.pallas_call(
        functools.partial(second_gather, rows, cols),
        out_shape=[
            jax.ShapeDtypeStruct((cols,) + tile, dtype),
            jax.ShapeDtypeStruct((rows,) + tile, dtype),
            jax.ShapeDtypeStruct((8, 128), jnp.float32),
        ],
        in_specs=[VMEM] * 3,
        out_specs=[ANY, ANY, VMEM],
        scratch_shapes=[
            pltpu.VMEM((cols, 8, 128), jnp.float32),
            pltpu.VMEM((rows, 8, 128), jnp.float32),
            pltpu.VMEM((8, 128), jnp.float32),
        ]
        + chunk_sems + col_sems + col_sems + row_sems + [dma((2,))],
        compiler_params=pltpu.CompilerParams(collective_id=1, has_side_effects=True),
        name="second_gather",
    )(p_values, ph_values, part)
    php_values, energy = products(0, False, prow_meta, col_meta, frow, pcol, energy)
    return (ph_values, php_values, energy[0, 0])


CAP_H_Z, CAP_P_Z = 17, 12
CAP_H, CAP_P = 14, 9
CAP_R, CAP_V, CAP_D = 7, 7, 3
CAP_1, CAP_2 = 18, 12
LIST, LIST_Z, LIST_1, EIGHT = 16, 24, 24, 8
F32, BF16, I32 = jnp.float32, jnp.bfloat16, jnp.int32


def log2(n):
    return n.bit_length() - 1


def power(n):
    return n > 0 and n & (n - 1) == 0


class Shape:
    def __init__(self, rows, cols, slots, size):
        self.rows, self.cols, self.slots, self.size = rows, cols, slots, size
        self.devices = rows * cols
        self.nblk = rows * TILE
        self.inner = 2 if rows % 2 == 0 else 1
        self.outer = rows // self.inner
        self.layer = self.inner * TILE
        self.team = self.inner * cols
        self.strip = size // self.team
        self.width = self.nblk // cols
        self.chips = cols // 2
        self.others = 2 * slots

    def trace_member(self, z, xd):
        return xd * self.cols + (z * self.inner + xd) * TILE // self.width

    def layer_at(self, z, t):
        down = self.outer - 1 - t
        return jnp.where(
            z < self.outer // 2,
            down - jnp.where(down <= z, 1, 0),
            t + jnp.where(t >= z, 1, 0),
        )

    def fits(self):
        return (
            power(self.rows)
            and power(self.cols)
            and self.cols >= 2
            and self.outer >= 2
            and self.nblk <= 64
            and TILE <= self.width <= 128 // TILE
            and self.slots <= 15
            and self.strip % 16 == 0
            and self.team * LIST <= 128
            and (self.outer - 1) * LIST_Z <= 128
            and (self.chips - 1) * EIGHT <= 128
        )


def mm(a, b):
    return lax.dot_general(a.astype(BF16), b.astype(BF16), (((1,), (0,)), ((), ())), preferred_element_type=F32)


def mt(a, b):
    return lax.dot_general(a.astype(BF16), b.astype(BF16), (((1,), (1,)), ((), ())), preferred_element_type=F32)


def tm(a, b):
    return lax.dot_general(a.astype(BF16), b.astype(BF16), (((0,), (0,)), ((), ())), preferred_element_type=F32)


def ones(cond):
    return jnp.where(cond, 1.0, 0.0).astype(F32)


def iota(shape, dim):
    return lax.broadcasted_iota(I32, shape, dim)


def block_index(shape, dim, size):
    return iota(shape, dim) // size


def total_over(ends, cap):
    over = ones(ends > cap + 0.5)
    return jnp.sum(jnp.sum(over, axis=0, keepdims=True), axis=1, keepdims=True)


def stack(parts):
    return jnp.concatenate(parts, axis=0)


class Lists:
    def __init__(self, sh, x, z, j, message):
        self.sh, self.x, self.z, self.j = sh, x, z, j
        n, width, layer = sh.nblk, sh.width, sh.layer
        lw = log2(width)
        r, l = iota((n, n), 0), iota((n, n), 1)
        a0, d0 = iota((sh.cols * n, sh.devices), 0), iota((sh.cols * n, sh.devices), 1)
        spread = mm(ones(d0 == ((a0 & (n - 1)) >> 3) * sh.cols + (a0 >> log2(n))), message)
        a1, l1 = iota((sh.cols * n, 128), 0), iota((sh.cols * n, 128), 1)
        spread = jnp.where((l1 >> lw) == (a1 & 7), spread, 0.0)
        l2, m2 = iota((128, n), 0), iota((128, n), 1)
        spread = mm(spread, ones((l2 & (width - 1)) == (m2 & (width - 1))))
        both = jnp.zeros((n, n), F32)
        for c in range(sh.cols):
            both = both + jnp.where((l >> lw) == c, spread[c * n : (c + 1) * n], 0.0)
        hs = jnp.floor(both * (1.0 / 16.0))
        ps = both - 16.0 * hs
        self.pos = {}
        self.pm, self.hm = ones(ps > 0.5), ones(hs > 0.5)
        self.fm = self.pm * ones(mm(self.pm, self.hm) > 0.5)
        self.up, self.low, self.up_to = ones(r < l), ones(l < r), ones(r <= l)
        self.low_layer = ones((l < r) & (l // layer == r // layer))
        self.full = jnp.ones((n, n), F32)
        self.r, self.l, self.lane_tile = r, l, l >> lw
        team = ((r >> 3) & (sh.inner - 1)) * sh.cols + self.lane_tile
        at = (team * sh.slots).astype(F32)
        self.near = {"H": at + hs - 1.0, "P": at + ps - 1.0}
        s0, s1 = iota((layer, n), 0), iota((layer, n), 1)
        self.sel = ones(s1 == z * layer + s0)
        self.row_i, self.row_tile = s0, (s1 >> lw)
        self.p_layer, self.f_layer = mm(self.sel, self.pm), mm(self.sel, self.fm)
        self.slot_layer = mm(self.sel, ps) - 1.0

    def enumerate(self, v, count, lane_pos=None):
        k, n = v.shape
        counts = mt(jnp.ones((count, n), F32), v)
        a, b = iota((k, k), 0), iota((k, k), 1)
        starts, ends = mm(counts, ones(a < b)), mm(counts, ones(a <= b))
        at = iota((count, k), 0).astype(F32)
        rows = ones((starts <= at) & (at < ends))
        local = mm(rows * (at - starts + 1.0), jnp.ones((k, n), F32))
        if lane_pos is None:
            lane_pos = mm(v, self.up)
        found = mm(rows, v * (lane_pos + 1.0))
        lanes = ones((found == local) & (local > 0.5))
        return rows, lanes, starts, ends, lane_pos

    def position(self, v, low):
        return mm(v, self.up) + mm(low, mm(v, self.full))

    def across(self, tab):
        sh, z, layer, n = self.sh, self.z, self.sh.layer, self.sh.nblk
        p_s, f_s = mt(self.sel, self.pm), mt(self.sel, self.fm)
        i_layer = self.l[0:layer] // layer
        lhs, live, pay = [], [], []
        for kind, left, right in (("H", p_s, self.hm), ("P", f_s, self.pm)):
            live_kind, pay_kind = mm(self.sel, right), mm(self.sel, self.near[kind])
            for dz in range(1, sh.outer):
                lhs.append(left * ones(i_layer == sh.layer_at(z, dz - 1)))
                live.append(live_kind)
                pay.append(pay_kind)
        v = ones(mm(stack(lhs), self.pm) > 0.5) * stack(live)
        k = v.shape[0]
        lists = 2 * (sh.outer - 1)
        a, b = iota((k, k), 0), iota((k, k), 1)
        counts = mt(jnp.ones((EIGHT, n), F32), v)
        starts = mm(counts, ones((a < b) & (a // layer == b // layer)))
        ends = mm(counts, ones((a <= b) & (a // layer == b // layer)))
        t0 = iota((lists * LIST_Z, k), 0)
        at = (t0 % LIST_Z).astype(F32)
        rows = ones(
            (starts[0:1] <= at)
            & (at < ends[0:1])
            & (t0 // LIST_Z == block_index((lists * LIST_Z, k), 1, layer))
        )
        local = mm(rows * (at - starts[0:1] + 1.0), jnp.ones((k, n), F32))
        found = mm(rows, v * (mm(v, self.up) + 1.0))
        picked = jnp.where((found == local) & (local > 0.5), mm(rows, stack(pay)), 0.0)
        half = (sh.outer - 1) * LIST_Z
        for which in range(2):
            line = mt(jnp.ones((EIGHT, n), F32), picked[which * half : (which + 1) * half])
            tab[which : which + 1, 0:half] = line[0:1].astype(I32)
        lane_h = block_index((EIGHT, k), 1, layer) < sh.outer - 1
        cap = jnp.where(lane_h, 1.0 * CAP_H_Z, 1.0 * CAP_P_Z)
        return total_over(ends - cap, 0.0)

    def row_lists(self, tab):
        sh, x, j, layer, n = self.sh, self.x, self.j, self.sh.layer, self.sh.nblk
        tiles = [ones(self.row_tile == c) for c in range(sh.cols)]
        wide = stack([self.p_layer * t for t in tiles])
        passed = ones(mt(wide, self.pm) > 0.5) * stack([self.f_layer] * sh.cols)
        own = wide
        self.outputs = jnp.maximum(own, passed)
        self.remote_f = passed * (1.0 - ones(stack([t for t in tiles]) > 0.5))
        reads = ones(mt(self.outputs, self.hm) > 0.5) * stack([self.p_layer] * sh.cols)
        mine = ones((self.row_i >> 3) == x)
        chip = j // 2
        low = ones(iota((layer, layer), 1) < iota((layer, layer), 0))
        seg_tri = ones((self.lane_tile == (self.r >> log2(sh.width))) & (self.r < self.l))
        seg_full = ones(self.lane_tile == (self.r >> log2(sh.width)))
        over = jnp.zeros((1, 1), F32)
        for dc in range(sh.chips):
            c = (chip + dc) % sh.chips
            v = jnp.zeros((layer, n), F32)
            for k in range(sh.cols):
                v = jnp.maximum(v, reads[k * layer : (k + 1) * layer] * jnp.where(k // 2 == c, 1.0, 0.0))
            v = v * mine
            if dc == 0:
                pos = mm(v, seg_tri) + mm(low, mm(v, seg_full))
                pos = jnp.minimum(pos, CAP_R - 1.0)
                continue
            v = v * ones(self.row_tile == j)
            rows, lanes, starts, ends, _ = self.enumerate(v, EIGHT)
            line = mt(jnp.ones((EIGHT, n), F32), lanes * mm(rows, self.slot_layer))
            tab[0:1, (dc - 1) * EIGHT : dc * EIGHT] = line[0:1].astype(I32)
            over = over + total_over(ends, CAP_R)
        self.left_1 = jnp.where(
            self.row_tile == j,
            self.slot_layer,
            jnp.where(
                self.row_tile // 2 == chip,
                sh.slots + self.slot_layer,
                sh.others + self.row_tile.astype(F32) * CAP_R + pos,
            ),
        )
        return over

    def team_lists(self, which, tab):
        sh, x, z, j, layer, n = self.sh, self.x, self.z, self.j, self.sh.layer, self.sh.nblk
        a, b = iota((layer, layer), 0), iota((layer, layer), 1)
        turn = lambda m: tm(m, ones(a == b))
        kind, cap_z, cap = (("H", CAP_H_Z, CAP_H), ("P", CAP_P_Z, CAP_P))[which]
        turned = turn(self.p_layer if kind == "H" else self.f_layer)
        live = self.hm if kind == "H" else self.pm
        lane_x = iota((n, layer), 1) >> 3
        k_layer = self.r // layer
        pos_z = self.position(ones(mm(turned, self.p_layer) > 0.5) * live, self.low_layer)
        far = (sh.team * sh.slots + k_layer * cap_z).astype(F32) + jnp.minimum(pos_z, cap_z - 1.0)
        payload = jnp.where(k_layer == z, self.near[kind], far)
        by_x = stack([turned * ones(lane_x == xd) for xd in range(sh.inner)])
        needs = []
        if kind == "H":
            made = [
                ones(mm(by_x, self.outputs[c * layer : (c + 1) * layer]) > 0.5) for c in range(sh.cols)
            ]
        else:
            one = ones(mm(by_x, self.p_layer) > 0.5)
            made = [one * ones((iota((sh.inner * n, n), 1) >> log2(sh.width)) == c) for c in range(sh.cols)]
        for xd in range(sh.inner):
            for c in range(sh.cols):
                needs.append(made[c][xd * n : (xd + 1) * n] * live)
        all_needs = stack(needs)
        lane_pos = mm(all_needs, self.up)
        counts = stack([mt(jnp.ones((LIST, n), F32), v) for v in needs])
        starts, ends = mm(counts, self.up), mm(counts, self.up_to)
        over = total_over(ends, cap)
        if kind == "H":
            over = over + self.trace_lists(payload, tab)
        at = (iota((sh.team * LIST, n), 0) % LIST).astype(F32)
        rows = ones((starts <= at) & (at < ends))
        local = mm(rows * (at - starts + 1.0), self.full)
        marked = all_needs * (lane_pos + 1.0)
        found = stack(
            [
                mm(rows[t * LIST : (t + 1) * LIST], marked[t * n : (t + 1) * n])
                for t in range(sh.team)
            ]
        )
        picked = jnp.where((found == local) & (local > 0.5), mm(rows, payload), 0.0)
        line = mt(jnp.ones((EIGHT, n), F32), picked)
        tab[0:1, 0 : sh.team * LIST] = line[0:1].astype(I32)
        me = x * sh.cols + j
        mine = jnp.zeros((n, n), F32)
        for t in range(sh.team):
            mine = mine + needs[t] * jnp.where(me == t, 1.0, 0.0)
        self.pos[kind] = jnp.minimum(self.position(mine, self.low), cap - 1.0)
        return over

    def trace_lists(self, payload, tab):
        sh, n = self.sh, self.sh.nblk
        eye = ones(self.r == self.l)
        diagonal = jnp.sum(self.pm * eye, axis=0, keepdims=True)
        every = tm(self.pm, eye) * self.hm * diagonal
        eight = jnp.ones((EIGHT, n), F32)
        over = jnp.zeros((1, 1), F32)
        mine_rows, mine_lanes = jnp.zeros((EIGHT, n), F32), jnp.zeros((EIGHT, n), F32)
        for xd in range(sh.inner):
            v = every * ones((self.l >> 3) == self.z * sh.inner + xd)
            rows, lanes, starts, ends, _ = self.enumerate(v, EIGHT)
            over = over + total_over(ends, CAP_D)
            line = mt(eight, lanes * mm(rows, payload))
            tab[1:2, xd * EIGHT : (xd + 1) * EIGHT] = line[0:1].astype(I32)
            here = jnp.where(self.x == xd, 1.0, 0.0)
            mine_rows, mine_lanes = mine_rows + here * rows, mine_lanes + here * lanes
        left = mm(mt(mine_lanes, self.sel), self.left_1 * self.p_layer) * mine_rows
        for q, value in enumerate((left, mine_rows)):
            line = mt(eight, value)
            tab[2:3, 32 * q : 32 * q + EIGHT] = line[0:1].astype(I32)
        return over

    def products(self, pw, p_count, tab):
        sh, x, z, j, layer, n = self.sh, self.x, self.z, self.j, self.sh.layer, self.sh.nblk
        v = jnp.zeros((layer, n), F32)
        for c in range(sh.cols):
            v = v + self.remote_f[c * layer : (c + 1) * layer] * jnp.where(c == j, 1.0, 0.0)
        v = v * ones((self.row_i >> 3) == x)
        extra_rows, extra_cols, starts, ends, lane_pos = self.enumerate(v, EIGHT)
        over = total_over(ends, CAP_V)
        low = ones(iota((layer, layer), 1) < iota((layer, layer), 0))
        pos_v = jnp.minimum(lane_pos + mm(low, mm(v, self.full)), CAP_V - 1.0)
        s0, s1 = iota((LIST, n), 0), iota((LIST, n), 1)
        u0, u1 = iota((LIST, layer), 0), iota((LIST, layer), 1)
        row_of = jnp.full((LIST, layer), -1, I32)
        col_of = jnp.full((LIST, n), -1, I32)
        for s in range(sh.slots):
            live = s < p_count[0, 0]
            row_of = jnp.where((u0 == s) & live, pw[0, s] - z * layer, row_of)
            col_of = jnp.where((s0 == s) & live, pw[1, s], col_of)
        own_rows, own_cols = ones(row_of == u1), ones(col_of == s1)
        left_2 = jnp.where(self.row_tile == j, self.slot_layer, sh.slots + pos_v)
        for step in range(2):
            if step == 0:
                oh_row, oh_col = stack([own_rows, extra_rows]), stack([own_cols, extra_cols])
                left, right, from_left, kind, cap, count = self.p_layer, self.hm, self.left_1, "H", CAP_1, LIST_1
            else:
                oh_row, oh_col = own_rows, own_cols
                left, right, from_left, kind, cap, count = self.f_layer, self.pm, left_2, "P", CAP_2, LIST
            w = mm(oh_row, left) * mt(oh_col, right)
            rows, lanes, starts, ends, _ = self.enumerate(w, count)
            over = over + total_over(ends, cap)
            k = w.shape[0]
            at = iota((count, k), 0).astype(F32)
            eight = jnp.ones((EIGHT, n), F32)
            lines = (
                mt(eight, lanes * mm(rows, mm(oh_row, from_left * left))),
                mt(eight, lanes * mm(rows, mt(oh_col, self.pos[kind]))),
                mt(jnp.ones((EIGHT, k), F32), rows * ones(at > starts)),
                jnp.where(ends > starts, jnp.minimum(ends - 1.0, cap), 1.0 * cap),
            )
            for q, line in enumerate(lines):
                size = line.shape[1]
                tab[2 + step : 3 + step, 32 * q : 32 * q + size] = line[0:1].astype(I32)
        return over


def sparse_products(
    sh, p_hbm, h_hbm, pw_hbm, pc_hbm, hw_hbm, hc_hbm, out, e_out, over_out,
    p_ref, h_ref, pw, pc, hw, hc,
    message, messages, near_h, near_p, store_h, store_p, prow, pack_r, pack_hz, pack_pz, pack_h, pack_p,
    pack_d, land_d, land_h, land_p, terms_1, terms_2, fstore, tabv_z, tabv_r, tabv_h, tabv, tab_z, tab_r, tab_h, tab, emsg, emsgs,
    m_send, m_recv, s_send, s_recv, p_send, p_fwd, p_recv, z_send, z_recv,
    t_send, t_recv, d_send, d_recv, e_send, e_recv, t_copy, fetch,
):
    i, j = lax.axis_index("row"), lax.axis_index("col")
    x, z = i % sh.inner, i // sh.inner
    me = i * sh.cols + j
    chip, core = j // 2, j % 2
    mate = (i, chip * 2 + 1 - core)
    team = x * sh.cols + j
    slots, strip, size = sh.slots, sh.strip, sh.size
    all_but_me = sh.devices - 1

    def member(d):
        e = sh.team - d
        qx = (x + e // sh.cols) % sh.inner
        qj = (chip + (e // 2) % sh.chips) % sh.chips * 2 + (core + e % 2) % 2
        return qx * sh.cols + qj, (z * sh.inner + qx, qj)

    def for_others(act):
        for t in range(sh.outer - 1):
            zt = sh.layer_at(z, t)

            @pl.loop(0, sh.team)
            def _(q):
                act((zt * sh.inner + q // sh.cols, q % sh.cols))

        @pl.loop(1, sh.team)
        def _(d):
            act(member(d)[1])

    def in_strip(q):
        return pl.ds(pl.multiple_of(q * strip, strip), strip)

    fetches = [
        pltpu.make_async_copy(source, target, fetch.at[k])
        for k, (source, target) in enumerate(
            (
                (pw_hbm, pw), (pc_hbm, pc), (hw_hbm, hw), (hc_hbm, hc),
                (h_hbm, h_ref), (p_hbm, p_ref),
            )
        )
    ]
    for copy in fetches:
        copy.start()
    barrier = pltpu.get_barrier_semaphore()

    for_others(lambda dev: pl.semaphore_signal(barrier, inc=1, device_id=dev, device_id_type=MESH))

    for copy in fetches[:4]:
        copy.wait()
    lane = iota((1, 128), 1)
    packed = jnp.zeros((1, 128), F32)
    for where, count, scale in ((pw, pc, 1.0), (hw, hc, 16.0)):
        for s in range(slots):
            at = (where[0, s] - i * TILE) * sh.width + where[1, s] - j * sh.width
            packed = packed + jnp.where((lane == at) & (s < count[0, 0]), scale * (s + 1), 0.0)
    message[0] = packed
    messages[me] = packed
    for copy in fetches[4:]:
        copy.wait()
    for s in range(slots):
        near_h[team * slots + s] = h_ref[s, in_strip(team), :]
        near_p[team * slots + s] = p_ref[s, in_strip(team), :]
        prow[s] = p_ref[s]
    pl.semaphore_wait(barrier, all_but_me)

    def tell(dev):
        remote(message.at[pl.ds(0, 1)], messages.at[pl.ds(me, 1)], m_send, m_recv, dev).start()

    for_others(tell)

    def strips(d, which):
        q, dev = member(d)
        ref, near = ((h_ref, near_h), (p_ref, near_p))[which]
        return remote(
            ref.at[:, in_strip(q), :], near.at[pl.ds(team * slots, slots)],
            s_send.at[which, d], s_recv.at[which, team], dev,
        )

    def strips_in(d, which):
        q, dev = member(d)
        ref, near = ((h_ref, near_h), (p_ref, near_p))[which]
        return remote(
            ref.at[:, in_strip(q), :], near.at[pl.ds(q * slots, slots)],
            s_send.at[which, d], s_recv.at[which, q], dev,
        )

    for which in range(2):
        for d in range(1, sh.team):
            strips(d, which).start()

    def other(dc):
        c = (chip + dc) % sh.chips
        return c, c * 2 + core

    p_mate = remote(p_ref, prow.at[pl.ds(slots, slots)], p_send.at[0], p_recv.at[sh.cols], mate)
    p_mate.start()

    def p_block(col):
        return prow.at[pl.ds(sh.others + col * CAP_R, CAP_R)]

    def p_out(dc):
        return remote(pack_r.at[dc - 1], p_block(j), p_send.at[dc], p_recv.at[j], (i, other(dc)[1]))

    def p_in(dc):
        col = other(dc)[1]
        return remote(pack_r.at[dc - 1], p_block(col), p_send.at[dc], p_recv.at[col], (i, col))

    def p_forward(dc):
        col = other(dc)[1]
        return remote(p_block(col), p_block(col), p_fwd.at[dc], p_recv.at[col], mate)

    def p_forward_in(dc):
        col = other(dc)[0] * 2 + 1 - core
        return remote(p_block(col), p_block(col), p_fwd.at[dc], p_recv.at[col], mate)

    def bulk(ref, sem):
        part = ref.at[pl.ds(0, all_but_me)]
        return pltpu.make_async_copy(part, part, sem)

    bulk(messages, m_recv).wait()
    lists = Lists(sh, x, z, j, messages[:, 0, :])

    def publish(source, target, which):
        copy = pltpu.make_async_copy(source, target, t_copy.at[which])
        copy.start()
        copy.wait()

    def entry(ref, table, row, lane):
        return ref[jnp.minimum(jnp.maximum(table[row, lane], 0), ref.shape[0] - 1)]

    kinds = (
        (store_h, pack_hz, pack_h, land_h, CAP_H_Z, CAP_H, near_h, tab_h),
        (store_p, pack_pz, pack_p, land_p, CAP_P_Z, CAP_P, near_p, tab),
    )

    def zone(which, layer):
        store, cap = kinds[which][0], kinds[which][4]
        return store.at[pl.ds(sh.team * slots + layer * cap, cap)]

    def across(which, dz):
        pack = kinds[which][1]
        zd = sh.layer_at(z, dz - 1)
        return remote(
            pack.at[dz - 1], zone(which, z), z_send.at[which, dz], z_recv.at[which, z],
            (zd * sh.inner + x, j),
        )

    def across_in(which, dz):
        pack = kinds[which][1]
        zs = sh.layer_at(z, dz - 1)
        return remote(
            pack.at[dz - 1], zone(which, zs), z_send.at[which, dz], z_recv.at[which, zs],
            (zs * sh.inner + x, j),
        )

    def part(which, d):
        pack, land = kinds[which][2], kinds[which][3]
        _, dev = member(d)
        return remote(
            pack.at[d - 1], land.at[:, in_strip(team), :], t_send.at[which, d], t_recv.at[which, team], dev
        )

    def part_in(which, d):
        pack, land = kinds[which][2], kinds[which][3]
        q, dev = member(d)
        return remote(
            pack.at[d - 1], land.at[:, in_strip(q), :], t_send.at[which, d], t_recv.at[which, q], dev
        )

    def send_across(which):
        store, pack, _, _, cap, _, near, _ = kinds[which]
        for d in range(1, sh.team):
            strips_in(d, which).wait_recv()
        for dz in range(1, sh.outer):
            for k in range(cap):
                pack[dz - 1, k] = entry(near, tab_z, which, (dz - 1) * LIST_Z + k)
        for dz in range(1, sh.outer):
            across(which, dz).start()
        store[0 : sh.team * slots] = near[...]

    def to_trace(xd):
        return remote(
            pack_d.at[xd], land_d.at[:, in_strip(team), :], d_send.at[xd], d_recv.at[team],
            (z * sh.inner + xd, sh.trace_member(z, xd) % sh.cols),
        )

    def trace_in(d):
        q, dev = member(d)
        return remote(pack_d.at[0], land_d.at[:, in_strip(q), :], d_send.at[0], d_recv.at[q], dev)

    def send_trace():
        for xd in range(sh.inner):
            for k in range(CAP_D):
                pack_d[xd, k] = entry(store_h, tab_h, 1, xd * EIGHT + k)
        for xd in range(sh.inner):
            @pl.when(sh.trace_member(z, xd) != team)
            def _():
                to_trace(xd).start()

            @pl.when(sh.trace_member(z, xd) == team)
            def _():
                for k in range(CAP_D):
                    land_d[k, in_strip(team), :] = pack_d[xd, k]

    def send_parts(which):
        store, _, pack, land, _, cap, _, table = kinds[which]
        for dz in range(1, sh.outer):
            across_in(which, dz).wait_recv()
        if which == 0:
            send_trace()

        @pl.loop(1, sh.team)
        def _(d):
            q, _ = member(d)
            for k in range(cap):
                pack[d - 1, k] = entry(store, table, 0, q * LIST + k)

        for d in range(1, sh.team):
            part(which, d).start()
        for k in range(cap):
            land[k, in_strip(team), :] = entry(store, table, 0, team * LIST + k)

    over = lists.across(tabv_z)
    publish(tabv_z, tab_z, 0)
    send_across(0)
    over = over + lists.row_lists(tabv_r)
    publish(tabv_r, tab_r, 1)
    for dc in range(1, sh.chips):
        for k in range(CAP_R):
            pack_r[dc - 1, k] = entry(p_ref, tab_r, 0, (dc - 1) * EIGHT + k)
    for dc in range(1, sh.chips):
        p_out(dc).start()
    over = over + lists.team_lists(0, tabv_h)
    publish(tabv_h, tab_h, 2)
    send_across(1)
    send_parts(0)
    for dc in range(1, sh.chips):
        p_in(dc).wait_recv()
        p_forward(dc).start()
    over = over + lists.team_lists(1, tabv)
    over = over + lists.products(pw, pc, tabv)
    publish(tabv, tab, 3)
    p_mate.wait_recv()
    for dc in range(1, sh.chips):
        p_forward_in(dc).wait_recv()
    emsg[0, 0] = jnp.zeros((1, 128), F32)

    @pl.when(sh.trace_member(z, x) == team)
    def _():
        for d in range(1, sh.team):
            trace_in(d).wait_recv()
        for k in range(CAP_D):
            part_of = entry(prow, tab_h, 2, k).astype(F32) * jnp.transpose(land_d[k].astype(F32))
            total = jnp.sum(part_of, axis=0, keepdims=True)
            emsg[0, 0] += total * tab_h[2, 32 + k].astype(F32)

    emsg[0, 1] = over + jnp.zeros((1, 128), F32)
    emsgs[me] = emsg[0]

    def tell_energy(dev):
        remote(emsg.at[pl.ds(0, 1)], emsgs.at[pl.ds(me, 1)], e_send, e_recv, dev).start()

    for_others(tell_energy)
    send_parts(1)

    def multiply(step, left, right, terms, cap):
        row = 2 + step
        acc = None
        for k in range(cap):
            d = jnp.dot(entry(left, tab, row, k), entry(right, tab, row, 32 + k), preferred_element_type=F32)
            acc = d if acc is None else d + acc * tab[row, 64 + k].astype(F32)
            terms[k] = acc
        terms[cap] = jnp.zeros((size, size), F32)

    for d in range(1, sh.team):
        part_in(0, d).wait_recv()
    multiply(0, prow, land_h, terms_1, CAP_1)
    for s in range(slots):
        value = entry(terms_1, tab, 2, 96 + s)
        rounded = value.astype(BF16)
        fstore[s] = rounded
        out[s] = rounded

    for k in range(CAP_V):
        fstore[slots + k] = entry(terms_1, tab, 2, 96 + LIST + k).astype(BF16)


    for d in range(1, sh.team):
        part_in(1, d).wait_recv()
    multiply(1, fstore, land_p, terms_2, CAP_2)
    for s in range(slots):
        out[slots + s] = entry(terms_2, tab, 3, 96 + s).astype(BF16)

    bulk(emsgs, e_recv).wait()
    e_out[0, 0] = jnp.sum(jnp.sum(emsgs[:, 0], axis=0))
    over_out[0, 0] = jnp.sum(jnp.sum(emsgs[:, 1], axis=0))

    bulk(messages, m_send).wait()
    bulk(emsgs, e_send).wait()
    for which in range(2):
        for d in range(1, sh.team):
            strips(d, which).wait_send()
            part(which, d).wait_send()
        for dz in range(1, sh.outer):
            across(which, dz).wait_send()
    for xd in range(sh.inner):
        @pl.when(sh.trace_member(z, xd) != team)
        def _():
            to_trace(xd).wait_send()
    p_mate.wait_send()
    for dc in range(1, sh.chips):
        p_out(dc).wait_send()
        p_forward(dc).wait_send()


def sparse_path(sh, p_values, p_where, p_count, h_values, h_where, h_count):
    slots, size, strip = sh.slots, sh.size, sh.strip
    block, piece = (size, size), (strip, size)
    bf = lambda *shape: pltpu.VMEM(shape, BF16)
    f32 = lambda *shape: pltpu.VMEM(shape, F32)
    dma = pltpu.SemaphoreType.DMA
    near = sh.team * slots
    away = max(sh.outer - 1, 1)
    chips = max(sh.chips - 1, 1)
    scalar = jax.ShapeDtypeStruct((1, 1), F32)
    return pl.pallas_call(
        functools.partial(sparse_products, sh),
        out_shape=[jax.ShapeDtypeStruct((2 * slots,) + block, BF16), scalar, scalar],
        in_specs=[ANY] * 6,
        out_specs=[VMEM, SMEM, SMEM],
        scratch_shapes=[
            bf(slots, *block),
            bf(slots, *block),
            pltpu.SMEM((2, slots), I32),
            pltpu.SMEM((1, 1), I32),
            pltpu.SMEM((2, slots), I32),
            pltpu.SMEM((1, 1), I32),
            f32(1, 1, 128),
            f32(sh.devices, 1, 128),
            bf(near, *piece),
            bf(near, *piece),
            bf(near + sh.outer * CAP_H_Z, *piece),
            bf(near + sh.outer * CAP_P_Z, *piece),
            bf(sh.others + sh.cols * CAP_R, *block),
            bf(chips, CAP_R, *block),
            bf(away, CAP_H_Z, *piece),
            bf(away, CAP_P_Z, *piece),
            bf(sh.team, CAP_H, *piece),
            bf(sh.team, CAP_P, *piece),
            bf(sh.inner, CAP_D, *piece),
            bf(CAP_D, *block),
            bf(CAP_H, *block),
            bf(CAP_P, *block),
            f32(CAP_1 + 1, *block),
            f32(CAP_2 + 1, *block),
            bf(slots + CAP_V, *block),
            pltpu.VMEM((8, 128), I32),
            pltpu.VMEM((8, 128), I32),
            pltpu.VMEM((8, 128), I32),
            pltpu.VMEM((8, 128), I32),
            pltpu.SMEM((8, 128), I32),
            pltpu.SMEM((8, 128), I32),
            pltpu.SMEM((8, 128), I32),
            pltpu.SMEM((8, 128), I32),
            f32(1, 2, 1, 128),
            f32(sh.devices, 2, 1, 128),
            dma, dma,
            dma((2, sh.team)), dma((2, sh.team)),
            dma((sh.chips,)), dma((sh.chips,)), dma((sh.cols + 1,)),
            dma((2, sh.outer)), dma((2, sh.outer)),
            dma((2, sh.team)), dma((2, sh.team)),
            dma((sh.inner,)), dma((sh.team,)),
            dma, dma, dma((4,)), dma((6,)),
        ],
        compiler_params=pltpu.CompilerParams(collective_id=2, has_side_effects=True, vmem_limit_bytes=24 << 20),
        name="sparse_products",
    )(p_values, h_values, p_where.T, p_count, h_where.T, h_count)


def deliver(both):
    def kernel(both_ref, first, second, sems):
        slots = first.shape[0]
        copies = [
            pltpu.make_async_copy(both_ref.at[pl.ds(k * slots, slots)], ref, sems.at[k])
            for k, ref in enumerate((first, second))
        ]
        for copy in copies:
            copy.start()
        for copy in copies:
            copy.wait()

    half = jax.ShapeDtypeStruct((both.shape[0] // 2,) + both.shape[1:], both.dtype)
    return pl.pallas_call(
        kernel,
        out_shape=[half, half],
        in_specs=[VMEM],
        out_specs=[ANY, ANY],
        scratch_shapes=[pltpu.SemaphoreType.DMA((2,))],
        name="deliver",
    )(both)


def per_device(rows, cols, *args):
    slots, size, _ = args[0].shape
    sh = Shape(rows, cols, slots, size)
    if not sh.fits():
        return dense_path(rows, cols, *args)
    both, energy, over = sparse_path(sh, *args)
    return lax.cond(
        over[0, 0] > 0.0,
        lambda: dense_path(rows, cols, *args),
        lambda: (*deliver(both), energy[0, 0]),
    )


def solution(mesh):
    placed = (
        P("row", "col", None),
        P("row", "col"),
        P("row", "col"),
        P("row", "col", None),
        P("row", "col"),
        P("row", "col"),
    )
    return jax.shard_map(
        functools.partial(per_device, mesh.shape["row"], mesh.shape["col"]),
        mesh=mesh,
        in_specs=placed,
        out_specs=(P("row", "col", None), P("row", "col", None), P()),
        check_vma=False,
    )
```

```python
import functools

import jax
import jax.numpy as jnp
from jax import lax
from jax.experimental import pallas as pl
from jax.experimental.pallas import tpu as pltpu
from jax.sharding import PartitionSpec as P

TILE = 8
CHUNKS = 6
IN_FLIGHT = 16
MESH = pl.DeviceIdType.MESH
ANY = pl.BlockSpec(memory_space=pl.ANY)
VMEM = pl.BlockSpec(memory_space=pltpu.VMEM)
SMEM = pl.BlockSpec(memory_space=pltpu.SMEM)


def at_row(r):
    return (r, lax.axis_index("col"))


def at_col(c):
    return (lax.axis_index("row"), c)


def remote(src, dst, send_sem, recv_sem, device):
    return pltpu.make_async_remote_copy(
        src_ref=src,
        dst_ref=dst,
        send_sem=send_sem,
        recv_sem=recv_sem,
        device_id=device,
        device_id_type=MESH,
    )


def greet(rows, cols):
    me_row, me_col = lax.axis_index("row"), lax.axis_index("col")
    barrier = pltpu.get_barrier_semaphore()
    for d in range(1, rows):
        pl.semaphore_signal(
            barrier, inc=1, device_id=at_row((me_row + d) % rows), device_id_type=MESH
        )
    for d in range(1, cols):
        pl.semaphore_signal(
            barrier, inc=1, device_id=at_col((me_col + d) % cols), device_id_type=MESH
        )
    pl.semaphore_wait(barrier, rows + cols - 2)


class ColumnGather:
    def __init__(self, rows, own, land, out, up_send, down_send, x_send, recv, local):
        self.own, self.land, self.out = own, land, out
        self.up_send, self.down_send, self.x_send = up_send, down_send, x_send
        self.recv, self.local = recv, local
        self.inner = 2 if rows % 2 == 0 else 1
        self.outer = rows // self.inner
        self.chunks = recv.shape[1]
        self.size = own.shape[0] // self.chunks
        self.me = lax.axis_index("row")
        self.x, self.z = self.me % self.inner, self.me // self.inner
        self.cross_first = 1 if self.inner == 2 and self.chunks > 1 else 0

    def later(self, ch):
        return (ch + self.cross_first) % self.chunks

    def row(self, z, line):
        return z * self.inner + (self.x if line == 0 else self.inner - 1 - self.x)

    def part(self, ch):
        return pl.ds(ch * self.size, self.size)

    def copy(self, r, ch, own, way):
        sems, target = {
            "up": (self.up_send, self.me + self.inner),
            "down": (self.down_send, self.me - self.inner),
            "x": (self.x_send, self.row(self.z, 1)),
        }[way]
        part = self.part(ch)
        src = self.own.at[part] if own else self.land.at[r, part]
        return remote(src, self.land.at[r, part], sems.at[r, ch], self.recv.at[r, ch], at_row(target))

    def keep(self, r, ch):
        part = self.part(ch)
        return pltpu.make_async_copy(self.land.at[r, part], self.out.at[r, part], self.local.at[r, ch])

    def along(self, r, ch, own, act):
        @pl.when(self.z < self.outer - 1)
        def _():
            act(self.copy(r, ch, own, "up"))

        @pl.when(self.z > 0)
        def _():
            act(self.copy(r, ch, own, "down"))

    def arrive(self, r, ch):
        self.copy(r, ch, False, "x").wait_recv()
        self.keep(r, ch).start()

    def start(self):
        for ch in range(self.chunks):
            if self.inner == 2:
                self.copy(self.me, ch, True, "x").start()
            self.along(self.me, self.later(ch), True, lambda copy: copy.start())
        if self.cross_first:
            r = self.row(self.z, 1)
            self.arrive(r, 0)
            self.along(r, 0, False, lambda copy: copy.start())

    def pieces(self):
        lines = [(self.later(ch), 0) for ch in range(self.chunks)]
        return lines + [(0, 1)] * self.cross_first

    def relayed(self, d, side, ch, line, act):
        z = self.z - d if side == 0 else self.z + d
        there = self.z >= d if side == 0 else self.z + d < self.outer
        r = self.row(z, line)

        @pl.when(there)
        def _():
            if act == "start":
                self.arrive(r, ch)
            on = self.z < self.outer - 1 if side == 0 else self.z > 0

            @pl.when(on)
            def _():
                copy = self.copy(r, ch, False, "up" if side == 0 else "down")
                copy.start() if act == "start" else copy.wait_send()

            if self.inner == 2 and ch >= self.cross_first:
                copy = self.copy(r, ch, False, "x")
                copy.start() if act == "start" else copy.wait_send()

    def relay(self, d):
        for ch, line in self.pieces():
            for side in range(2):
                self.relayed(d, side, ch, line, "start")

    def finish(self):
        if self.inner == 2:
            for ch in range(self.cross_first, self.chunks):
                self.arrive(self.row(self.z, 1), ch)
            for d in range(1, self.outer):
                for side in range(2):
                    z = self.z - d if side == 0 else self.z + d
                    there = self.z >= d if side == 0 else self.z + d < self.outer

                    @pl.when(there)
                    def _():
                        for ch in range(self.cross_first, self.chunks):
                            self.arrive(self.row(z, 1), ch)
        for ch in range(self.chunks):
            if self.inner == 2:
                self.copy(self.me, ch, True, "x").wait_send()
            self.along(self.me, ch, True, lambda copy: copy.wait_send())
        if self.cross_first:
            self.along(self.row(self.z, 1), 0, False, lambda copy: copy.wait_send())
        for d in range(1, self.outer):
            for ch, line in self.pieces():
                for side in range(2):
                    self.relayed(d, side, ch, line, "wait")
        for r in range(self.inner * self.outer):
            @pl.when(r != self.me)
            def _():
                for ch in range(self.chunks):
                    self.keep(r, ch).wait()


def col_copies(cols, own, out, send, recv):
    me = lax.axis_index("col")
    made = []
    for d in range(1, cols):
        made.append(
            remote(own, out.at[me], send.at[d], recv.at[d], at_col((me + d) % cols))
        )
    return made


def row_copies(rows, own, out, send, recv):
    me = lax.axis_index("row")
    made = []
    for d in range(1, rows):
        made.append(
            remote(own, out.at[me], send.at[d], recv.at[d], at_row((me + d) % rows))
        )
    return made


def first_gather(
    rows, cols, p_ref, h_ref, meta_ref, prow, hcol, prow_meta, col_meta,
    land, up_send, down_send, x_send, recv, out_sems,
    p_send, p_recv, mc_send, mc_recv, mr_send, mr_recv, local,
):
    me_row, me_col = lax.axis_index("row"), lax.axis_index("col")
    keep = [
        pltpu.make_async_copy(h_ref, hcol.at[me_row], local.at[0]),
        pltpu.make_async_copy(p_ref, prow.at[me_col], local.at[1]),
        pltpu.make_async_copy(meta_ref, prow_meta.at[me_col], local.at[2]),
        pltpu.make_async_copy(meta_ref, col_meta.at[me_row], local.at[3]),
    ]
    greet(rows, cols)
    gather = ColumnGather(
        rows, h_ref, land, hcol, up_send, down_send, x_send, recv, out_sems
    )
    across = (
        col_copies(cols, p_ref, prow, p_send, p_recv)
        + col_copies(cols, meta_ref, prow_meta, mc_send, mc_recv)
        + row_copies(rows, meta_ref, col_meta, mr_send, mr_recv)
    )
    for copy in across + keep:
        copy.start()
    gather.start()
    for d in range(1, gather.outer):
        gather.relay(d)
    gather.finish()
    for copy in across + keep:
        copy.wait()


def second_gather(
    rows, cols, p_ref, f_ref, e_ref, frow, pcol, e_out,
    e_cols, e_rows, e_sum,
    land, up_send, down_send, x_send, recv, out_sems,
    p_send, p_recv, ec_send, ec_recv, er_send, er_recv, local,
):
    me_row, me_col = lax.axis_index("row"), lax.axis_index("col")
    keep = [
        pltpu.make_async_copy(p_ref, pcol.at[me_row], local.at[0]),
        pltpu.make_async_copy(f_ref, frow.at[me_col], local.at[1]),
    ]
    greet(rows, cols)
    energies = col_copies(cols, e_ref, e_cols, ec_send, ec_recv)
    for copy in energies:
        copy.start()
    gather = ColumnGather(
        rows, p_ref, land, pcol, up_send, down_send, x_send, recv, out_sems
    )
    across = col_copies(cols, f_ref, frow, p_send, p_recv)
    for copy in across + keep:
        copy.start()
    gather.start()
    e_cols[me_col] = e_ref[...]
    for copy in energies:
        copy.wait()
    total = e_cols[0]
    for c in range(1, cols):
        total = total + e_cols[c]
    e_sum[...] = total
    e_rows[me_row] = total
    if gather.outer > 1:
        gather.relay(1)
    sums = row_copies(rows, e_sum, e_rows, er_send, er_recv)
    for copy in sums:
        copy.start()
    for d in range(2, gather.outer):
        gather.relay(d)
    for copy in sums:
        copy.wait()
    total = e_rows[0]
    for r in range(1, rows):
        total = total + e_rows[r]
    e_out[...] = total
    gather.finish()
    for copy in across + keep:
        copy.wait()


def block_products(
    rows, cols, right_lane, with_trace, lmeta, rmeta, left, right, *rest
):
    if with_trace:
        out, e_out = rest[:2]
    else:
        e_in, out, e_out = rest[:3]
    acc, lbuf, rbuf, head, nxt, inner, mask, table, ml, mr, ms, sems = rest[-12:]
    slots = out.shape[0]
    i, j = lax.axis_index("row"), lax.axis_index("col")
    nblk = rows * TILE
    tile_cols = nblk // cols
    words = -(-nblk // 32)
    count_lane = 4 * slots
    acc[...] = jnp.zeros_like(acc)

    for t in range(TILE + 1):
        head[t] = -1

    for t in range(tile_cols * words + 1):
        mask[t] = 0

    @pl.loop(0, cols)
    def _(c):
        live = lmeta[c, 0, count_lane]
        for s in range(slots):
            row = jnp.where(s < live, lmeta[c, 0, s] - i * TILE, TILE)
            idx = c * slots + s
            inner[idx] = lmeta[c, 0, slots + s]
            nxt[idx] = head[row]
            head[row] = idx

    @pl.loop(0, rows)
    def _(r):
        live = rmeta[r, 0, count_lane + (1 if right_lane else 0)]
        for s in range(slots):
            k = rmeta[r, 0, right_lane + s]
            col = rmeta[r, 0, right_lane + slots + s] - j * tile_cols
            word = jnp.where(s < live, col * words + (k >> 5), tile_cols * words)
            mask[word] = mask[word] | (jnp.int32(1) << (k & 31))
            table[jnp.where(s < live, k * tile_cols + col, nblk * tile_cols)] = r * slots + s

    def find_slot(s, n):
        row = lmeta[j, 0, s] - i * TILE
        col = lmeta[j, 0, slots + s] - j * tile_cols

        def more(state):
            return state[0] >= 0

        def step(state):
            at, n = state
            k = inner[at]
            ml[n] = at
            mr[n] = table[k * tile_cols + col]
            ms[n] = s
            return nxt[at], n + ((mask[col * words + (k >> 5)] >> (k & 31)) & 1)

        return lax.while_loop(more, step, (head[row], n))[1]

    own_count = lmeta[j, 0, count_lane]
    found = lax.fori_loop(0, own_count, find_slot, jnp.int32(0))

    def fetch(base, m):
        a, b = ml[base + m], mr[base + m]
        return (
            pltpu.make_async_copy(left.at[a], lbuf.at[m], sems.at[0, m]),
            pltpu.make_async_copy(right.at[b], rbuf.at[m], sems.at[1, m]),
        )

    @pl.loop(0, (found + IN_FLIGHT - 1) // IN_FLIGHT)
    def _(chunk):
        base = chunk * IN_FLIGHT
        size = jnp.minimum(found - base, IN_FLIGHT)

        @pl.loop(0, size)
        def _(m):
            for copy in fetch(base, m):
                copy.start()

        @pl.loop(0, size)
        def _(m):
            for copy in fetch(base, m):
                copy.wait()
            s = ms[base + m]
            acc[s] += jnp.dot(lbuf[m], rbuf[m], preferred_element_type=jnp.float32)

    out[...] = acc[...].astype(out.dtype)
    if with_trace:
        size = acc.shape[1]
        e_out[...] = jnp.zeros_like(e_out)
        diagonal = lax.broadcasted_iota(jnp.int32, (size, size), 0) == lax.broadcasted_iota(
            jnp.int32, (size, size), 1
        )

        @pl.loop(0, own_count)
        def _(s):
            @pl.when(lmeta[j, 0, s] == lmeta[j, 0, slots + s])
            def _():
                e_out[...] += jnp.sum(jnp.where(diagonal, acc[s], 0.0))
    else:
        e_out[0, 0] = e_in[0, 0]


def dense_path(rows, cols, p_values, p_where, p_count, h_values, h_where, h_count):
    slots, size, _ = p_values.shape
    dtype = p_values.dtype
    nblk = rows * TILE
    tile_cols = nblk // cols
    words = -(-nblk // 32)
    meta = jnp.concatenate(
        [p_where[:, 0], p_where[:, 1], h_where[:, 0], h_where[:, 1], p_count[0], h_count[0]]
    )
    meta = jnp.broadcast_to(jnp.pad(meta, (0, 128 - meta.shape[0]))[None, :], (8, 128))
    dma = pltpu.SemaphoreType.DMA
    chunks = CHUNKS if slots % CHUNKS == 0 else 1
    chunk_sems = [pltpu.VMEM((rows, slots, size, size), dtype)] + [dma((rows, chunks))] * 5
    col_sems = [dma((cols,)), dma((cols,))]
    row_sems = [dma((rows,)), dma((rows,))]
    tile = (slots, size, size)
    prow, hcol, prow_meta, col_meta = pl.pallas_call(
        functools.partial(first_gather, rows, cols),
        out_shape=[
            jax.ShapeDtypeStruct((cols,) + tile, dtype),
            jax.ShapeDtypeStruct((rows,) + tile, dtype),
            jax.ShapeDtypeStruct((cols, 8, 128), jnp.int32),
            jax.ShapeDtypeStruct((rows, 8, 128), jnp.int32),
        ],
        in_specs=[VMEM] * 3,
        out_specs=[ANY] * 4,
        scratch_shapes=chunk_sems + col_sems + col_sems + row_sems + [dma((4,))],
        compiler_params=pltpu.CompilerParams(collective_id=0, has_side_effects=True),
        name="first_gather",
    )(p_values, h_values, meta)

    def products(right_lane, with_trace, lmeta, rmeta, left, right, *more):
        smem = lambda n: pltpu.SMEM((n,), jnp.int32)
        most = slots * nblk + 1
        return pl.pallas_call(
            functools.partial(block_products, rows, cols, right_lane, with_trace),
            out_shape=[
                jax.ShapeDtypeStruct(tile, dtype),
                jax.ShapeDtypeStruct((8, 128) if with_trace else (1, 1), jnp.float32),
            ],
            in_specs=[SMEM, SMEM, ANY, ANY] + [SMEM] * len(more),
            out_specs=[VMEM, VMEM if with_trace else SMEM],
            scratch_shapes=[
                pltpu.VMEM(tile, jnp.float32),
                pltpu.VMEM((IN_FLIGHT, size, size), dtype),
                pltpu.VMEM((IN_FLIGHT, size, size), dtype),
                smem(TILE + 1),
                smem(cols * slots),
                smem(cols * slots),
                smem(tile_cols * words + 1),
                smem(nblk * tile_cols + 1),
                smem(most),
                smem(most),
                smem(most),
                dma((2, IN_FLIGHT)),
            ],
            name="products",
        )(
            lmeta,
            rmeta,
            left.reshape((cols * slots, size, size)),
            right.reshape((rows * slots, size, size)),
            *more,
        )

    ph_values, part = products(2 * slots, True, prow_meta, col_meta, prow, hcol)
    frow, pcol, energy = pl.pallas_call(
        functools.partial(second_gather, rows, cols),
        out_shape=[
            jax.ShapeDtypeStruct((cols,) + tile, dtype),
            jax.ShapeDtypeStruct((rows,) + tile, dtype),
            jax.ShapeDtypeStruct((8, 128), jnp.float32),
        ],
        in_specs=[VMEM] * 3,
        out_specs=[ANY, ANY, VMEM],
        scratch_shapes=[
            pltpu.VMEM((cols, 8, 128), jnp.float32),
            pltpu.VMEM((rows, 8, 128), jnp.float32),
            pltpu.VMEM((8, 128), jnp.float32),
        ]
        + chunk_sems + col_sems + col_sems + row_sems + [dma((2,))],
        compiler_params=pltpu.CompilerParams(collective_id=1, has_side_effects=True),
        name="second_gather",
    )(p_values, ph_values, part)
    php_values, energy = products(0, False, prow_meta, col_meta, frow, pcol, energy)
    return (ph_values, php_values, energy[0, 0])


CAP_H_Z, CAP_P_Z = 17, 12
CAP_H, CAP_P = 14, 9
CAP_R, CAP_V, CAP_D = 7, 7, 3
CAP_1, CAP_2 = 18, 12
LIST, LIST_Z, LIST_1, EIGHT = 16, 24, 24, 8
F32, BF16, I32 = jnp.float32, jnp.bfloat16, jnp.int32


def log2(n):
    return n.bit_length() - 1


def power(n):
    return n > 0 and n & (n - 1) == 0


class Shape:
    def __init__(self, rows, cols, slots, size):
        self.rows, self.cols, self.slots, self.size = rows, cols, slots, size
        self.devices = rows * cols
        self.nblk = rows * TILE
        self.inner = 2 if rows % 2 == 0 else 1
        self.outer = rows // self.inner
        self.layer = self.inner * TILE
        self.team = self.inner * cols
        self.strip = size // self.team
        self.width = self.nblk // cols
        self.chips = cols // 2
        self.others = 2 * slots

    def trace_member(self, z, xd):
        return xd * self.cols + (z * self.inner + xd) * TILE // self.width

    def layer_at(self, z, t):
        down = self.outer - 1 - t
        return jnp.where(
            z < self.outer // 2,
            down - jnp.where(down <= z, 1, 0),
            t + jnp.where(t >= z, 1, 0),
        )

    def fits(self):
        return (
            power(self.rows)
            and power(self.cols)
            and self.cols >= 2
            and self.outer >= 2
            and self.nblk <= 64
            and TILE <= self.width <= 128 // TILE
            and self.slots <= 15
            and self.strip % 16 == 0
            and self.team * LIST <= 128
            and (self.outer - 1) * LIST_Z <= 128
            and (self.chips - 1) * EIGHT <= 128
        )


def mm(a, b):
    return lax.dot_general(a.astype(BF16), b.astype(BF16), (((1,), (0,)), ((), ())), preferred_element_type=F32)


def mt(a, b):
    return lax.dot_general(a.astype(BF16), b.astype(BF16), (((1,), (1,)), ((), ())), preferred_element_type=F32)


def tm(a, b):
    return lax.dot_general(a.astype(BF16), b.astype(BF16), (((0,), (0,)), ((), ())), preferred_element_type=F32)


def ones(cond):
    return jnp.where(cond, 1.0, 0.0).astype(F32)


def iota(shape, dim):
    return lax.broadcasted_iota(I32, shape, dim)


def block_index(shape, dim, size):
    return iota(shape, dim) // size


def total_over(ends, cap):
    over = ones(ends > cap + 0.5)
    return jnp.sum(jnp.sum(over, axis=0, keepdims=True), axis=1, keepdims=True)


def stack(parts):
    return jnp.concatenate(parts, axis=0)


class Lists:
    def __init__(self, sh, x, z, j, message):
        self.sh, self.x, self.z, self.j = sh, x, z, j
        n, width, layer = sh.nblk, sh.width, sh.layer
        lw = log2(width)
        r, l = iota((n, n), 0), iota((n, n), 1)
        a0, d0 = iota((sh.cols * n, sh.devices), 0), iota((sh.cols * n, sh.devices), 1)
        spread = mm(ones(d0 == ((a0 & (n - 1)) >> 3) * sh.cols + (a0 >> log2(n))), message)
        a1, l1 = iota((sh.cols * n, 128), 0), iota((sh.cols * n, 128), 1)
        spread = jnp.where((l1 >> lw) == (a1 & 7), spread, 0.0)
        l2, m2 = iota((128, n), 0), iota((128, n), 1)
        spread = mm(spread, ones((l2 & (width - 1)) == (m2 & (width - 1))))
        both = jnp.zeros((n, n), F32)
        for c in range(sh.cols):
            both = both + jnp.where((l >> lw) == c, spread[c * n : (c + 1) * n], 0.0)
        hs = jnp.floor(both * (1.0 / 16.0))
        ps = both - 16.0 * hs
        self.pos = {}
        self.pm, self.hm = ones(ps > 0.5), ones(hs > 0.5)
        self.fm = self.pm * ones(mm(self.pm, self.hm) > 0.5)
        self.up, self.low, self.up_to = ones(r < l), ones(l < r), ones(r <= l)
        self.low_layer = ones((l < r) & (l // layer == r // layer))
        self.full = jnp.ones((n, n), F32)
        self.r, self.l, self.lane_tile = r, l, l >> lw
        team = ((r >> 3) & (sh.inner - 1)) * sh.cols + self.lane_tile
        at = (team * sh.slots).astype(F32)
        self.near = {"H": at + hs - 1.0, "P": at + ps - 1.0}
        s0, s1 = iota((layer, n), 0), iota((layer, n), 1)
        self.sel = ones(s1 == z * layer + s0)
        self.row_i, self.row_tile = s0, (s1 >> lw)
        self.p_layer, self.f_layer = mm(self.sel, self.pm), mm(self.sel, self.fm)
        self.slot_layer = mm(self.sel, ps) - 1.0

    def enumerate(self, v, count, lane_pos=None):
        k, n = v.shape
        counts = mt(jnp.ones((count, n), F32), v)
        a, b = iota((k, k), 0), iota((k, k), 1)
        starts, ends = mm(counts, ones(a < b)), mm(counts, ones(a <= b))
        at = iota((count, k), 0).astype(F32)
        rows = ones((starts <= at) & (at < ends))
        local = mm(rows * (at - starts + 1.0), jnp.ones((k, n), F32))
        if lane_pos is None:
            lane_pos = mm(v, self.up)
        found = mm(rows, v * (lane_pos + 1.0))
        lanes = ones((found == local) & (local > 0.5))
        return rows, lanes, starts, ends, lane_pos

    def position(self, v, low):
        return mm(v, self.up) + mm(low, mm(v, self.full))

    def across(self, tab):
        sh, z, layer, n = self.sh, self.z, self.sh.layer, self.sh.nblk
        p_s, f_s = mt(self.sel, self.pm), mt(self.sel, self.fm)
        i_layer = self.l[0:layer] // layer
        lhs, live, pay = [], [], []
        for kind, left, right in (("H", p_s, self.hm), ("P", f_s, self.pm)):
            live_kind, pay_kind = mm(self.sel, right), mm(self.sel, self.near[kind])
            for dz in range(1, sh.outer):
                lhs.append(left * ones(i_layer == sh.layer_at(z, dz - 1)))
                live.append(live_kind)
                pay.append(pay_kind)
        v = ones(mm(stack(lhs), self.pm) > 0.5) * stack(live)
        k = v.shape[0]
        lists = 2 * (sh.outer - 1)
        a, b = iota((k, k), 0), iota((k, k), 1)
        counts = mt(jnp.ones((EIGHT, n), F32), v)
        starts = mm(counts, ones((a < b) & (a // layer == b // layer)))
        ends = mm(counts, ones((a <= b) & (a // layer == b // layer)))
        t0 = iota((lists * LIST_Z, k), 0)
        at = (t0 % LIST_Z).astype(F32)
        rows = ones(
            (starts[0:1] <= at)
            & (at < ends[0:1])
            & (t0 // LIST_Z == block_index((lists * LIST_Z, k), 1, layer))
        )
        local = mm(rows * (at - starts[0:1] + 1.0), jnp.ones((k, n), F32))
        found = mm(rows, v * (mm(v, self.up) + 1.0))
        picked = jnp.where((found == local) & (local > 0.5), mm(rows, stack(pay)), 0.0)
        half = (sh.outer - 1) * LIST_Z
        for which in range(2):
            line = mt(jnp.ones((EIGHT, n), F32), picked[which * half : (which + 1) * half])
            tab[which : which + 1, 0:half] = line[0:1].astype(I32)
        lane_h = block_index((EIGHT, k), 1, layer) < sh.outer - 1
        cap = jnp.where(lane_h, 1.0 * CAP_H_Z, 1.0 * CAP_P_Z)
        return total_over(ends - cap, 0.0)

    def row_lists(self, tab):
        sh, x, j, layer, n = self.sh, self.x, self.j, self.sh.layer, self.sh.nblk
        tiles = [ones(self.row_tile == c) for c in range(sh.cols)]
        wide = stack([self.p_layer * t for t in tiles])
        passed = ones(mt(wide, self.pm) > 0.5) * stack([self.f_layer] * sh.cols)
        own = wide
        self.outputs = jnp.maximum(own, passed)
        self.remote_f = passed * (1.0 - ones(stack([t for t in tiles]) > 0.5))
        reads = ones(mt(self.outputs, self.hm) > 0.5) * stack([self.p_layer] * sh.cols)
        mine = ones((self.row_i >> 3) == x)
        chip = j // 2
        low = ones(iota((layer, layer), 1) < iota((layer, layer), 0))
        seg_tri = ones((self.lane_tile == (self.r >> log2(sh.width))) & (self.r < self.l))
        seg_full = ones(self.lane_tile == (self.r >> log2(sh.width)))
        over = jnp.zeros((1, 1), F32)
        for dc in range(sh.chips):
            c = (chip + dc) % sh.chips
            v = jnp.zeros((layer, n), F32)
            for k in range(sh.cols):
                v = jnp.maximum(v, reads[k * layer : (k + 1) * layer] * jnp.where(k // 2 == c, 1.0, 0.0))
            v = v * mine
            if dc == 0:
                pos = mm(v, seg_tri) + mm(low, mm(v, seg_full))
                pos = jnp.minimum(pos, CAP_R - 1.0)
                continue
            v = v * ones(self.row_tile == j)
            rows, lanes, starts, ends, _ = self.enumerate(v, EIGHT)
            line = mt(jnp.ones((EIGHT, n), F32), lanes * mm(rows, self.slot_layer))
            tab[0:1, (dc - 1) * EIGHT : dc * EIGHT] = line[0:1].astype(I32)
            over = over + total_over(ends, CAP_R)
        self.left_1 = jnp.where(
            self.row_tile == j,
            self.slot_layer,
            jnp.where(
                self.row_tile // 2 == chip,
                sh.slots + self.slot_layer,
                sh.others + self.row_tile.astype(F32) * CAP_R + pos,
            ),
        )
        return over

    def team_lists(self, which, tab):
        sh, x, z, j, layer, n = self.sh, self.x, self.z, self.j, self.sh.layer, self.sh.nblk
        a, b = iota((layer, layer), 0), iota((layer, layer), 1)
        turn = lambda m: tm(m, ones(a == b))
        kind, cap_z, cap = (("H", CAP_H_Z, CAP_H), ("P", CAP_P_Z, CAP_P))[which]
        turned = turn(self.p_layer if kind == "H" else self.f_layer)
        live = self.hm if kind == "H" else self.pm
        lane_x = iota((n, layer), 1) >> 3
        k_layer = self.r // layer
        pos_z = self.position(ones(mm(turned, self.p_layer) > 0.5) * live, self.low_layer)
        far = (sh.team * sh.slots + k_layer * cap_z).astype(F32) + jnp.minimum(pos_z, cap_z - 1.0)
        payload = jnp.where(k_layer == z, self.near[kind], far)
        by_x = stack([turned * ones(lane_x == xd) for xd in range(sh.inner)])
        needs = []
        if kind == "H":
            made = [
                ones(mm(by_x, self.outputs[c * layer : (c + 1) * layer]) > 0.5) for c in range(sh.cols)
            ]
        else:
            one = ones(mm(by_x, self.p_layer) > 0.5)
            made = [one * ones((iota((sh.inner * n, n), 1) >> log2(sh.width)) == c) for c in range(sh.cols)]
        for xd in range(sh.inner):
            for c in range(sh.cols):
                needs.append(made[c][xd * n : (xd + 1) * n] * live)
        all_needs = stack(needs)
        lane_pos = mm(all_needs, self.up)
        counts = stack([mt(jnp.ones((LIST, n), F32), v) for v in needs])
        starts, ends = mm(counts, self.up), mm(counts, self.up_to)
        over = total_over(ends, cap)
        if kind == "H":
            over = over + self.trace_lists(payload, tab)
        at = (iota((sh.team * LIST, n), 0) % LIST).astype(F32)
        rows = ones((starts <= at) & (at < ends))
        local = mm(rows * (at - starts + 1.0), self.full)
        marked = all_needs * (lane_pos + 1.0)
        found = stack(
            [
                mm(rows[t * LIST : (t + 1) * LIST], marked[t * n : (t + 1) * n])
                for t in range(sh.team)
            ]
        )
        picked = jnp.where((found == local) & (local > 0.5), mm(rows, payload), 0.0)
        line = mt(jnp.ones((EIGHT, n), F32), picked)
        tab[0:1, 0 : sh.team * LIST] = line[0:1].astype(I32)
        me = x * sh.cols + j
        mine = jnp.zeros((n, n), F32)
        for t in range(sh.team):
            mine = mine + needs[t] * jnp.where(me == t, 1.0, 0.0)
        self.pos[kind] = jnp.minimum(self.position(mine, self.low), cap - 1.0)
        return over

    def trace_lists(self, payload, tab):
        sh, n = self.sh, self.sh.nblk
        eye = ones(self.r == self.l)
        diagonal = jnp.sum(self.pm * eye, axis=0, keepdims=True)
        every = tm(self.pm, eye) * self.hm * diagonal
        eight = jnp.ones((EIGHT, n), F32)
        over = jnp.zeros((1, 1), F32)
        mine_rows, mine_lanes = jnp.zeros((EIGHT, n), F32), jnp.zeros((EIGHT, n), F32)
        for xd in range(sh.inner):
            v = every * ones((self.l >> 3) == self.z * sh.inner + xd)
            rows, lanes, starts, ends, _ = self.enumerate(v, EIGHT)
            over = over + total_over(ends, CAP_D)
            line = mt(eight, lanes * mm(rows, payload))
            tab[1:2, xd * EIGHT : (xd + 1) * EIGHT] = line[0:1].astype(I32)
            here = jnp.where(self.x == xd, 1.0, 0.0)
            mine_rows, mine_lanes = mine_rows + here * rows, mine_lanes + here * lanes
        left = mm(mt(mine_lanes, self.sel), self.left_1 * self.p_layer) * mine_rows
        for q, value in enumerate((left, mine_rows)):
            line = mt(eight, value)
            tab[2:3, 32 * q : 32 * q + EIGHT] = line[0:1].astype(I32)
        return over

    def products(self, pw, p_count, tab):
        sh, x, z, j, layer, n = self.sh, self.x, self.z, self.j, self.sh.layer, self.sh.nblk
        v = jnp.zeros((layer, n), F32)
        for c in range(sh.cols):
            v = v + self.remote_f[c * layer : (c + 1) * layer] * jnp.where(c == j, 1.0, 0.0)
        v = v * ones((self.row_i >> 3) == x)
        extra_rows, extra_cols, starts, ends, lane_pos = self.enumerate(v, EIGHT)
        over = total_over(ends, CAP_V)
        low = ones(iota((layer, layer), 1) < iota((layer, layer), 0))
        pos_v = jnp.minimum(lane_pos + mm(low, mm(v, self.full)), CAP_V - 1.0)
        s0, s1 = iota((LIST, n), 0), iota((LIST, n), 1)
        u0, u1 = iota((LIST, layer), 0), iota((LIST, layer), 1)
        row_of = jnp.full((LIST, layer), -1, I32)
        col_of = jnp.full((LIST, n), -1, I32)
        for s in range(sh.slots):
            live = s < p_count[0, 0]
            row_of = jnp.where((u0 == s) & live, pw[0, s] - z * layer, row_of)
            col_of = jnp.where((s0 == s) & live, pw[1, s], col_of)
        own_rows, own_cols = ones(row_of == u1), ones(col_of == s1)
        left_2 = jnp.where(self.row_tile == j, self.slot_layer, sh.slots + pos_v)
        for step in range(2):
            if step == 0:
                oh_row, oh_col = stack([own_rows, extra_rows]), stack([own_cols, extra_cols])
                left, right, from_left, kind, cap, count = self.p_layer, self.hm, self.left_1, "H", CAP_1, LIST_1
            else:
                oh_row, oh_col = own_rows, own_cols
                left, right, from_left, kind, cap, count = self.f_layer, self.pm, left_2, "P", CAP_2, LIST
            w = mm(oh_row, left) * mt(oh_col, right)
            rows, lanes, starts, ends, _ = self.enumerate(w, count)
            over = over + total_over(ends, cap)
            k = w.shape[0]
            at = iota((count, k), 0).astype(F32)
            eight = jnp.ones((EIGHT, n), F32)
            lines = (
                mt(eight, lanes * mm(rows, mm(oh_row, from_left * left))),
                mt(eight, lanes * mm(rows, mt(oh_col, self.pos[kind]))),
                mt(jnp.ones((EIGHT, k), F32), rows * ones(at > starts)),
                jnp.where(ends > starts, jnp.minimum(ends - 1.0, cap), 1.0 * cap),
            )
            for q, line in enumerate(lines):
                size = line.shape[1]
                tab[2 + step : 3 + step, 32 * q : 32 * q + size] = line[0:1].astype(I32)
        return over


def sparse_products(
    sh, p_hbm, h_hbm, pw_hbm, pc_hbm, hw_hbm, hc_hbm, out, e_out, over_out,
    p_ref, h_ref, pw, pc, hw, hc,
    message, messages, near_h, near_p, store_h, store_p, prow, pack_r, pack_hz, pack_pz, pack_h, pack_p,
    pack_d, land_d, land_h, land_p, terms_1, terms_2, fstore, tabv_z, tabv_r, tabv_h, tabv, tab_z, tab_r, tab_h, tab, emsg, emsgs,
    m_send, m_recv, s_send, s_recv, p_send, p_fwd, p_recv, z_send, z_recv,
    t_send, t_recv, d_send, d_recv, e_send, e_recv, t_copy, fetch,
):
    i, j = lax.axis_index("row"), lax.axis_index("col")
    x, z = i % sh.inner, i // sh.inner
    me = i * sh.cols + j
    chip, core = j // 2, j % 2
    mate = (i, chip * 2 + 1 - core)
    team = x * sh.cols + j
    slots, strip, size = sh.slots, sh.strip, sh.size
    all_but_me = sh.devices - 1

    def member(d):
        e = sh.team - d
        qx = (x + e // sh.cols) % sh.inner
        qj = (chip + (e // 2) % sh.chips) % sh.chips * 2 + (core + e % 2) % 2
        return qx * sh.cols + qj, (z * sh.inner + qx, qj)

    def for_others(act):
        for t in range(sh.outer - 1):
            zt = sh.layer_at(z, t)

            @pl.loop(0, sh.team)
            def _(q):
                act((zt * sh.inner + q // sh.cols, q % sh.cols))

        @pl.loop(1, sh.team)
        def _(d):
            act(member(d)[1])

    def in_strip(q):
        return pl.ds(pl.multiple_of(q * strip, strip), strip)

    fetches = [
        pltpu.make_async_copy(source, target, fetch.at[k])
        for k, (source, target) in enumerate(
            (
                (pw_hbm, pw), (pc_hbm, pc), (hw_hbm, hw), (hc_hbm, hc),
                (h_hbm, h_ref), (p_hbm, p_ref),
            )
        )
    ]
    for copy in fetches:
        copy.start()
    barrier = pltpu.get_barrier_semaphore()

    for_others(lambda dev: pl.semaphore_signal(barrier, inc=1, device_id=dev, device_id_type=MESH))

    for copy in fetches[:4]:
        copy.wait()
    lane = iota((1, 128), 1)
    packed = jnp.zeros((1, 128), F32)
    for where, count, scale in ((pw, pc, 1.0), (hw, hc, 16.0)):
        for s in range(slots):
            at = (where[0, s] - i * TILE) * sh.width + where[1, s] - j * sh.width
            packed = packed + jnp.where((lane == at) & (s < count[0, 0]), scale * (s + 1), 0.0)
    message[0] = packed
    messages[me] = packed
    for copy in fetches[4:]:
        copy.wait()
    for s in range(slots):
        near_h[team * slots + s] = h_ref[s, in_strip(team), :]
        near_p[team * slots + s] = p_ref[s, in_strip(team), :]
        prow[s] = p_ref[s]
    pl.semaphore_wait(barrier, all_but_me)

    def tell(dev):
        remote(message.at[pl.ds(0, 1)], messages.at[pl.ds(me, 1)], m_send, m_recv, dev).start()

    for_others(tell)

    def strips(d, which):
        q, dev = member(d)
        ref, near = ((h_ref, near_h), (p_ref, near_p))[which]
        return remote(
            ref.at[:, in_strip(q), :], near.at[pl.ds(team * slots, slots)],
            s_send.at[which, d], s_recv.at[which, team], dev,
        )

    def strips_in(d, which):
        q, dev = member(d)
        ref, near = ((h_ref, near_h), (p_ref, near_p))[which]
        return remote(
            ref.at[:, in_strip(q), :], near.at[pl.ds(q * slots, slots)],
            s_send.at[which, d], s_recv.at[which, q], dev,
        )

    for which in range(2):
        for d in range(1, sh.team):
            strips(d, which).start()

    def other(dc):
        c = (chip + dc) % sh.chips
        return c, c * 2 + core

    p_mate = remote(p_ref, prow.at[pl.ds(slots, slots)], p_send.at[0], p_recv.at[sh.cols], mate)
    p_mate.start()

    def p_block(col):
        return prow.at[pl.ds(sh.others + col * CAP_R, CAP_R)]

    def p_out(dc):
        return remote(pack_r.at[dc - 1], p_block(j), p_send.at[dc], p_recv.at[j], (i, other(dc)[1]))

    def p_in(dc):
        col = other(dc)[1]
        return remote(pack_r.at[dc - 1], p_block(col), p_send.at[dc], p_recv.at[col], (i, col))

    def p_forward(dc):
        col = other(dc)[1]
        return remote(p_block(col), p_block(col), p_fwd.at[dc], p_recv.at[col], mate)

    def p_forward_in(dc):
        col = other(dc)[0] * 2 + 1 - core
        return remote(p_block(col), p_block(col), p_fwd.at[dc], p_recv.at[col], mate)

    def bulk(ref, sem):
        part = ref.at[pl.ds(0, all_but_me)]
        return pltpu.make_async_copy(part, part, sem)

    bulk(messages, m_recv).wait()
    lists = Lists(sh, x, z, j, messages[:, 0, :])

    def publish(source, target, which):
        copy = pltpu.make_async_copy(source, target, t_copy.at[which])
        copy.start()
        copy.wait()

    def entry(ref, table, row, lane):
        return ref[jnp.minimum(jnp.maximum(table[row, lane], 0), ref.shape[0] - 1)]

    kinds = (
        (store_h, pack_hz, pack_h, land_h, CAP_H_Z, CAP_H, near_h, tab_h),
        (store_p, pack_pz, pack_p, land_p, CAP_P_Z, CAP_P, near_p, tab),
    )

    def zone(which, layer):
        store, cap = kinds[which][0], kinds[which][4]
        return store.at[pl.ds(sh.team * slots + layer * cap, cap)]

    def across(which, dz):
        pack = kinds[which][1]
        zd = sh.layer_at(z, dz - 1)
        return remote(
            pack.at[dz - 1], zone(which, z), z_send.at[which, dz], z_recv.at[which, z],
            (zd * sh.inner + x, j),
        )

    def across_in(which, dz):
        pack = kinds[which][1]
        zs = sh.layer_at(z, dz - 1)
        return remote(
            pack.at[dz - 1], zone(which, zs), z_send.at[which, dz], z_recv.at[which, zs],
            (zs * sh.inner + x, j),
        )

    def part(which, d):
        pack, land = kinds[which][2], kinds[which][3]
        _, dev = member(d)
        return remote(
            pack.at[d - 1], land.at[:, in_strip(team), :], t_send.at[which, d], t_recv.at[which, team], dev
        )

    def part_in(which, d):
        pack, land = kinds[which][2], kinds[which][3]
        q, dev = member(d)
        return remote(
            pack.at[d - 1], land.at[:, in_strip(q), :], t_send.at[which, d], t_recv.at[which, q], dev
        )

    def send_across(which):
        store, pack, _, _, cap, _, near, _ = kinds[which]
        for d in range(1, sh.team):
            strips_in(d, which).wait_recv()
        for dz in range(1, sh.outer):
            for k in range(cap):
                pack[dz - 1, k] = entry(near, tab_z, which, (dz - 1) * LIST_Z + k)
        for dz in range(1, sh.outer):
            across(which, dz).start()
        store[0 : sh.team * slots] = near[...]

    def to_trace(xd):
        return remote(
            pack_d.at[xd], land_d.at[:, in_strip(team), :], d_send.at[xd], d_recv.at[team],
            (z * sh.inner + xd, sh.trace_member(z, xd) % sh.cols),
        )

    def trace_in(d):
        q, dev = member(d)
        return remote(pack_d.at[0], land_d.at[:, in_strip(q), :], d_send.at[0], d_recv.at[q], dev)

    def send_trace():
        for xd in range(sh.inner):
            for k in range(CAP_D):
                pack_d[xd, k] = entry(store_h, tab_h, 1, xd * EIGHT + k)
        for xd in range(sh.inner):
            @pl.when(sh.trace_member(z, xd) != team)
            def _():
                to_trace(xd).start()

            @pl.when(sh.trace_member(z, xd) == team)
            def _():
                for k in range(CAP_D):
                    land_d[k, in_strip(team), :] = pack_d[xd, k]

    def send_parts(which):
        store, _, pack, land, _, cap, _, table = kinds[which]
        for dz in range(1, sh.outer):
            across_in(which, dz).wait_recv()
        if which == 0:
            send_trace()

        @pl.loop(1, sh.team)
        def _(d):
            q, _ = member(d)
            for k in range(cap):
                pack[d - 1, k] = entry(store, table, 0, q * LIST + k)

        for d in range(1, sh.team):
            part(which, d).start()
        for k in range(cap):
            land[k, in_strip(team), :] = entry(store, table, 0, team * LIST + k)

    over = lists.across(tabv_z)
    publish(tabv_z, tab_z, 0)
    send_across(0)
    over = over + lists.row_lists(tabv_r)
    publish(tabv_r, tab_r, 1)
    for dc in range(1, sh.chips):
        for k in range(CAP_R):
            pack_r[dc - 1, k] = entry(p_ref, tab_r, 0, (dc - 1) * EIGHT + k)
    for dc in range(1, sh.chips):
        p_out(dc).start()
    over = over + lists.team_lists(0, tabv_h)
    publish(tabv_h, tab_h, 2)
    send_across(1)
    send_parts(0)
    for dc in range(1, sh.chips):
        p_in(dc).wait_recv()
        p_forward(dc).start()
    over = over + lists.team_lists(1, tabv)
    over = over + lists.products(pw, pc, tabv)
    publish(tabv, tab, 3)
    p_mate.wait_recv()
    for dc in range(1, sh.chips):
        p_forward_in(dc).wait_recv()
    emsg[0, 0] = jnp.zeros((1, 128), F32)

    @pl.when(sh.trace_member(z, x) == team)
    def _():
        for d in range(1, sh.team):
            trace_in(d).wait_recv()
        for k in range(CAP_D):
            part_of = entry(prow, tab_h, 2, k).astype(F32) * jnp.transpose(land_d[k].astype(F32))
            total = jnp.sum(part_of, axis=0, keepdims=True)
            emsg[0, 0] += total * tab_h[2, 32 + k].astype(F32)

    emsg[0, 1] = over + jnp.zeros((1, 128), F32)
    emsgs[me] = emsg[0]

    def tell_energy(dev):
        remote(emsg.at[pl.ds(0, 1)], emsgs.at[pl.ds(me, 1)], e_send, e_recv, dev).start()

    for_others(tell_energy)
    send_parts(1)

    def multiply(step, left, right, terms, cap):
        row = 2 + step
        acc = None
        for k in range(cap):
            d = jnp.dot(entry(left, tab, row, k), entry(right, tab, row, 32 + k), preferred_element_type=F32)
            acc = d if acc is None else d + acc * tab[row, 64 + k].astype(F32)
            terms[k] = acc
        terms[cap] = jnp.zeros((size, size), F32)

    for d in range(1, sh.team):
        part_in(0, d).wait_recv()
    multiply(0, prow, land_h, terms_1, CAP_1)
    for s in range(slots):
        value = entry(terms_1, tab, 2, 96 + s)
        rounded = value.astype(BF16)
        fstore[s] = rounded
        out[s] = rounded

    for k in range(CAP_V):
        fstore[slots + k] = entry(terms_1, tab, 2, 96 + LIST + k).astype(BF16)


    for d in range(1, sh.team):
        part_in(1, d).wait_recv()
    multiply(1, fstore, land_p, terms_2, CAP_2)
    for s in range(slots):
        out[slots + s] = entry(terms_2, tab, 3, 96 + s).astype(BF16)

    bulk(emsgs, e_recv).wait()
    e_out[...] = jnp.sum(jnp.sum(emsgs[:, 0], axis=0), axis=1, keepdims=True) + jnp.zeros((8, 128), F32)
    over_out[0, 0] = jnp.sum(jnp.sum(emsgs[:, 1], axis=0))

    bulk(messages, m_send).wait()
    bulk(emsgs, e_send).wait()
    for which in range(2):
        for d in range(1, sh.team):
            strips(d, which).wait_send()
            part(which, d).wait_send()
        for dz in range(1, sh.outer):
            across(which, dz).wait_send()
    for xd in range(sh.inner):
        @pl.when(sh.trace_member(z, xd) != team)
        def _():
            to_trace(xd).wait_send()
    p_mate.wait_send()
    for dc in range(1, sh.chips):
        p_out(dc).wait_send()
        p_forward(dc).wait_send()


def sparse_path(sh, p_values, p_where, p_count, h_values, h_where, h_count):
    slots, size, strip = sh.slots, sh.size, sh.strip
    block, piece = (size, size), (strip, size)
    bf = lambda *shape: pltpu.VMEM(shape, BF16)
    f32 = lambda *shape: pltpu.VMEM(shape, F32)
    dma = pltpu.SemaphoreType.DMA
    near = sh.team * slots
    away = max(sh.outer - 1, 1)
    chips = max(sh.chips - 1, 1)
    scalar = jax.ShapeDtypeStruct((1, 1), F32)
    return pl.pallas_call(
        functools.partial(sparse_products, sh),
        out_shape=[jax.ShapeDtypeStruct((2 * slots,) + block, BF16), jax.ShapeDtypeStruct((8, 128), F32), scalar],
        in_specs=[ANY] * 6,
        out_specs=[VMEM, VMEM, SMEM],
        scratch_shapes=[
            bf(slots, *block),
            bf(slots, *block),
            pltpu.SMEM((2, slots), I32),
            pltpu.SMEM((1, 1), I32),
            pltpu.SMEM((2, slots), I32),
            pltpu.SMEM((1, 1), I32),
            f32(1, 1, 128),
            f32(sh.devices, 1, 128),
            bf(near, *piece),
            bf(near, *piece),
            bf(near + sh.outer * CAP_H_Z, *piece),
            bf(near + sh.outer * CAP_P_Z, *piece),
            bf(sh.others + sh.cols * CAP_R, *block),
            bf(chips, CAP_R, *block),
            bf(away, CAP_H_Z, *piece),
            bf(away, CAP_P_Z, *piece),
            bf(sh.team, CAP_H, *piece),
            bf(sh.team, CAP_P, *piece),
            bf(sh.inner, CAP_D, *piece),
            bf(CAP_D, *block),
            bf(CAP_H, *block),
            bf(CAP_P, *block),
            f32(CAP_1 + 1, *block),
            f32(CAP_2 + 1, *block),
            bf(slots + CAP_V, *block),
            pltpu.VMEM((8, 128), I32),
            pltpu.VMEM((8, 128), I32),
            pltpu.VMEM((8, 128), I32),
            pltpu.VMEM((8, 128), I32),
            pltpu.SMEM((8, 128), I32),
            pltpu.SMEM((8, 128), I32),
            pltpu.SMEM((8, 128), I32),
            pltpu.SMEM((8, 128), I32),
            f32(1, 2, 1, 128),
            f32(sh.devices, 2, 1, 128),
            dma, dma,
            dma((2, sh.team)), dma((2, sh.team)),
            dma((sh.chips,)), dma((sh.chips,)), dma((sh.cols + 1,)),
            dma((2, sh.outer)), dma((2, sh.outer)),
            dma((2, sh.team)), dma((2, sh.team)),
            dma((sh.inner,)), dma((sh.team,)),
            dma, dma, dma((4,)), dma((6,)),
        ],
        compiler_params=pltpu.CompilerParams(collective_id=2, has_side_effects=True, vmem_limit_bytes=24 << 20),
        name="sparse_products",
    )(p_values, h_values, p_where.T, p_count, h_where.T, h_count)


def deliver(both, energy):
    def kernel(both_ref, e_in, first, second, e_out, e_one, sems):
        slots = first.shape[0]
        e_one[...] = e_in[0:1, 0:1]
        moves = (
            (both_ref.at[pl.ds(0, slots)], first),
            (both_ref.at[pl.ds(slots, slots)], second),
            (e_one, e_out),
        )
        copies = [pltpu.make_async_copy(*move, sems.at[k]) for k, move in enumerate(moves)]
        for copy in copies:
            copy.start()
        for copy in copies:
            copy.wait()

    half = jax.ShapeDtypeStruct((both.shape[0] // 2,) + both.shape[1:], both.dtype)
    return pl.pallas_call(
        kernel,
        out_shape=[half, half, jax.ShapeDtypeStruct((1, 1), F32)],
        in_specs=[VMEM, VMEM],
        out_specs=[ANY, ANY, ANY],
        scratch_shapes=[pltpu.VMEM((1, 1), F32), pltpu.SemaphoreType.DMA((3,))],
        name="deliver",
    )(both, energy)


def per_device(rows, cols, *args):
    slots, size, _ = args[0].shape
    sh = Shape(rows, cols, slots, size)
    if not sh.fits():
        return dense_path(rows, cols, *args)
    both, energy, over = sparse_path(sh, *args)
    def dense():
        ph, php, total = dense_path(rows, cols, *args)
        return ph, php, total.reshape((1, 1))

    ph, php, energy = lax.cond(over[0, 0] > 0.0, dense, lambda: tuple(deliver(both, energy)))
    return ph, php, energy[0, 0]


def solution(mesh):
    placed = (
        P("row", "col", None),
        P("row", "col"),
        P("row", "col"),
        P("row", "col", None),
        P("row", "col"),
        P("row", "col"),
    )
    return jax.shard_map(
        functools.partial(per_device, mesh.shape["row"], mesh.shape["col"]),
        mesh=mesh,
        in_specs=placed,
        out_specs=(P("row", "col", None), P("row", "col", None), P()),
        check_vma=False,
    )
```

```python
import functools

import jax
import jax.numpy as jnp
from jax import lax
from jax.experimental import pallas as pl
from jax.experimental.pallas import tpu as pltpu
from jax.sharding import PartitionSpec as P

TILE = 8
CHUNKS = 6
IN_FLIGHT = 16
MESH = pl.DeviceIdType.MESH
ANY = pl.BlockSpec(memory_space=pl.ANY)
VMEM = pl.BlockSpec(memory_space=pltpu.VMEM)
SMEM = pl.BlockSpec(memory_space=pltpu.SMEM)


def at_row(r):
    return (r, lax.axis_index("col"))


def at_col(c):
    return (lax.axis_index("row"), c)


def remote(src, dst, send_sem, recv_sem, device):
    return pltpu.make_async_remote_copy(
        src_ref=src,
        dst_ref=dst,
        send_sem=send_sem,
        recv_sem=recv_sem,
        device_id=device,
        device_id_type=MESH,
    )


def greet(rows, cols):
    me_row, me_col = lax.axis_index("row"), lax.axis_index("col")
    barrier = pltpu.get_barrier_semaphore()
    for d in range(1, rows):
        pl.semaphore_signal(
            barrier, inc=1, device_id=at_row((me_row + d) % rows), device_id_type=MESH
        )
    for d in range(1, cols):
        pl.semaphore_signal(
            barrier, inc=1, device_id=at_col((me_col + d) % cols), device_id_type=MESH
        )
    pl.semaphore_wait(barrier, rows + cols - 2)


class ColumnGather:
    def __init__(self, rows, own, land, out, up_send, down_send, x_send, recv, local):
        self.own, self.land, self.out = own, land, out
        self.up_send, self.down_send, self.x_send = up_send, down_send, x_send
        self.recv, self.local = recv, local
        self.inner = 2 if rows % 2 == 0 else 1
        self.outer = rows // self.inner
        self.chunks = recv.shape[1]
        self.size = own.shape[0] // self.chunks
        self.me = lax.axis_index("row")
        self.x, self.z = self.me % self.inner, self.me // self.inner
        self.cross_first = 1 if self.inner == 2 and self.chunks > 1 else 0

    def later(self, ch):
        return (ch + self.cross_first) % self.chunks

    def row(self, z, line):
        return z * self.inner + (self.x if line == 0 else self.inner - 1 - self.x)

    def part(self, ch):
        return pl.ds(ch * self.size, self.size)

    def copy(self, r, ch, own, way):
        sems, target = {
            "up": (self.up_send, self.me + self.inner),
            "down": (self.down_send, self.me - self.inner),
            "x": (self.x_send, self.row(self.z, 1)),
        }[way]
        part = self.part(ch)
        src = self.own.at[part] if own else self.land.at[r, part]
        return remote(src, self.land.at[r, part], sems.at[r, ch], self.recv.at[r, ch], at_row(target))

    def keep(self, r, ch):
        part = self.part(ch)
        return pltpu.make_async_copy(self.land.at[r, part], self.out.at[r, part], self.local.at[r, ch])

    def along(self, r, ch, own, act):
        @pl.when(self.z < self.outer - 1)
        def _():
            act(self.copy(r, ch, own, "up"))

        @pl.when(self.z > 0)
        def _():
            act(self.copy(r, ch, own, "down"))

    def arrive(self, r, ch):
        self.copy(r, ch, False, "x").wait_recv()
        self.keep(r, ch).start()

    def start(self):
        for ch in range(self.chunks):
            if self.inner == 2:
                self.copy(self.me, ch, True, "x").start()
            self.along(self.me, self.later(ch), True, lambda copy: copy.start())
        if self.cross_first:
            r = self.row(self.z, 1)
            self.arrive(r, 0)
            self.along(r, 0, False, lambda copy: copy.start())

    def pieces(self):
        lines = [(self.later(ch), 0) for ch in range(self.chunks)]
        return lines + [(0, 1)] * self.cross_first

    def relayed(self, d, side, ch, line, act):
        z = self.z - d if side == 0 else self.z + d
        there = self.z >= d if side == 0 else self.z + d < self.outer
        r = self.row(z, line)

        @pl.when(there)
        def _():
            if act == "start":
                self.arrive(r, ch)
            on = self.z < self.outer - 1 if side == 0 else self.z > 0

            @pl.when(on)
            def _():
                copy = self.copy(r, ch, False, "up" if side == 0 else "down")
                copy.start() if act == "start" else copy.wait_send()

            if self.inner == 2 and ch >= self.cross_first:
                copy = self.copy(r, ch, False, "x")
                copy.start() if act == "start" else copy.wait_send()

    def relay(self, d):
        for ch, line in self.pieces():
            for side in range(2):
                self.relayed(d, side, ch, line, "start")

    def finish(self):
        if self.inner == 2:
            for ch in range(self.cross_first, self.chunks):
                self.arrive(self.row(self.z, 1), ch)
            for d in range(1, self.outer):
                for side in range(2):
                    z = self.z - d if side == 0 else self.z + d
                    there = self.z >= d if side == 0 else self.z + d < self.outer

                    @pl.when(there)
                    def _():
                        for ch in range(self.cross_first, self.chunks):
                            self.arrive(self.row(z, 1), ch)
        for ch in range(self.chunks):
            if self.inner == 2:
                self.copy(self.me, ch, True, "x").wait_send()
            self.along(self.me, ch, True, lambda copy: copy.wait_send())
        if self.cross_first:
            self.along(self.row(self.z, 1), 0, False, lambda copy: copy.wait_send())
        for d in range(1, self.outer):
            for ch, line in self.pieces():
                for side in range(2):
                    self.relayed(d, side, ch, line, "wait")
        for r in range(self.inner * self.outer):
            @pl.when(r != self.me)
            def _():
                for ch in range(self.chunks):
                    self.keep(r, ch).wait()


def col_copies(cols, own, out, send, recv):
    me = lax.axis_index("col")
    made = []
    for d in range(1, cols):
        made.append(
            remote(own, out.at[me], send.at[d], recv.at[d], at_col((me + d) % cols))
        )
    return made


def row_copies(rows, own, out, send, recv):
    me = lax.axis_index("row")
    made = []
    for d in range(1, rows):
        made.append(
            remote(own, out.at[me], send.at[d], recv.at[d], at_row((me + d) % rows))
        )
    return made


def first_gather(
    rows, cols, p_ref, h_ref, meta_ref, prow, hcol, prow_meta, col_meta,
    land, up_send, down_send, x_send, recv, out_sems,
    p_send, p_recv, mc_send, mc_recv, mr_send, mr_recv, local,
):
    me_row, me_col = lax.axis_index("row"), lax.axis_index("col")
    keep = [
        pltpu.make_async_copy(h_ref, hcol.at[me_row], local.at[0]),
        pltpu.make_async_copy(p_ref, prow.at[me_col], local.at[1]),
        pltpu.make_async_copy(meta_ref, prow_meta.at[me_col], local.at[2]),
        pltpu.make_async_copy(meta_ref, col_meta.at[me_row], local.at[3]),
    ]
    greet(rows, cols)
    gather = ColumnGather(
        rows, h_ref, land, hcol, up_send, down_send, x_send, recv, out_sems
    )
    across = (
        col_copies(cols, p_ref, prow, p_send, p_recv)
        + col_copies(cols, meta_ref, prow_meta, mc_send, mc_recv)
        + row_copies(rows, meta_ref, col_meta, mr_send, mr_recv)
    )
    for copy in across + keep:
        copy.start()
    gather.start()
    for d in range(1, gather.outer):
        gather.relay(d)
    gather.finish()
    for copy in across + keep:
        copy.wait()


def second_gather(
    rows, cols, p_ref, f_ref, e_ref, frow, pcol, e_out,
    e_cols, e_rows, e_sum,
    land, up_send, down_send, x_send, recv, out_sems,
    p_send, p_recv, ec_send, ec_recv, er_send, er_recv, local,
):
    me_row, me_col = lax.axis_index("row"), lax.axis_index("col")
    keep = [
        pltpu.make_async_copy(p_ref, pcol.at[me_row], local.at[0]),
        pltpu.make_async_copy(f_ref, frow.at[me_col], local.at[1]),
    ]
    greet(rows, cols)
    energies = col_copies(cols, e_ref, e_cols, ec_send, ec_recv)
    for copy in energies:
        copy.start()
    gather = ColumnGather(
        rows, p_ref, land, pcol, up_send, down_send, x_send, recv, out_sems
    )
    across = col_copies(cols, f_ref, frow, p_send, p_recv)
    for copy in across + keep:
        copy.start()
    gather.start()
    e_cols[me_col] = e_ref[...]
    for copy in energies:
        copy.wait()
    total = e_cols[0]
    for c in range(1, cols):
        total = total + e_cols[c]
    e_sum[...] = total
    e_rows[me_row] = total
    if gather.outer > 1:
        gather.relay(1)
    sums = row_copies(rows, e_sum, e_rows, er_send, er_recv)
    for copy in sums:
        copy.start()
    for d in range(2, gather.outer):
        gather.relay(d)
    for copy in sums:
        copy.wait()
    total = e_rows[0]
    for r in range(1, rows):
        total = total + e_rows[r]
    e_out[...] = total
    gather.finish()
    for copy in across + keep:
        copy.wait()


def block_products(
    rows, cols, right_lane, with_trace, lmeta, rmeta, left, right, *rest
):
    if with_trace:
        out, e_out = rest[:2]
    else:
        e_in, out, e_out = rest[:3]
    acc, lbuf, rbuf, head, nxt, inner, mask, table, ml, mr, ms, sems = rest[-12:]
    slots = out.shape[0]
    i, j = lax.axis_index("row"), lax.axis_index("col")
    nblk = rows * TILE
    tile_cols = nblk // cols
    words = -(-nblk // 32)
    count_lane = 4 * slots
    acc[...] = jnp.zeros_like(acc)

    for t in range(TILE + 1):
        head[t] = -1

    for t in range(tile_cols * words + 1):
        mask[t] = 0

    @pl.loop(0, cols)
    def _(c):
        live = lmeta[c, 0, count_lane]
        for s in range(slots):
            row = jnp.where(s < live, lmeta[c, 0, s] - i * TILE, TILE)
            idx = c * slots + s
            inner[idx] = lmeta[c, 0, slots + s]
            nxt[idx] = head[row]
            head[row] = idx

    @pl.loop(0, rows)
    def _(r):
        live = rmeta[r, 0, count_lane + (1 if right_lane else 0)]
        for s in range(slots):
            k = rmeta[r, 0, right_lane + s]
            col = rmeta[r, 0, right_lane + slots + s] - j * tile_cols
            word = jnp.where(s < live, col * words + (k >> 5), tile_cols * words)
            mask[word] = mask[word] | (jnp.int32(1) << (k & 31))
            table[jnp.where(s < live, k * tile_cols + col, nblk * tile_cols)] = r * slots + s

    def find_slot(s, n):
        row = lmeta[j, 0, s] - i * TILE
        col = lmeta[j, 0, slots + s] - j * tile_cols

        def more(state):
            return state[0] >= 0

        def step(state):
            at, n = state
            k = inner[at]
            ml[n] = at
            mr[n] = table[k * tile_cols + col]
            ms[n] = s
            return nxt[at], n + ((mask[col * words + (k >> 5)] >> (k & 31)) & 1)

        return lax.while_loop(more, step, (head[row], n))[1]

    own_count = lmeta[j, 0, count_lane]
    found = lax.fori_loop(0, own_count, find_slot, jnp.int32(0))

    def fetch(base, m):
        a, b = ml[base + m], mr[base + m]
        return (
            pltpu.make_async_copy(left.at[a], lbuf.at[m], sems.at[0, m]),
            pltpu.make_async_copy(right.at[b], rbuf.at[m], sems.at[1, m]),
        )

    @pl.loop(0, (found + IN_FLIGHT - 1) // IN_FLIGHT)
    def _(chunk):
        base = chunk * IN_FLIGHT
        size = jnp.minimum(found - base, IN_FLIGHT)

        @pl.loop(0, size)
        def _(m):
            for copy in fetch(base, m):
                copy.start()

        @pl.loop(0, size)
        def _(m):
            for copy in fetch(base, m):
                copy.wait()
            s = ms[base + m]
            acc[s] += jnp.dot(lbuf[m], rbuf[m], preferred_element_type=jnp.float32)

    out[...] = acc[...].astype(out.dtype)
    if with_trace:
        size = acc.shape[1]
        e_out[...] = jnp.zeros_like(e_out)
        diagonal = lax.broadcasted_iota(jnp.int32, (size, size), 0) == lax.broadcasted_iota(
            jnp.int32, (size, size), 1
        )

        @pl.loop(0, own_count)
        def _(s):
            @pl.when(lmeta[j, 0, s] == lmeta[j, 0, slots + s])
            def _():
                e_out[...] += jnp.sum(jnp.where(diagonal, acc[s], 0.0))
    else:
        e_out[0, 0] = e_in[0, 0]


def dense_path(rows, cols, p_values, p_where, p_count, h_values, h_where, h_count):
    slots, size, _ = p_values.shape
    dtype = p_values.dtype
    nblk = rows * TILE
    tile_cols = nblk // cols
    words = -(-nblk // 32)
    meta = jnp.concatenate(
        [p_where[:, 0], p_where[:, 1], h_where[:, 0], h_where[:, 1], p_count[0], h_count[0]]
    )
    meta = jnp.broadcast_to(jnp.pad(meta, (0, 128 - meta.shape[0]))[None, :], (8, 128))
    dma = pltpu.SemaphoreType.DMA
    chunks = CHUNKS if slots % CHUNKS == 0 else 1
    chunk_sems = [pltpu.VMEM((rows, slots, size, size), dtype)] + [dma((rows, chunks))] * 5
    col_sems = [dma((cols,)), dma((cols,))]
    row_sems = [dma((rows,)), dma((rows,))]
    tile = (slots, size, size)
    prow, hcol, prow_meta, col_meta = pl.pallas_call(
        functools.partial(first_gather, rows, cols),
        out_shape=[
            jax.ShapeDtypeStruct((cols,) + tile, dtype),
            jax.ShapeDtypeStruct((rows,) + tile, dtype),
            jax.ShapeDtypeStruct((cols, 8, 128), jnp.int32),
            jax.ShapeDtypeStruct((rows, 8, 128), jnp.int32),
        ],
        in_specs=[VMEM] * 3,
        out_specs=[ANY] * 4,
        scratch_shapes=chunk_sems + col_sems + col_sems + row_sems + [dma((4,))],
        compiler_params=pltpu.CompilerParams(collective_id=0, has_side_effects=True),
        name="first_gather",
    )(p_values, h_values, meta)

    def products(right_lane, with_trace, lmeta, rmeta, left, right, *more):
        smem = lambda n: pltpu.SMEM((n,), jnp.int32)
        most = slots * nblk + 1
        return pl.pallas_call(
            functools.partial(block_products, rows, cols, right_lane, with_trace),
            out_shape=[
                jax.ShapeDtypeStruct(tile, dtype),
                jax.ShapeDtypeStruct((8, 128) if with_trace else (1, 1), jnp.float32),
            ],
            in_specs=[SMEM, SMEM, ANY, ANY] + [SMEM] * len(more),
            out_specs=[VMEM, VMEM if with_trace else SMEM],
            scratch_shapes=[
                pltpu.VMEM(tile, jnp.float32),
                pltpu.VMEM((IN_FLIGHT, size, size), dtype),
                pltpu.VMEM((IN_FLIGHT, size, size), dtype),
                smem(TILE + 1),
                smem(cols * slots),
                smem(cols * slots),
                smem(tile_cols * words + 1),
                smem(nblk * tile_cols + 1),
                smem(most),
                smem(most),
                smem(most),
                dma((2, IN_FLIGHT)),
            ],
            name="products",
        )(
            lmeta,
            rmeta,
            left.reshape((cols * slots, size, size)),
            right.reshape((rows * slots, size, size)),
            *more,
        )

    ph_values, part = products(2 * slots, True, prow_meta, col_meta, prow, hcol)
    frow, pcol, energy = pl.pallas_call(
        functools.partial(second_gather, rows, cols),
        out_shape=[
            jax.ShapeDtypeStruct((cols,) + tile, dtype),
            jax.ShapeDtypeStruct((rows,) + tile, dtype),
            jax.ShapeDtypeStruct((8, 128), jnp.float32),
        ],
        in_specs=[VMEM] * 3,
        out_specs=[ANY, ANY, VMEM],
        scratch_shapes=[
            pltpu.VMEM((cols, 8, 128), jnp.float32),
            pltpu.VMEM((rows, 8, 128), jnp.float32),
            pltpu.VMEM((8, 128), jnp.float32),
        ]
        + chunk_sems + col_sems + col_sems + row_sems + [dma((2,))],
        compiler_params=pltpu.CompilerParams(collective_id=1, has_side_effects=True),
        name="second_gather",
    )(p_values, ph_values, part)
    php_values, energy = products(0, False, prow_meta, col_meta, frow, pcol, energy)
    return (ph_values, php_values, energy[0, 0])


CAP_H_Z, CAP_P_Z = 16, 12
CAP_H, CAP_P = 14, 9
CAP_R, CAP_V, CAP_D = 7, 7, 3
CAP_1, CAP_2 = 18, 12
LIST, LIST_Z, LIST_1, EIGHT = 16, 24, 24, 8
F32, BF16, I32 = jnp.float32, jnp.bfloat16, jnp.int32


def log2(n):
    return n.bit_length() - 1


def power(n):
    return n > 0 and n & (n - 1) == 0


class Shape:
    def __init__(self, rows, cols, slots, size):
        self.rows, self.cols, self.slots, self.size = rows, cols, slots, size
        self.devices = rows * cols
        self.nblk = rows * TILE
        self.inner = 2 if rows % 2 == 0 else 1
        self.outer = rows // self.inner
        self.layer = self.inner * TILE
        self.team = self.inner * cols
        self.strip = size // self.team
        self.width = self.nblk // cols
        self.chips = cols // 2
        self.others = 2 * slots

    def trace_member(self, z, xd):
        return xd * self.cols + (z * self.inner + xd) * TILE // self.width

    def layer_at(self, z, t):
        down = self.outer - 1 - t
        return jnp.where(
            z < self.outer // 2,
            down - jnp.where(down <= z, 1, 0),
            t + jnp.where(t >= z, 1, 0),
        )

    def fits(self):
        return (
            power(self.rows)
            and power(self.cols)
            and self.cols >= 2
            and self.outer >= 2
            and self.nblk <= 64
            and TILE <= self.width <= 128 // TILE
            and self.slots <= 15
            and self.strip % 16 == 0
            and self.team * LIST <= 128
            and (self.outer - 1) * LIST_Z <= 128
            and (self.chips - 1) * EIGHT <= 128
        )


def mm(a, b):
    return lax.dot_general(a.astype(BF16), b.astype(BF16), (((1,), (0,)), ((), ())), preferred_element_type=F32)


def mt(a, b):
    return lax.dot_general(a.astype(BF16), b.astype(BF16), (((1,), (1,)), ((), ())), preferred_element_type=F32)


def tm(a, b):
    return lax.dot_general(a.astype(BF16), b.astype(BF16), (((0,), (0,)), ((), ())), preferred_element_type=F32)


def ones(cond):
    return jnp.where(cond, 1.0, 0.0).astype(F32)


def iota(shape, dim):
    return lax.broadcasted_iota(I32, shape, dim)


def block_index(shape, dim, size):
    return iota(shape, dim) // size


def total_over(ends, cap):
    over = ones(ends > cap + 0.5)
    return jnp.sum(jnp.sum(over, axis=0, keepdims=True), axis=1, keepdims=True)


def stack(parts):
    return jnp.concatenate(parts, axis=0)


class Lists:
    def __init__(self, sh, x, z, j, message):
        self.sh, self.x, self.z, self.j = sh, x, z, j
        n, width, layer = sh.nblk, sh.width, sh.layer
        lw = log2(width)
        r, l = iota((n, n), 0), iota((n, n), 1)
        a0, d0 = iota((sh.cols * n, sh.devices), 0), iota((sh.cols * n, sh.devices), 1)
        spread = mm(ones(d0 == ((a0 & (n - 1)) >> 3) * sh.cols + (a0 >> log2(n))), message)
        a1, l1 = iota((sh.cols * n, 128), 0), iota((sh.cols * n, 128), 1)
        spread = jnp.where((l1 >> lw) == (a1 & 7), spread, 0.0)
        l2, m2 = iota((128, n), 0), iota((128, n), 1)
        spread = mm(spread, ones((l2 & (width - 1)) == (m2 & (width - 1))))
        both = jnp.zeros((n, n), F32)
        for c in range(sh.cols):
            both = both + jnp.where((l >> lw) == c, spread[c * n : (c + 1) * n], 0.0)
        hs = jnp.floor(both * (1.0 / 16.0))
        ps = both - 16.0 * hs
        self.pos = {}
        self.pm, self.hm = ones(ps > 0.5), ones(hs > 0.5)
        self.fm = self.pm * ones(mm(self.pm, self.hm) > 0.5)
        self.up, self.low, self.up_to = ones(r < l), ones(l < r), ones(r <= l)
        self.low_layer = ones((l < r) & (l // layer == r // layer))
        self.full = jnp.ones((n, n), F32)
        self.r, self.l, self.lane_tile = r, l, l >> lw
        team = ((r >> 3) & (sh.inner - 1)) * sh.cols + self.lane_tile
        at = (team * sh.slots).astype(F32)
        self.near = {"H": at + hs - 1.0, "P": at + ps - 1.0}
        s0, s1 = iota((layer, n), 0), iota((layer, n), 1)
        self.sel = ones(s1 == z * layer + s0)
        self.row_i, self.row_tile = s0, (s1 >> lw)
        self.p_layer, self.f_layer = mm(self.sel, self.pm), mm(self.sel, self.fm)
        self.slot_layer = mm(self.sel, ps) - 1.0

    def enumerate(self, v, count, lane_pos=None):
        k, n = v.shape
        counts = mt(jnp.ones((count, n), F32), v)
        a, b = iota((k, k), 0), iota((k, k), 1)
        starts, ends = mm(counts, ones(a < b)), mm(counts, ones(a <= b))
        at = iota((count, k), 0).astype(F32)
        rows = ones((starts <= at) & (at < ends))
        local = mm(rows * (at - starts + 1.0), jnp.ones((k, n), F32))
        if lane_pos is None:
            lane_pos = mm(v, self.up)
        found = mm(rows, v * (lane_pos + 1.0))
        lanes = ones((found == local) & (local > 0.5))
        return rows, lanes, starts, ends, lane_pos

    def position(self, v, low):
        return mm(v, self.up) + mm(low, mm(v, self.full))

    def across(self, tab):
        sh, z, layer, n = self.sh, self.z, self.sh.layer, self.sh.nblk
        p_s, f_s = mt(self.sel, self.pm), mt(self.sel, self.fm)
        i_layer = self.l[0:layer] // layer
        lhs, live, pay = [], [], []
        for kind, left, right in (("H", p_s, self.hm), ("P", f_s, self.pm)):
            live_kind, pay_kind = mm(self.sel, right), mm(self.sel, self.near[kind])
            for dz in range(1, sh.outer):
                lhs.append(left * ones(i_layer == sh.layer_at(z, dz - 1)))
                live.append(live_kind)
                pay.append(pay_kind)
        v = ones(mm(stack(lhs), self.pm) > 0.5) * stack(live)
        k = v.shape[0]
        lists = 2 * (sh.outer - 1)
        a, b = iota((k, k), 0), iota((k, k), 1)
        counts = mt(jnp.ones((EIGHT, n), F32), v)
        starts = mm(counts, ones((a < b) & (a // layer == b // layer)))
        ends = mm(counts, ones((a <= b) & (a // layer == b // layer)))
        t0 = iota((lists * LIST_Z, k), 0)
        at = (t0 % LIST_Z).astype(F32)
        rows = ones(
            (starts[0:1] <= at)
            & (at < ends[0:1])
            & (t0 // LIST_Z == block_index((lists * LIST_Z, k), 1, layer))
        )
        local = mm(rows * (at - starts[0:1] + 1.0), jnp.ones((k, n), F32))
        found = mm(rows, v * (mm(v, self.up) + 1.0))
        picked = jnp.where((found == local) & (local > 0.5), mm(rows, stack(pay)), 0.0)
        half = (sh.outer - 1) * LIST_Z
        for which in range(2):
            line = mt(jnp.ones((EIGHT, n), F32), picked[which * half : (which + 1) * half])
            tab[which : which + 1, 0:half] = line[0:1].astype(I32)
        lane_h = block_index((EIGHT, k), 1, layer) < sh.outer - 1
        cap = jnp.where(lane_h, 1.0 * CAP_H_Z, 1.0 * CAP_P_Z)
        return total_over(ends - cap, 0.0)

    def row_lists(self, tab):
        sh, x, j, layer, n = self.sh, self.x, self.j, self.sh.layer, self.sh.nblk
        tiles = [ones(self.row_tile == c) for c in range(sh.cols)]
        wide = stack([self.p_layer * t for t in tiles])
        passed = ones(mt(wide, self.pm) > 0.5) * stack([self.f_layer] * sh.cols)
        own = wide
        self.outputs = jnp.maximum(own, passed)
        self.remote_f = passed * (1.0 - ones(stack([t for t in tiles]) > 0.5))
        reads = ones(mt(self.outputs, self.hm) > 0.5) * stack([self.p_layer] * sh.cols)
        mine = ones((self.row_i >> 3) == x)
        chip = j // 2
        low = ones(iota((layer, layer), 1) < iota((layer, layer), 0))
        seg_tri = ones((self.lane_tile == (self.r >> log2(sh.width))) & (self.r < self.l))
        seg_full = ones(self.lane_tile == (self.r >> log2(sh.width)))
        over = jnp.zeros((1, 1), F32)
        for dc in range(sh.chips):
            c = (chip + dc) % sh.chips
            v = jnp.zeros((layer, n), F32)
            for k in range(sh.cols):
                v = jnp.maximum(v, reads[k * layer : (k + 1) * layer] * jnp.where(k // 2 == c, 1.0, 0.0))
            v = v * mine
            if dc == 0:
                pos = mm(v, seg_tri) + mm(low, mm(v, seg_full))
                pos = jnp.minimum(pos, CAP_R - 1.0)
                continue
            v = v * ones(self.row_tile == j)
            rows, lanes, starts, ends, _ = self.enumerate(v, EIGHT)
            line = mt(jnp.ones((EIGHT, n), F32), lanes * mm(rows, self.slot_layer))
            tab[0:1, (dc - 1) * EIGHT : dc * EIGHT] = line[0:1].astype(I32)
            over = over + total_over(ends, CAP_R)
        self.left_1 = jnp.where(
            self.row_tile == j,
            self.slot_layer,
            jnp.where(
                self.row_tile // 2 == chip,
                sh.slots + self.slot_layer,
                sh.others + self.row_tile.astype(F32) * CAP_R + pos,
            ),
        )
        return over

    def team_lists(self, which, tab):
        sh, x, z, j, layer, n = self.sh, self.x, self.z, self.j, self.sh.layer, self.sh.nblk
        a, b = iota((layer, layer), 0), iota((layer, layer), 1)
        turn = lambda m: tm(m, ones(a == b))
        kind, cap_z, cap = (("H", CAP_H_Z, CAP_H), ("P", CAP_P_Z, CAP_P))[which]
        turned = turn(self.p_layer if kind == "H" else self.f_layer)
        live = self.hm if kind == "H" else self.pm
        lane_x = iota((n, layer), 1) >> 3
        k_layer = self.r // layer
        pos_z = self.position(ones(mm(turned, self.p_layer) > 0.5) * live, self.low_layer)
        far = (sh.team * sh.slots + k_layer * cap_z).astype(F32) + jnp.minimum(pos_z, cap_z - 1.0)
        payload = jnp.where(k_layer == z, self.near[kind], far)
        by_x = stack([turned * ones(lane_x == xd) for xd in range(sh.inner)])
        needs = []
        if kind == "H":
            made = [
                ones(mm(by_x, self.outputs[c * layer : (c + 1) * layer]) > 0.5) for c in range(sh.cols)
            ]
        else:
            one = ones(mm(by_x, self.p_layer) > 0.5)
            made = [one * ones((iota((sh.inner * n, n), 1) >> log2(sh.width)) == c) for c in range(sh.cols)]
        for xd in range(sh.inner):
            for c in range(sh.cols):
                needs.append(made[c][xd * n : (xd + 1) * n] * live)
        all_needs = stack(needs)
        lane_pos = mm(all_needs, self.up)
        counts = stack([mt(jnp.ones((LIST, n), F32), v) for v in needs])
        starts, ends = mm(counts, self.up), mm(counts, self.up_to)
        over = total_over(ends, cap)
        if kind == "H":
            over = over + self.trace_lists(payload, tab)
        at = (iota((sh.team * LIST, n), 0) % LIST).astype(F32)
        rows = ones((starts <= at) & (at < ends))
        local = mm(rows * (at - starts + 1.0), self.full)
        marked = all_needs * (lane_pos + 1.0)
        found = stack(
            [
                mm(rows[t * LIST : (t + 1) * LIST], marked[t * n : (t + 1) * n])
                for t in range(sh.team)
            ]
        )
        picked = jnp.where((found == local) & (local > 0.5), mm(rows, payload), 0.0)
        line = mt(jnp.ones((EIGHT, n), F32), picked)
        tab[0:1, 0 : sh.team * LIST] = line[0:1].astype(I32)
        me = x * sh.cols + j
        mine = jnp.zeros((n, n), F32)
        for t in range(sh.team):
            mine = mine + needs[t] * jnp.where(me == t, 1.0, 0.0)
        self.pos[kind] = jnp.minimum(self.position(mine, self.low), cap - 1.0)
        return over

    def trace_lists(self, payload, tab):
        sh, n = self.sh, self.sh.nblk
        eye = ones(self.r == self.l)
        diagonal = jnp.sum(self.pm * eye, axis=0, keepdims=True)
        every = tm(self.pm, eye) * self.hm * diagonal
        eight = jnp.ones((EIGHT, n), F32)
        over = jnp.zeros((1, 1), F32)
        mine_rows, mine_lanes = jnp.zeros((EIGHT, n), F32), jnp.zeros((EIGHT, n), F32)
        for xd in range(sh.inner):
            v = every * ones((self.l >> 3) == self.z * sh.inner + xd)
            rows, lanes, starts, ends, _ = self.enumerate(v, EIGHT)
            over = over + total_over(ends, CAP_D)
            line = mt(eight, lanes * mm(rows, payload))
            tab[1:2, xd * EIGHT : (xd + 1) * EIGHT] = line[0:1].astype(I32)
            here = jnp.where(self.x == xd, 1.0, 0.0)
            mine_rows, mine_lanes = mine_rows + here * rows, mine_lanes + here * lanes
        left = mm(mt(mine_lanes, self.sel), self.left_1 * self.p_layer) * mine_rows
        for q, value in enumerate((left, mine_rows)):
            line = mt(eight, value)
            tab[2:3, 32 * q : 32 * q + EIGHT] = line[0:1].astype(I32)
        return over

    def products(self, pw, p_count, tab):
        sh, x, z, j, layer, n = self.sh, self.x, self.z, self.j, self.sh.layer, self.sh.nblk
        v = jnp.zeros((layer, n), F32)
        for c in range(sh.cols):
            v = v + self.remote_f[c * layer : (c + 1) * layer] * jnp.where(c == j, 1.0, 0.0)
        v = v * ones((self.row_i >> 3) == x)
        extra_rows, extra_cols, starts, ends, lane_pos = self.enumerate(v, EIGHT)
        over = total_over(ends, CAP_V)
        low = ones(iota((layer, layer), 1) < iota((layer, layer), 0))
        pos_v = jnp.minimum(lane_pos + mm(low, mm(v, self.full)), CAP_V - 1.0)
        s0, s1 = iota((LIST, n), 0), iota((LIST, n), 1)
        u0, u1 = iota((LIST, layer), 0), iota((LIST, layer), 1)
        row_of = jnp.full((LIST, layer), -1, I32)
        col_of = jnp.full((LIST, n), -1, I32)
        for s in range(sh.slots):
            live = s < p_count[0, 0]
            row_of = jnp.where((u0 == s) & live, pw[0, s] - z * layer, row_of)
            col_of = jnp.where((s0 == s) & live, pw[1, s], col_of)
        own_rows, own_cols = ones(row_of == u1), ones(col_of == s1)
        left_2 = jnp.where(self.row_tile == j, self.slot_layer, sh.slots + pos_v)
        for step in range(2):
            if step == 0:
                oh_row, oh_col = stack([own_rows, extra_rows]), stack([own_cols, extra_cols])
                left, right, from_left, kind, cap, count = self.p_layer, self.hm, self.left_1, "H", CAP_1, LIST_1
            else:
                oh_row, oh_col = own_rows, own_cols
                left, right, from_left, kind, cap, count = self.f_layer, self.pm, left_2, "P", CAP_2, LIST
            w = mm(oh_row, left) * mt(oh_col, right)
            rows, lanes, starts, ends, _ = self.enumerate(w, count)
            over = over + total_over(ends, cap)
            k = w.shape[0]
            at = iota((count, k), 0).astype(F32)
            eight = jnp.ones((EIGHT, n), F32)
            lines = (
                mt(eight, lanes * mm(rows, mm(oh_row, from_left * left))),
                mt(eight, lanes * mm(rows, mt(oh_col, self.pos[kind]))),
                mt(jnp.ones((EIGHT, k), F32), rows * ones(at > starts)),
                jnp.where(ends > starts, jnp.minimum(ends - 1.0, cap), 1.0 * cap),
            )
            for q, line in enumerate(lines):
                size = line.shape[1]
                tab[2 + step : 3 + step, 32 * q : 32 * q + size] = line[0:1].astype(I32)
        return over


def sparse_products(
    sh, p_hbm, h_hbm, pw_hbm, pc_hbm, hw_hbm, hc_hbm, out, e_out, over_out,
    p_ref, h_ref, pw, pc, hw, hc,
    message, messages, near_h, near_p, store_h, store_p, prow, pack_r, pack_hz, pack_pz, pack_h, pack_p,
    pack_d, land_d, land_h, land_p, terms_1, terms_2, fstore, tabv_z, tabv_r, tabv_h, tabv, tab_z, tab_r, tab_h, tab, emsg, emsgs,
    m_send, m_recv, s_send, s_recv, p_send, p_fwd, p_recv, z_send, z_recv,
    t_send, t_recv, d_send, d_recv, e_send, e_recv, t_copy, fetch,
):
    i, j = lax.axis_index("row"), lax.axis_index("col")
    x, z = i % sh.inner, i // sh.inner
    me = i * sh.cols + j
    chip, core = j // 2, j % 2
    mate = (i, chip * 2 + 1 - core)
    team = x * sh.cols + j
    slots, strip, size = sh.slots, sh.strip, sh.size
    all_but_me = sh.devices - 1

    def member(d):
        e = sh.team - d
        qx = (x + e // sh.cols) % sh.inner
        qj = (chip + (e // 2) % sh.chips) % sh.chips * 2 + (core + e % 2) % 2
        return qx * sh.cols + qj, (z * sh.inner + qx, qj)

    def for_others(act):
        for t in range(sh.outer - 1):
            zt = sh.layer_at(z, t)

            @pl.loop(0, sh.team)
            def _(q):
                act((zt * sh.inner + q // sh.cols, q % sh.cols))

        @pl.loop(1, sh.team)
        def _(d):
            act(member(d)[1])

    def in_strip(q):
        return pl.ds(pl.multiple_of(q * strip, strip), strip)

    fetches = [
        pltpu.make_async_copy(source, target, fetch.at[k])
        for k, (source, target) in enumerate(
            (
                (pw_hbm, pw), (pc_hbm, pc), (hw_hbm, hw), (hc_hbm, hc),
                (h_hbm, h_ref), (p_hbm, p_ref),
            )
        )
    ]
    for copy in fetches:
        copy.start()
    barrier = pltpu.get_barrier_semaphore()

    for_others(lambda dev: pl.semaphore_signal(barrier, inc=1, device_id=dev, device_id_type=MESH))

    for copy in fetches[:4]:
        copy.wait()
    lane = iota((1, 128), 1)
    packed = jnp.zeros((1, 128), F32)
    for where, count, scale in ((pw, pc, 1.0), (hw, hc, 16.0)):
        for s in range(slots):
            at = (where[0, s] - i * TILE) * sh.width + where[1, s] - j * sh.width
            packed = packed + jnp.where((lane == at) & (s < count[0, 0]), scale * (s + 1), 0.0)
    message[0] = packed
    messages[me] = packed
    for copy in fetches[4:]:
        copy.wait()
    for s in range(slots):
        near_h[team * slots + s] = h_ref[s, in_strip(team), :]
        near_p[team * slots + s] = p_ref[s, in_strip(team), :]
        prow[s] = p_ref[s]
    pl.semaphore_wait(barrier, all_but_me)

    def tell(dev):
        remote(message.at[pl.ds(0, 1)], messages.at[pl.ds(me, 1)], m_send, m_recv, dev).start()

    for_others(tell)

    def strips(d, which):
        q, dev = member(d)
        ref, near = ((h_ref, near_h), (p_ref, near_p))[which]
        return remote(
            ref.at[:, in_strip(q), :], near.at[pl.ds(team * slots, slots)],
            s_send.at[which, d], s_recv.at[which, team], dev,
        )

    def strips_in(d, which):
        q, dev = member(d)
        ref, near = ((h_ref, near_h), (p_ref, near_p))[which]
        return remote(
            ref.at[:, in_strip(q), :], near.at[pl.ds(q * slots, slots)],
            s_send.at[which, d], s_recv.at[which, q], dev,
        )

    for which in range(2):
        for d in range(1, sh.team):
            strips(d, which).start()

    def other(dc):
        c = (chip + dc) % sh.chips
        return c, c * 2 + core

    p_mate = remote(p_ref, prow.at[pl.ds(slots, slots)], p_send.at[0], p_recv.at[sh.cols], mate)
    p_mate.start()

    def p_block(col):
        return prow.at[pl.ds(sh.others + col * CAP_R, CAP_R)]

    def p_out(dc):
        return remote(pack_r.at[dc - 1], p_block(j), p_send.at[dc], p_recv.at[j], (i, other(dc)[1]))

    def p_in(dc):
        col = other(dc)[1]
        return remote(pack_r.at[dc - 1], p_block(col), p_send.at[dc], p_recv.at[col], (i, col))

    def p_forward(dc):
        col = other(dc)[1]
        return remote(p_block(col), p_block(col), p_fwd.at[dc], p_recv.at[col], mate)

    def p_forward_in(dc):
        col = other(dc)[0] * 2 + 1 - core
        return remote(p_block(col), p_block(col), p_fwd.at[dc], p_recv.at[col], mate)

    def bulk(ref, sem):
        part = ref.at[pl.ds(0, all_but_me)]
        return pltpu.make_async_copy(part, part, sem)

    bulk(messages, m_recv).wait()
    lists = Lists(sh, x, z, j, messages[:, 0, :])

    def publish(source, target, which):
        copy = pltpu.make_async_copy(source, target, t_copy.at[which])
        copy.start()
        copy.wait()

    def entry(ref, table, row, lane):
        return ref[jnp.minimum(jnp.maximum(table[row, lane], 0), ref.shape[0] - 1)]

    kinds = (
        (store_h, pack_hz, pack_h, land_h, CAP_H_Z, CAP_H, near_h, tab_h),
        (store_p, pack_pz, pack_p, land_p, CAP_P_Z, CAP_P, near_p, tab),
    )

    def zone(which, layer):
        store, cap = kinds[which][0], kinds[which][4]
        return store.at[pl.ds(sh.team * slots + layer * cap, cap)]

    def across(which, dz):
        pack = kinds[which][1]
        zd = sh.layer_at(z, dz - 1)
        return remote(
            pack.at[dz - 1], zone(which, z), z_send.at[which, dz], z_recv.at[which, z],
            (zd * sh.inner + x, j),
        )

    def across_in(which, dz):
        pack = kinds[which][1]
        zs = sh.layer_at(z, dz - 1)
        return remote(
            pack.at[dz - 1], zone(which, zs), z_send.at[which, dz], z_recv.at[which, zs],
            (zs * sh.inner + x, j),
        )

    def part(which, d):
        pack, land = kinds[which][2], kinds[which][3]
        _, dev = member(d)
        return remote(
            pack.at[d - 1], land.at[:, in_strip(team), :], t_send.at[which, d], t_recv.at[which, team], dev
        )

    def part_in(which, d):
        pack, land = kinds[which][2], kinds[which][3]
        q, dev = member(d)
        return remote(
            pack.at[d - 1], land.at[:, in_strip(q), :], t_send.at[which, d], t_recv.at[which, q], dev
        )

    def send_across(which):
        store, pack, _, _, cap, _, near, _ = kinds[which]
        for d in range(1, sh.team):
            strips_in(d, which).wait_recv()
        for dz in range(1, sh.outer):
            for k in range(cap):
                pack[dz - 1, k] = entry(near, tab_z, which, (dz - 1) * LIST_Z + k)
        for dz in range(1, sh.outer):
            across(which, dz).start()
        store[0 : sh.team * slots] = near[...]

    def to_trace(xd):
        return remote(
            pack_d.at[xd], land_d.at[:, in_strip(team), :], d_send.at[xd], d_recv.at[team],
            (z * sh.inner + xd, sh.trace_member(z, xd) % sh.cols),
        )

    def trace_in(d):
        q, dev = member(d)
        return remote(pack_d.at[0], land_d.at[:, in_strip(q), :], d_send.at[0], d_recv.at[q], dev)

    def send_trace():
        for xd in range(sh.inner):
            for k in range(CAP_D):
                pack_d[xd, k] = entry(store_h, tab_h, 1, xd * EIGHT + k)
        for xd in range(sh.inner):
            @pl.when(sh.trace_member(z, xd) != team)
            def _():
                to_trace(xd).start()

            @pl.when(sh.trace_member(z, xd) == team)
            def _():
                for k in range(CAP_D):
                    land_d[k, in_strip(team), :] = pack_d[xd, k]

    def send_parts(which):
        store, _, pack, land, _, cap, _, table = kinds[which]
        for dz in range(1, sh.outer):
            across_in(which, dz).wait_recv()
        if which == 0:
            send_trace()

        @pl.loop(1, sh.team)
        def _(d):
            q, _ = member(d)
            for k in range(cap):
                pack[d - 1, k] = entry(store, table, 0, q * LIST + k)

        for d in range(1, sh.team):
            part(which, d).start()
        for k in range(cap):
            land[k, in_strip(team), :] = entry(store, table, 0, team * LIST + k)

    over = lists.across(tabv_z)
    publish(tabv_z, tab_z, 0)
    send_across(0)
    over = over + lists.row_lists(tabv_r)
    publish(tabv_r, tab_r, 1)
    for dc in range(1, sh.chips):
        for k in range(CAP_R):
            pack_r[dc - 1, k] = entry(p_ref, tab_r, 0, (dc - 1) * EIGHT + k)
    for dc in range(1, sh.chips):
        p_out(dc).start()
    over = over + lists.team_lists(0, tabv_h)
    publish(tabv_h, tab_h, 2)
    send_across(1)
    send_parts(0)
    for dc in range(1, sh.chips):
        p_in(dc).wait_recv()
        p_forward(dc).start()
    over = over + lists.team_lists(1, tabv)
    over = over + lists.products(pw, pc, tabv)
    publish(tabv, tab, 3)
    p_mate.wait_recv()
    for dc in range(1, sh.chips):
        p_forward_in(dc).wait_recv()
    emsg[0, 0] = jnp.zeros((1, 128), F32)

    @pl.when(sh.trace_member(z, x) == team)
    def _():
        for d in range(1, sh.team):
            trace_in(d).wait_recv()
        for k in range(CAP_D):
            part_of = entry(prow, tab_h, 2, k).astype(F32) * jnp.transpose(land_d[k].astype(F32))
            total = jnp.sum(part_of, axis=0, keepdims=True)
            emsg[0, 0] += total * tab_h[2, 32 + k].astype(F32)

    emsg[0, 1] = over + jnp.zeros((1, 128), F32)
    emsgs[me] = emsg[0]

    def tell_energy(dev):
        remote(emsg.at[pl.ds(0, 1)], emsgs.at[pl.ds(me, 1)], e_send, e_recv, dev).start()

    for_others(tell_energy)
    send_parts(1)

    def multiply(step, left, right, terms, cap):
        row = 2 + step
        acc = None
        for k in range(cap):
            d = jnp.dot(entry(left, tab, row, k), entry(right, tab, row, 32 + k), preferred_element_type=F32)
            acc = d if acc is None else d + acc * tab[row, 64 + k].astype(F32)
            terms[k] = acc
        terms[cap] = jnp.zeros((size, size), F32)

    for d in range(1, sh.team):
        part_in(0, d).wait_recv()
    multiply(0, prow, land_h, terms_1, CAP_1)
    for s in range(slots):
        value = entry(terms_1, tab, 2, 96 + s)
        rounded = value.astype(BF16)
        fstore[s] = rounded
        out[s] = rounded

    for k in range(CAP_V):
        fstore[slots + k] = entry(terms_1, tab, 2, 96 + LIST + k).astype(BF16)


    for d in range(1, sh.team):
        part_in(1, d).wait_recv()
    multiply(1, fstore, land_p, terms_2, CAP_2)
    for s in range(slots):
        out[slots + s] = entry(terms_2, tab, 3, 96 + s).astype(BF16)

    bulk(emsgs, e_recv).wait()
    e_out[...] = jnp.sum(jnp.sum(emsgs[:, 0], axis=0), axis=1, keepdims=True) + jnp.zeros((8, 128), F32)
    over_out[0, 0] = jnp.sum(jnp.sum(emsgs[:, 1], axis=0))

    bulk(messages, m_send).wait()
    bulk(emsgs, e_send).wait()
    for which in range(2):
        for d in range(1, sh.team):
            strips(d, which).wait_send()
            part(which, d).wait_send()
        for dz in range(1, sh.outer):
            across(which, dz).wait_send()
    for xd in range(sh.inner):
        @pl.when(sh.trace_member(z, xd) != team)
        def _():
            to_trace(xd).wait_send()
    p_mate.wait_send()
    for dc in range(1, sh.chips):
        p_out(dc).wait_send()
        p_forward(dc).wait_send()


def sparse_path(sh, p_values, p_where, p_count, h_values, h_where, h_count):
    slots, size, strip = sh.slots, sh.size, sh.strip
    block, piece = (size, size), (strip, size)
    bf = lambda *shape: pltpu.VMEM(shape, BF16)
    f32 = lambda *shape: pltpu.VMEM(shape, F32)
    dma = pltpu.SemaphoreType.DMA
    near = sh.team * slots
    away = max(sh.outer - 1, 1)
    chips = max(sh.chips - 1, 1)
    scalar = jax.ShapeDtypeStruct((1, 1), F32)
    return pl.pallas_call(
        functools.partial(sparse_products, sh),
        out_shape=[jax.ShapeDtypeStruct((2 * slots,) + block, BF16), jax.ShapeDtypeStruct((8, 128), F32), scalar],
        in_specs=[ANY] * 6,
        out_specs=[VMEM, VMEM, SMEM],
        scratch_shapes=[
            bf(slots, *block),
            bf(slots, *block),
            pltpu.SMEM((2, slots), I32),
            pltpu.SMEM((1, 1), I32),
            pltpu.SMEM((2, slots), I32),
            pltpu.SMEM((1, 1), I32),
            f32(1, 1, 128),
            f32(sh.devices, 1, 128),
            bf(near, *piece),
            bf(near, *piece),
            bf(near + sh.outer * CAP_H_Z, *piece),
            bf(near + sh.outer * CAP_P_Z, *piece),
            bf(sh.others + sh.cols * CAP_R, *block),
            bf(chips, CAP_R, *block),
            bf(away, CAP_H_Z, *piece),
            bf(away, CAP_P_Z, *piece),
            bf(sh.team, CAP_H, *piece),
            bf(sh.team, CAP_P, *piece),
            bf(sh.inner, CAP_D, *piece),
            bf(CAP_D, *block),
            bf(CAP_H, *block),
            bf(CAP_P, *block),
            f32(CAP_1 + 1, *block),
            f32(CAP_2 + 1, *block),
            bf(slots + CAP_V, *block),
            pltpu.VMEM((8, 128), I32),
            pltpu.VMEM((8, 128), I32),
            pltpu.VMEM((8, 128), I32),
            pltpu.VMEM((8, 128), I32),
            pltpu.SMEM((8, 128), I32),
            pltpu.SMEM((8, 128), I32),
            pltpu.SMEM((8, 128), I32),
            pltpu.SMEM((8, 128), I32),
            f32(1, 2, 1, 128),
            f32(sh.devices, 2, 1, 128),
            dma, dma,
            dma((2, sh.team)), dma((2, sh.team)),
            dma((sh.chips,)), dma((sh.chips,)), dma((sh.cols + 1,)),
            dma((2, sh.outer)), dma((2, sh.outer)),
            dma((2, sh.team)), dma((2, sh.team)),
            dma((sh.inner,)), dma((sh.team,)),
            dma, dma, dma((4,)), dma((6,)),
        ],
        compiler_params=pltpu.CompilerParams(collective_id=2, has_side_effects=True, vmem_limit_bytes=24 << 20),
        name="sparse_products",
    )(p_values, h_values, p_where.T, p_count, h_where.T, h_count)


def deliver(both, energy):
    def kernel(both_ref, e_in, first, second, e_out, e_one, sems):
        slots = first.shape[0]
        e_one[...] = e_in[0:1, 0:1]
        moves = (
            (both_ref.at[pl.ds(0, slots)], first),
            (both_ref.at[pl.ds(slots, slots)], second),
            (e_one, e_out),
        )
        copies = [pltpu.make_async_copy(*move, sems.at[k]) for k, move in enumerate(moves)]
        for copy in copies:
            copy.start()
        for copy in copies:
            copy.wait()

    half = jax.ShapeDtypeStruct((both.shape[0] // 2,) + both.shape[1:], both.dtype)
    return pl.pallas_call(
        kernel,
        out_shape=[half, half, jax.ShapeDtypeStruct((1, 1), F32)],
        in_specs=[VMEM, VMEM],
        out_specs=[ANY, ANY, ANY],
        scratch_shapes=[pltpu.VMEM((1, 1), F32), pltpu.SemaphoreType.DMA((3,))],
        name="deliver",
    )(both, energy)


def per_device(rows, cols, *args):
    slots, size, _ = args[0].shape
    sh = Shape(rows, cols, slots, size)
    if not sh.fits():
        return dense_path(rows, cols, *args)
    both, energy, over = sparse_path(sh, *args)
    def dense():
        ph, php, total = dense_path(rows, cols, *args)
        return ph, php, total.reshape((1, 1))

    ph, php, energy = lax.cond(over[0, 0] > 0.0, dense, lambda: tuple(deliver(both, energy)))
    return ph, php, energy[0, 0]


def solution(mesh):
    placed = (
        P("row", "col", None),
        P("row", "col"),
        P("row", "col"),
        P("row", "col", None),
        P("row", "col"),
        P("row", "col"),
    )
    return jax.shard_map(
        functools.partial(per_device, mesh.shape["row"], mesh.shape["col"]),
        mesh=mesh,
        in_specs=placed,
        out_specs=(P("row", "col", None), P("row", "col", None), P()),
        check_vma=False,
    )
```
